512 devices in a mesh: gy: 4 (over x), gx: 4 (over z_hi, core), probe: 32 (over y, z_lo).
Axes of the slice: x: 4, y: 8, z: 8 (z_hi: 2, z_lo: 4; z = z_hi * 4 + z_lo), core: 2. Of those that a mesh axis runs over, the one named last changes fastest.
Arguments:
- state: bfloat16 [4, 16, 16, 640], P(None, 'gy', 'gx'), may hold values from -6 to 6
- probe_signs: int32 [64, 4, 16, 16, 640], P('probe', None, 'gy', 'gx'), may hold values from -1 to 1, as said below
- timesteps: int32 [4], replicated, may hold values from 0 to 999
- time_table: float32 [1000, 640], replicated, may hold values from -4 to 4
- gn_gain: float32 [640], replicated, may hold values from 0.5 to 1.5
- gn_shift: float32 [640], replicated, may hold values from -3 to 3
- conv_weight: bfloat16 [9, 640, 640], P(None, 'probe'), may hold values from -0.078125 to 0.078125
- conv_bias: float32 [640], replicated, may hold values from -3 to 3
Outputs:
- next_state: bfloat16 [4, 16, 16, 640], P(None, 'gy', 'gx')
- logp_delta: float32 [4], replicated
The draws below stay inside these ranges and needn't reach their ends.
Inputs may be any that keep to these rules, and one draw needn't show every extreme that they name: `probe_signs`: every entry is -1 or 1.
All inputs are finite; a program needn't handle non-finite values.
Results may differ from the reference program's by a relative error of at most 0.0034.
Values may be sent and summed in bfloat16 or wider, within the bound.
No kernel may reach another device: no remote copies, remote signals or barrier semaphores. Data moves between devices by JAX's collectives and lax.ppermute only.
A program may use at most 64 MiB of HBM per device.

```python
import jax
import jax.numpy as jnp
from jax import lax

C = 640
GROUPS = 32
STEPS = 1000
BATCH = 4
PROBES = 64
H = 16
W = 16


def draw_probe_signs(key, part):
    bits = jax.random.randint(key, (PROBES, BATCH, H, W, C), 0, 2, dtype=jnp.int32)
    return bits * 2 - 1


def plant(result, key, least, largest):
    longest = result.shape.index(max(result.shape))
    spots = []
    for shift in (0, 1):
        where = [jax.random.randint(jax.random.fold_in(key, axis), (), 0, length) for axis, length in enumerate(result.shape)]
        where[longest] = (where[longest] + shift) % result.shape[longest]
        spots.append(tuple(where))
    return result.at[spots[0]].set(least).at[spots[1]].set(largest)


def shard_levels(stream_key, extent, shards, least, top_value):
    def one(position, parts):
        heights = jax.random.uniform(jax.random.fold_in(jax.random.fold_in(stream_key, 6), position), (parts,), jnp.float32, least / len(shards), top_value / len(shards))
        return jnp.repeat(jnp.exp(heights), extent[position] // parts).reshape((-1,) + (1,) * (len(extent) - position - 1))

    gain = one(*shards[0])
    for cut in shards[1:]:
        gain = gain * one(*cut)
    return gain


def normal_values(key, extent, scale, most, pieces=(), kind=jnp.bfloat16):
    loudness = shard_levels(key, extent, pieces, -0.22, 0.18) if pieces else 1.0
    result = jax.random.normal(key, extent, jnp.float32) * scale * loudness
    return jnp.minimum(jnp.maximum(result, -most), most).astype(kind)


def setup_inputs(seed: int = 0) -> dict:
    key_of = jax.random.split(jax.random.key(seed), 9)
    state = normal_values(key_of[0], (BATCH, H, W, C), 1.0, 6.0, ((1, 4), (2, 4)))
    probe_signs = draw_probe_signs(jax.random.fold_in(key_of[8], 71), 0)
    timesteps = plant(jax.random.randint(key_of[2], (BATCH,), 0, STEPS), jax.random.fold_in(key_of[2], 1), 0, STEPS - 1).astype(jnp.int32)
    time_table = normal_values(key_of[3], (STEPS, C), 0.5, 4.0, (), jnp.float32)
    gn_gain = jnp.clip(1.0 + 0.1 * jax.random.normal(key_of[4], (C,), jnp.float32), 0.5, 1.5)
    gn_shift = normal_values(key_of[5], (C,), 0.5, 3.0, (), jnp.float32)
    conv_weight = normal_values(key_of[6], (9, C, C), (9 * C) ** -0.5, 0.078125, ((1, 32),))
    conv_bias = normal_values(key_of[7], (C,), 0.5, 3.0, (), jnp.float32)
    return {"state": state, "probe_signs": probe_signs, "timesteps": timesteps, "time_table": time_table, "gn_gain": gn_gain, "gn_shift": gn_shift, "conv_weight": conv_weight, "conv_bias": conv_bias}


def convolve(stack, weight):
    padded = jnp.pad(stack, ((0, 0), (1, 1), (1, 1), (0, 0)))
    count, height, width, chans = stack.shape
    total = jnp.zeros((count * height * width, weight.shape[2]), jnp.float32)
    for tap in range(9):
        row_off = tap // 3
        col_off = tap % 3
        window = padded[:, row_off:row_off + height, col_off:col_off + width, :].reshape(-1, chans)
        total = total + jnp.dot(window, weight[tap], preferred_element_type=jnp.float32)
    return total.reshape(count, height, width, weight.shape[2])

def reference(state, probe_signs, timesteps, time_table, gn_gain, gn_shift, conv_weight, conv_bias):
    batch, height, width, chans = state.shape
    group_width = chans // GROUPS
    count = height * width * group_width
    xf = state.astype(jnp.float32)
    grouped = xf.reshape(batch, height, width, GROUPS, group_width)
    mean_x = lax.optimization_barrier(jnp.sum(grouped, axis=(1, 2, 4))) / count
    var_x = lax.optimization_barrier(jnp.sum(grouped * grouped, axis=(1, 2, 4))) / count - mean_x * mean_x
    sigma = jnp.sqrt(var_x + 1e-05)[:, None, None, :, None]
    centered = grouped - mean_x[:, None, None, :, None]
    normal = (centered / sigma).reshape(batch, height, width, chans)
    embed = time_table[timesteps]
    pre = normal * gn_gain + gn_shift + embed[:, None, None, :]
    sig = jax.nn.sigmoid(pre)
    hidden = (pre * sig).astype(jnp.bfloat16)
    slope = sig * (1.0 + pre * (1.0 - sig)) * gn_gain
    velocity = convolve(hidden, conv_weight) + conv_bias
    next_state = (xf + 0.25 * velocity).astype(jnp.bfloat16)

    def one_probe(signs):
        ug = signs.astype(jnp.float32).reshape(batch, height, width, GROUPS, group_width)
        mean_u = lax.optimization_barrier(jnp.sum(ug, axis=(1, 2, 4))) / count
        mean_cu = lax.optimization_barrier(jnp.sum(ug * centered, axis=(1, 2, 4))) / count
        dnormal = (ug - mean_u[:, None, None, :, None]) / sigma - centered * mean_cu[:, None, None, :, None] / (sigma * sigma * sigma)
        dhidden = (slope * dnormal.reshape(batch, height, width, chans)).astype(jnp.bfloat16)
        tangent = convolve(dhidden, conv_weight)
        return lax.optimization_barrier(jnp.sum(signs.astype(jnp.float32) * tangent, axis=(1, 2, 3)))
    partials = lax.map(one_probe, probe_signs)
    logp_delta = -0.25 / probe_signs.shape[0] * lax.optimization_barrier(jnp.sum(partials, axis=0))
    return (next_state, logp_delta)
```

```python
import jax
import jax.numpy as jnp
from jax import lax
from jax.experimental import pallas as pl
from jax.experimental.pallas import tpu as pltpu
from jax.sharding import Mesh
from jax.sharding import PartitionSpec as P

GROUPS = 32
GX = ("gx_0", "gx_1")
PROBE = ("probe_0", "probe_1")
LANES = 128
PAIRS = 6
F32 = jnp.float32
BF16 = jnp.bfloat16
VMEM = pl.BlockSpec(memory_space=pltpu.VMEM)
SMEM = pl.BlockSpec(memory_space=pltpu.SMEM)
HBM = pl.BlockSpec(memory_space=pltpu.HBM)


def three_parts(value):
    high = value.astype(BF16)
    rest = value - high.astype(F32)
    mid = rest.astype(BF16)
    low = (rest - mid.astype(F32)).astype(BF16)
    return high, mid, low


def lane_block(index):
    return slice(index * LANES, (index + 1) * LANES)


def doubled_rows(rows):
    turned = pltpu.roll(rows, 4, axis=0)
    upper = lax.broadcasted_iota(jnp.int32, rows.shape, 0) < 4
    return jnp.where(upper, rows, turned), jnp.where(upper, turned, rows)


def pair_of(index):
    member = lax.axis_index("gy") * 2 + lax.axis_index("gx_1")
    number = member * PAIRS + index
    return lax.rem(number, 9), lax.div(number, 9)


def pack_kernel(
    signs_hbm, state_hbm, weight_hbm, wsend_ref, main_ref, rim_ref,
    signs_ref, state_ref, weight_ref, uf, xf, wf, rim, sums, arrived,
):
    blocks = uf.shape[0]
    loads = [
        pltpu.make_async_copy(src, dst, arrived.at[index])
        for index, (src, dst) in enumerate(
            ((weight_hbm, weight_ref), (state_hbm, state_ref), (signs_hbm, signs_ref))
        )
    ]
    for load in loads:
        load.start()
    loads[0].wait()
    for index in range(PAIRS):
        tap, ob = pair_of(index)
        rows = weight_ref[tap].astype(F32)
        picked = jnp.zeros((rows.shape[0], LANES), F32)
        for o in range(blocks):
            picked = picked + jnp.where(ob == o, rows[:, lane_block(o)], 0.0)
        wf[pl.ds(index, rows.shape[0], stride=PAIRS), :] = picked
    packed = wf[...].astype(BF16)
    for target in range(wsend_ref.shape[0]):
        wsend_ref[target] = packed

    loads[1].wait()
    loads[2].wait()
    for p in range(2):
        for b in range(4):
            for r in range(4):
                line = signs_ref[p, b, r].astype(F32)
                for o in range(blocks):
                    uf[o, pl.ds(r * 32 + p * 4 + b, 4, stride=8), :] = line[:, lane_block(o)]
    for b in range(4):
        for r in range(4):
            line = state_ref[b, r].astype(F32)
            for o in range(blocks):
                xf[o, pl.ds(r * 16 + b, 4, stride=4), :] = line[:, lane_block(o)]

    edge = jnp.where(lax.axis_index("gx_0") == 0, 3, 0)
    for o in range(blocks):
        sum_u = jnp.zeros((8, LANES), F32)
        cross = jnp.zeros((8, LANES), F32)
        sum_x = jnp.zeros((8, LANES), F32)
        sum_xx = jnp.zeros((8, LANES), F32)
        for two in range(8):
            pair = doubled_rows(xf[o, two * 8 : two * 8 + 8, :])
            for half in range(2):
                cell = two * 2 + half
                x = pair[half]
                u = uf[o, cell * 8 : cell * 8 + 8, :]
                sum_u, cross = sum_u + u, cross + u * x
                sum_x, sum_xx = sum_x + x, sum_xx + x * x
        for kind, part in enumerate((sum_u, cross, sum_x, sum_xx)):
            sums[kind * 8 : kind * 8 + 8, lane_block(o)] = part
        for r in range(4):
            rim[r * 8 : r * 8 + 8, lane_block(o)] = uf[o, pl.ds(pl.multiple_of((r * 4 + edge) * 8, 8), 8), :]
            rim[32 + r * 4 : 36 + r * 4, lane_block(o)] = xf[o, pl.ds((r * 4 + edge) * 4, 4), :]

    width = sums.shape[1] // GROUPS
    row = lax.broadcasted_iota(jnp.int32, (sums.shape[1], LANES), 0)
    first = lax.broadcasted_iota(jnp.int32, (sums.shape[1], LANES), 1) * width
    member = jnp.where((row >= first) & (row < first + width), 1.0, 0.0).astype(BF16)
    grouped = jnp.zeros((32, LANES), F32)
    for part in three_parts(sums[...]):
        grouped = grouped + jnp.dot(part, member, preferred_element_type=F32)
    stats = grouped[0:8]
    for kind in range(1, 4):
        stats = stats + pltpu.roll(grouped[kind * 8 : kind * 8 + 8], GROUPS * kind, axis=1)
    rim[48:56, :] = jnp.zeros((8, rim.shape[1]), F32)
    for index, part in enumerate(three_parts(stats)):
        rim[48:56, lane_block(index)] = part.astype(F32)

    for o in range(blocks):
        main_ref[0:128, lane_block(o)] = uf[o].astype(BF16)
        main_ref[128:192, lane_block(o)] = xf[o].astype(BF16)
    rim_ref[...] = rim[...].astype(BF16)


def mix_kernel(
    own0, own1, own2, own3, other0, other1, other2, other3, weight_ref, gain_ref, offset_ref,
    out_ref, ug, xg, embed, picked, lhs_ref, slope_ref, rows_ref, wf, wc, velocity,
):
    blocks = ug.shape[0]
    core = lax.axis_index("gx_1")
    half = lax.axis_index("gx_0")
    probe = lax.axis_index("probe_0") * lax.axis_size("probe_1") + lax.axis_index("probe_1")
    chans = own0.shape[1]
    ug[...] = jnp.zeros(ug.shape, F32)
    xg[...] = jnp.zeros(xg.shape, F32)

    def spot(row, col):
        return pl.multiple_of((row * 10 + col) * 8, 8)

    total = jnp.zeros((8, chans), F32)
    rim_here = core == 1 - half
    rim_col = jnp.where(half == 0, 9, 0)
    for back, (own_ref, other_ref) in enumerate(((own0, other0), (own1, other1), (own2, other2), (own3, other3))):
        tile = lax.rem(lax.axis_index("gy") + 4 - back, 4)
        for src, base in ((own_ref, 4 * core), (other_ref, 4 * (1 - core))):
            for r in range(4):
                at = spot(4 * tile + r + 1, base + 1)
                lines = src[r * 32 : r * 32 + 32, :].astype(F32)
                states = src[128 + r * 16 : 144 + r * 16, :].astype(F32)
                for o in range(blocks):
                    ug[o, pl.ds(at, 32), :] = lines[:, lane_block(o)]
                    for two in range(2):
                        pair = doubled_rows(states[two * 8 : two * 8 + 8, lane_block(o)])
                        xg[o, pl.ds(pl.multiple_of(at + two * 16, 8), 8), :] = pair[0]
                        xg[o, pl.ds(pl.multiple_of(at + two * 16 + 8, 8), 8), :] = pair[1]
        mine = own_ref[192:256, :].astype(F32)
        theirs = other_ref[192:256, :].astype(F32)
        total = total + mine[48:56] + mine[56:64] + theirs[48:56] + theirs[56:64]
        rim = jnp.where(rim_here, mine[0:48], theirs[0:48])
        for r in range(4):
            at = spot(4 * tile + r + 1, rim_col)
            for o in range(blocks):
                ug[o, pl.ds(at, 8), :] = rim[r * 8 : r * 8 + 8, lane_block(o)]
        for two in range(2):
            for o in range(blocks):
                pair = doubled_rows(rim[32 + two * 8 : 40 + two * 8, lane_block(o)])
                for one in range(2):
                    at = spot(4 * tile + two * 2 + one + 1, rim_col)
                    xg[o, pl.ds(at, 8), :] = pair[one]

    stats = total[:, lane_block(0)] + total[:, lane_block(1)] + total[:, lane_block(2)]
    width = chans // GROUPS
    lane = lax.broadcasted_iota(jnp.int32, (LANES, chans), 1)
    first = lax.broadcasted_iota(jnp.int32, (LANES, chans), 0) * width
    spread = jnp.where((lane >= first) & (lane < first + width), 1.0, 0.0).astype(BF16)

    def expanded(kind):
        turned = stats if kind == 0 else pltpu.roll(stats, LANES - GROUPS * kind, axis=1)
        out = jnp.zeros((8, chans), F32)
        for part in three_parts(turned):
            out = out + jnp.dot(part, spread, preferred_element_type=F32)
        return out

    count = 256 * width
    sum_u, cross, sum_x, sum_xx = (expanded(kind) for kind in range(4))
    mean = sum_x / count
    sigma = jnp.sqrt(sum_xx / count - mean * mean + 1e-05)
    inverse = 1.0 / sigma
    mean_u = sum_u / count
    mean_cu = (cross - mean * sum_u) / count
    bend = mean_cu / (sigma * sigma * sigma)
    for b in range(4):
        line = offset_ref[b : b + 1, :]
        embed[b : b + 1, :] = line
        embed[b + 4 : b + 5, :] = line
    offset = embed[...]
    gain = gain_ref[...]

    def fields(x, o):
        at = lane_block(o)
        centered = x - mean[:, at]
        pre = centered * inverse[:, at] * gain[:, at] + offset[:, at]
        sig = 1.0 / (1.0 + jnp.exp(-pre))
        return centered, pre, sig

    def grid_row(gr, carry):
        at = spot(gr + 1, 1)
        for o in range(blocks):
            ln = lane_block(o)
            x = xg[o, pl.ds(at, 64), :].reshape(8, 8, LANES)
            u = ug[o, pl.ds(at, 64), :].reshape(8, 8, LANES)
            centered, pre, sig = fields(x, o)
            xg[o, pl.ds(at, 64), :] = (pre * sig).reshape(64, LANES)
            slope = sig * (1.0 + pre * (1.0 - sig)) * gain[:, ln]
            direction = (u - mean_u[:, ln]) * inverse[:, ln] - centered * bend[:, ln]
            out = (slope * direction).reshape(64, LANES).astype(BF16)
            slope_ref[pl.ds(pl.multiple_of(gr * 64, 64), 64), ln] = out
            edge = spot(gr + 1, rim_col)
            _, pre, sig = fields(xg[o, pl.ds(edge, 8), :], o)
            xg[o, pl.ds(edge, 8), :] = pre * sig
        return carry

    lax.fori_loop(0, 16, grid_row, 0)

    taps = [pair_of(index) for index in range(PAIRS)]

    def lhs_row(gr, carry):
        for index, (tap, ob) in enumerate(taps):
            dy, dx = lax.div(tap, 3), lax.rem(tap, 3)
            at = spot(gr + 2 - dy, 2 - dx)
            value = ug[jnp.minimum(ob, blocks - 1), pl.ds(at, 64), :]
            lhs_ref[pl.ds(pl.multiple_of(gr * 64, 64), 64), lane_block(index)] = value.astype(BF16)
        return carry

    lax.fori_loop(0, 16, lhs_row, 0)

    latent, spots = lax.div(probe, 8), lax.rem(probe, 8)
    row, col = lax.div(spots, 2), 2 * lax.rem(spots, 2)
    for index, (tap, ob) in enumerate(taps):
        dy, dx = lax.div(tap, 3), lax.rem(tap, 3)
        for target in range(8):
            at = ((4 * (target // 2) + row + dy) * 10 + 4 * (target % 2) + col + dx) * 8 + latent
            for o in range(blocks):
                picked[o, index * 16 + target * 2 : index * 16 + target * 2 + 2, :] = xg[o, pl.ds(at, 2, stride=8), :]
    for o in range(blocks):
        rows_ref[:, lane_block(o)] = picked[o].astype(BF16)

    each = weight_ref.shape[1]
    for source in range(weight_ref.shape[0]):
        wf[source * each : (source + 1) * each, :] = weight_ref[source].astype(F32)
    for index in range(PAIRS):
        wc[:, lane_block(index)] = wf[pl.ds(index, chans, stride=PAIRS), :].astype(BF16)

    chunk = 256
    total = jnp.zeros((8, chans), F32)
    for start in range(0, lhs_ref.shape[0], chunk):
        value = lax.dot_general(
            lhs_ref[start : start + chunk, :], wc[...], (((1,), (1,)), ((), ())), preferred_element_type=F32
        )
        value = value * slope_ref[start : start + chunk, :].astype(F32)
        total = total + jnp.sum(value.reshape(chunk // 8, 8, chans), axis=0)
    lanes = total[:, lane_block(0)]
    for o in range(1, blocks):
        lanes = lanes + total[:, lane_block(o)]
    lanes = lanes + pltpu.roll(lanes, 4, axis=0)

    velocity[...] = jnp.zeros(velocity.shape, F32)
    for index in range(PAIRS):
        ob = jnp.minimum(taps[index][1], blocks - 1)
        part = jnp.dot(rows_ref[index * 16 : index * 16 + 16, :], wc[:, lane_block(index)], preferred_element_type=F32)
        velocity[ob] = velocity[ob] + part
    for o in range(blocks):
        for j in range(2):
            out_ref[pl.ds(o * 2 + j, 8, stride=16), :] = velocity[o, pl.ds(j, 8, stride=2), :]
    for b in range(4):
        out_ref[pl.ds(10 + b, 8, stride=16), :] = jnp.broadcast_to(lanes[b : b + 1, :], (8, LANES))
    for b in range(2):
        out_ref[pl.ds(14 + b, 8, stride=16), :] = jnp.zeros((8, LANES), F32)


def step_kernel(parts_ref, state_ref, bias_ref, out_ref, lines, message):
    blocks = bias_ref.shape[1] // LANES
    probe = lax.axis_index("probe_0") * lax.axis_size("probe_1") + lax.axis_index("probe_1")
    latent, spots = lax.div(probe, 8), lax.rem(probe, 8)
    row, col = lax.div(spots, 2), 2 * lax.rem(spots, 2)
    total = parts_ref[0:16, :]
    for source in range(1, 8):
        total = total + parts_ref[source * 16 : source * 16 + 16, :]
    here = state_ref[latent, row].astype(F32)
    for o in range(blocks):
        lines[o] = here[:, lane_block(o)]
    for o in range(blocks):
        x = lines[o, pl.ds(col, 2), :]
        message[o * 2 : o * 2 + 2, :] = x + 0.25 * (total[o * 2 : o * 2 + 2, :] + bias_ref[:, lane_block(o)])
    mass = jnp.sum(total[10:14, :], axis=1, keepdims=True)
    lane = lax.broadcasted_iota(jnp.int32, (4, LANES), 1)
    coded = jnp.zeros((4, LANES), F32)
    for index, part in enumerate(three_parts(jnp.broadcast_to(mass, (4, LANES)))):
        coded = jnp.where(lane == index, part.astype(F32), coded)
    message[10:14, :] = coded
    message[14:16, :] = jnp.zeros((2, LANES), F32)
    packed = message[...].astype(BF16)
    for target in range(out_ref.shape[0]):
        out_ref[target] = packed


def final_kernel(scale, parts_ref, next_ref, mass_ref, wide, lines):
    blocks = lines.shape[0]
    total = jnp.zeros((16, LANES), F32)
    for source in range(64):
        value = parts_ref[source].astype(F32)
        wide[source * 16 : source * 16 + 16, :] = value
        total = total + value
    for b in range(4):
        mass_ref[b] = scale * jnp.sum(total[10 + b : 11 + b, :])
    start = lax.axis_index("gx_0") * 512
    for o in range(blocks):
        for j in range(2):
            lines[o, pl.ds(j, 32, stride=2), :] = wide[pl.ds(start + o * 2 + j, 32, stride=16), :]
    for o in range(blocks):
        for b in range(4):
            for r in range(4):
                at = b * 16 + r * 4
                next_ref[b, r, :, lane_block(o)] = lines[o, at : at + 4, :].astype(BF16)


def shape(dims, kind):
    return jax.ShapeDtypeStruct(dims, kind)


def body(state, probe_signs, timesteps, time_table, gn_gain, gn_shift, conv_weight, conv_bias):
    chans = state.shape[3]
    blocks = chans // LANES
    each = conv_weight.shape[1] * PAIRS
    params = pltpu.CompilerParams(vmem_limit_bytes=40 * 1024 * 1024)
    wsend, main, rim = pl.pallas_call(
        pack_kernel,
        out_shape=(shape((32, each, LANES), BF16), shape((192, chans), BF16), shape((56, chans), BF16)),
        in_specs=[HBM] * 3,
        out_specs=(VMEM,) * 3,
        scratch_shapes=[
            pltpu.VMEM(probe_signs.shape, jnp.int32),
            pltpu.VMEM(state.shape, BF16),
            pltpu.VMEM(conv_weight.shape, BF16),
            pltpu.VMEM((blocks, 128, LANES), F32),
            pltpu.VMEM((blocks, 64, LANES), F32),
            pltpu.VMEM((each, LANES), F32),
            pltpu.VMEM((56, chans), F32),
            pltpu.VMEM((32, chans), F32),
            pltpu.SemaphoreType.DMA((3,)),
        ],
        compiler_params=params,
        name="pack",
    )(probe_signs, state, conv_weight)

    across = [(a * 2 + b, (1 - a) * 2 + 1 - b) for a in range(2) for b in range(2)]
    with jax.named_scope("facing"):
        facing = lax.ppermute(rim, GX, across)
    with jax.named_scope("spread"):
        weights = lax.all_to_all(wsend, PROBE, 0, 0, tiled=True)
    block = jnp.concatenate([main, facing, rim[48:56]], axis=0)
    own = [block] + [None] * 3
    with jax.named_scope("column"):
        for back in (1, 3, 2):
            own[back] = lax.ppermute(block, "gy", [(i, (i + back) % 4) for i in range(4)])
    with jax.named_scope("partner"):
        other = [lax.ppermute(tile, "gx_1", [(0, 1), (1, 0)]) for tile in own]

    lines = [lax.dynamic_slice(time_table, (timesteps[b], jnp.int32(0)), (1, chans), allow_negative_indices=False) for b in range(4)]
    offset = jnp.concatenate(lines, axis=0) + gn_shift[None]
    partial = pl.pallas_call(
        mix_kernel,
        out_shape=shape((128, LANES), F32),
        in_specs=[VMEM] * 11,
        out_specs=VMEM,
        scratch_shapes=[
            pltpu.VMEM((blocks, 1440, LANES), F32),
            pltpu.VMEM((blocks, 1440, LANES), F32),
            pltpu.VMEM((8, chans), F32),
            pltpu.VMEM((blocks, PAIRS * 16, LANES), F32),
            pltpu.VMEM((1024, PAIRS * LANES), BF16),
            pltpu.VMEM((1024, chans), BF16),
            pltpu.VMEM((PAIRS * 16, chans), BF16),
            pltpu.VMEM((32 * each, LANES), F32),
            pltpu.VMEM((chans, PAIRS * LANES), BF16),
            pltpu.VMEM((blocks, 16, LANES), F32),
        ],
        compiler_params=params,
        name="mix",
    )(*own, *other, weights, gn_gain[None], offset)

    partial = lax.all_to_all(partial.reshape(8, 16, LANES), ("gy", "gx_1"), 0, 0, tiled=True)
    message = pl.pallas_call(
        step_kernel,
        out_shape=shape((64, 16, LANES), BF16),
        in_specs=[VMEM] * 3,
        out_specs=VMEM,
        scratch_shapes=[pltpu.VMEM((blocks, 4, LANES), F32), pltpu.VMEM((16, LANES), F32)],
        compiler_params=params,
        name="step",
    )(partial.reshape(128, LANES), state, conv_bias[None])
    parts = lax.all_to_all(message, ("gx_0",) + PROBE, 0, 0, tiled=True)
    scale = -0.25 / (probe_signs.shape[0] * lax.axis_size(PROBE))
    following, mass = pl.pallas_call(
        lambda *refs: final_kernel(scale, *refs),
        out_shape=(shape(state.shape, BF16), shape((4,), F32)),
        in_specs=[VMEM],
        out_specs=(VMEM, SMEM),
        scratch_shapes=[pltpu.VMEM((1024, LANES), F32), pltpu.VMEM((blocks, 64, LANES), F32)],
        compiler_params=params,
        name="final",
    )(parts)
    return following, mass


def solution(mesh):
    split = Mesh(
        mesh.devices.reshape(mesh.shape["gy"], 2, 2, 8, 4),
        ("gy", "gx_0", "gx_1", "probe_0", "probe_1"),
    )
    return jax.shard_map(
        body,
        mesh=split,
        in_specs=(
            P(None, "gy", GX, None),
            P(PROBE, None, "gy", GX, None),
            P(),
            P(),
            P(),
            P(),
            P(None, PROBE, None),
            P(),
        ),
        out_specs=(P(None, "gy", GX, None), P()),
        check_vma=False,
    )
```

```python
import jax
import jax.numpy as jnp
from jax import lax
from jax.experimental import pallas as pl
from jax.experimental.pallas import tpu as pltpu
from jax.sharding import Mesh
from jax.sharding import PartitionSpec as P


GROUPS = 32
GX = ("gx_0", "gx_1")
PROBE = ("probe_0", "probe_1")
LANES = 128
PAIRS = 6
F32 = jnp.float32
BF16 = jnp.bfloat16
VMEM = pl.BlockSpec(memory_space=pltpu.VMEM)
SMEM = pl.BlockSpec(memory_space=pltpu.SMEM)
HBM = pl.BlockSpec(memory_space=pltpu.HBM)


def three_parts(value):
    high = value.astype(BF16)
    rest = value - high.astype(F32)
    mid = rest.astype(BF16)
    low = (rest - mid.astype(F32)).astype(BF16)
    return high, mid, low


def lane_block(index):
    return slice(index * LANES, (index + 1) * LANES)


def doubled_rows(rows):
    turned = pltpu.roll(rows, 4, axis=0)
    upper = lax.broadcasted_iota(jnp.int32, rows.shape, 0) < 4
    return jnp.where(upper, rows, turned), jnp.where(upper, turned, rows)


def quarter():
    return 2 * lax.rem(lax.axis_index("probe_0"), 2) + lax.rem(lax.axis_index("probe_1"), 2)


def pair_of(index):
    member = lax.axis_index("gy") * 2 + lax.axis_index("gx_1")
    number = member * PAIRS + index
    return lax.rem(number, 9), lax.div(number, 9)


def pack_kernel(
    step_ref, signs_hbm, state_hbm, weight_hbm, table_hbm, shift_ref, wsend_ref, main_ref, rim_ref, offset_ref,
    signs_ref, state_ref, weight_ref, table, uf, xf, wf, rim, sums, arrived, found,
):
    blocks = uf.shape[0]
    loads = [
        pltpu.make_async_copy(src, dst, arrived.at[index])
        for index, (src, dst) in enumerate(
            ((weight_hbm, weight_ref), (state_hbm, state_ref), (signs_hbm, signs_ref))
        )
    ]
    for load in loads:
        load.start()
    steps = [step_ref[b] for b in range(4)]
    finds = [
        pltpu.make_async_copy(
            table_hbm.at[pl.ds(pl.multiple_of(lax.div(steps[b], 8) * 8, 8), 8), :], table.at[b], found.at[b]
        )
        for b in range(4)
    ]
    for find in finds:
        find.start()
    loads[0].wait()
    for index in range(PAIRS):
        tap, ob = pair_of(index)
        rows = weight_ref[tap].astype(F32)
        picked = jnp.zeros((rows.shape[0], LANES), F32)
        for o in range(blocks):
            picked = picked + jnp.where(ob == o, rows[:, lane_block(o)], 0.0)
        wf[pl.ds(index, rows.shape[0], stride=PAIRS), :] = picked
    packed = wf[...].astype(BF16)
    for target in range(wsend_ref.shape[0]):
        wsend_ref[target] = packed

    loads[1].wait()
    loads[2].wait()
    for p in range(2):
        for b in range(4):
            for r in range(4):
                line = signs_ref[p, b, r].astype(F32)
                for o in range(blocks):
                    uf[o, pl.ds(r * 32 + p * 4 + b, 4, stride=8), :] = line[:, lane_block(o)]
    for b in range(4):
        for r in range(4):
            line = state_ref[b, r].astype(F32)
            for o in range(blocks):
                xf[o, pl.ds(r * 16 + b, 4, stride=4), :] = line[:, lane_block(o)]

    edge = jnp.where(lax.axis_index("gx_0") == 0, 3, 0)
    for o in range(blocks):
        sum_u = jnp.zeros((8, LANES), F32)
        cross = jnp.zeros((8, LANES), F32)
        sum_x = jnp.zeros((8, LANES), F32)
        sum_xx = jnp.zeros((8, LANES), F32)
        for two in range(8):
            pair = doubled_rows(xf[o, two * 8 : two * 8 + 8, :])
            for half in range(2):
                cell = two * 2 + half
                x = pair[half]
                u = uf[o, cell * 8 : cell * 8 + 8, :]
                sum_u, cross = sum_u + u, cross + u * x
                sum_x, sum_xx = sum_x + x, sum_xx + x * x
        for kind, part in enumerate((sum_u, cross, sum_x, sum_xx)):
            sums[kind * 8 : kind * 8 + 8, lane_block(o)] = part
        for r in range(4):
            rim[r * 8 : r * 8 + 8, lane_block(o)] = uf[o, pl.ds(pl.multiple_of((r * 4 + edge) * 8, 8), 8), :]
            rim[32 + r * 4 : 36 + r * 4, lane_block(o)] = xf[o, pl.ds((r * 4 + edge) * 4, 4), :]

    width = sums.shape[1] // GROUPS
    row = lax.broadcasted_iota(jnp.int32, (sums.shape[1], LANES), 0)
    first = lax.broadcasted_iota(jnp.int32, (sums.shape[1], LANES), 1) * width
    member = jnp.where((row >= first) & (row < first + width), 1.0, 0.0).astype(BF16)
    grouped = jnp.zeros((32, LANES), F32)
    for part in three_parts(sums[...]):
        grouped = grouped + jnp.dot(part, member, preferred_element_type=F32)
    stats = grouped[0:8]
    for kind in range(1, 4):
        stats = stats + pltpu.roll(grouped[kind * 8 : kind * 8 + 8], GROUPS * kind, axis=1)
    rim[48:56, :] = jnp.zeros((8, rim.shape[1]), F32)
    for index, part in enumerate(three_parts(stats)):
        rim[48:56, lane_block(index)] = part.astype(F32)

    for o in range(blocks):
        main_ref[0:128, lane_block(o)] = uf[o].astype(BF16)
        main_ref[128:192, lane_block(o)] = xf[o].astype(BF16)
    rim_ref[...] = rim[...].astype(BF16)
    for b in range(4):
        finds[b].wait()
        line = table[b, pl.ds(lax.rem(steps[b], 8), 1), :] + shift_ref[...]
        offset_ref[b : b + 1, :] = line
        offset_ref[b + 4 : b + 5, :] = line


def mix_kernel(
    own0, own1, own3, own2a, own2b, other0, other1, other3, other2a, other2b, weight_ref, gain_ref, offset_ref,
    out_ref, ug, xg, picked, lhs_ref, slope_ref, rows_ref, wf, wc, velocity,
):
    blocks = ug.shape[0]
    core = lax.axis_index("gx_1")
    half = lax.axis_index("gx_0")
    chans = own0.shape[1]
    ug[...] = jnp.zeros(ug.shape, F32)
    xg[...] = jnp.zeros(xg.shape, F32)

    def spot(row, col):
        return pl.multiple_of((row * 10 + col) * 8, 8)

    total = jnp.zeros((8, chans), F32)
    rim_here = core == 1 - half
    rim_col = jnp.where(half == 0, 9, 0)
    whole = lambda ref: (ref.at[0:128], ref.at[128:256])
    sources = (
        (0, whole(own0), whole(other0)),
        (1, whole(own1), whole(other1)),
        (3, whole(own3), whole(other3)),
        (2, (own2a, own2b), (other2a, other2b)),
    )
    for back, own_ref, other_ref in sources:
        tile = lax.rem(lax.axis_index("gy") + 4 - back, 4)
        for (upper, lower), base in ((own_ref, 4 * core), (other_ref, 4 * (1 - core))):
            for r in range(4):
                at = spot(4 * tile + r + 1, base + 1)
                lines = upper[r * 32 : r * 32 + 32, :].astype(F32)
                states = lower[r * 16 : r * 16 + 16, :].astype(F32)
                for o in range(blocks):
                    ug[o, pl.ds(at, 32), :] = lines[:, lane_block(o)]
                    for two in range(2):
                        pair = doubled_rows(states[two * 8 : two * 8 + 8, lane_block(o)])
                        xg[o, pl.ds(pl.multiple_of(at + two * 16, 8), 8), :] = pair[0]
                        xg[o, pl.ds(pl.multiple_of(at + two * 16 + 8, 8), 8), :] = pair[1]
        mine = own_ref[1][64:128, :].astype(F32)
        theirs = other_ref[1][64:128, :].astype(F32)
        total = total + mine[48:56] + mine[56:64] + theirs[48:56] + theirs[56:64]
        rim = jnp.where(rim_here, mine[0:48], theirs[0:48])
        for r in range(4):
            at = spot(4 * tile + r + 1, rim_col)
            for o in range(blocks):
                ug[o, pl.ds(at, 8), :] = rim[r * 8 : r * 8 + 8, lane_block(o)]
        for two in range(2):
            for o in range(blocks):
                pair = doubled_rows(rim[32 + two * 8 : 40 + two * 8, lane_block(o)])
                for one in range(2):
                    at = spot(4 * tile + two * 2 + one + 1, rim_col)
                    xg[o, pl.ds(at, 8), :] = pair[one]

    stats = total[:, lane_block(0)] + total[:, lane_block(1)] + total[:, lane_block(2)]
    width = chans // GROUPS
    lane = lax.broadcasted_iota(jnp.int32, (LANES, chans), 1)
    first = lax.broadcasted_iota(jnp.int32, (LANES, chans), 0) * width
    spread = jnp.where((lane >= first) & (lane < first + width), 1.0, 0.0).astype(BF16)

    def expanded(kind):
        turned = stats if kind == 0 else pltpu.roll(stats, LANES - GROUPS * kind, axis=1)
        out = jnp.zeros((8, chans), F32)
        for part in three_parts(turned):
            out = out + jnp.dot(part, spread, preferred_element_type=F32)
        return out

    count = 256 * width
    sum_u, cross, sum_x, sum_xx = (expanded(kind) for kind in range(4))
    mean = sum_x / count
    sigma = jnp.sqrt(sum_xx / count - mean * mean + 1e-05)
    inverse = 1.0 / sigma
    mean_u = sum_u / count
    mean_cu = (cross - mean * sum_u) / count
    bend = mean_cu / (sigma * sigma * sigma)
    offset = offset_ref[...]
    gain = gain_ref[...]

    def fields(x, o):
        at = lane_block(o)
        centered = x - mean[:, at]
        pre = centered * inverse[:, at] * gain[:, at] + offset[:, at]
        sig = 1.0 / (1.0 + jnp.exp(-pre))
        return centered, pre, sig

    def grid_row(gr, carry):
        at = spot(gr + 1, 1)
        for o in range(blocks):
            ln = lane_block(o)
            x = xg[o, pl.ds(at, 64), :].reshape(8, 8, LANES)
            u = ug[o, pl.ds(at, 64), :].reshape(8, 8, LANES)
            centered, pre, sig = fields(x, o)
            xg[o, pl.ds(at, 64), :] = (pre * sig).reshape(64, LANES)
            slope = sig * (1.0 + pre * (1.0 - sig)) * gain[:, ln]
            direction = (u - mean_u[:, ln]) * inverse[:, ln] - centered * bend[:, ln]
            out = (slope * direction).reshape(64, LANES).astype(BF16)
            slope_ref[pl.ds(pl.multiple_of(gr * 64, 64), 64), ln] = out
            edge = spot(gr + 1, rim_col)
            _, pre, sig = fields(xg[o, pl.ds(edge, 8), :], o)
            xg[o, pl.ds(edge, 8), :] = pre * sig
        return carry

    lax.fori_loop(0, 16, grid_row, 0)

    taps = [pair_of(index) for index in range(PAIRS)]

    def lhs_row(gr, carry):
        for index, (tap, ob) in enumerate(taps):
            dy, dx = lax.div(tap, 3), lax.rem(tap, 3)
            at = spot(gr + 2 - dy, 2 - dx)
            value = ug[jnp.minimum(ob, blocks - 1), pl.ds(at, 64), :]
            lhs_ref[pl.ds(pl.multiple_of(gr * 64, 64), 64), lane_block(index)] = value.astype(BF16)
        return carry

    lax.fori_loop(0, 16, lhs_row, 0)

    row = quarter()
    early = lax.broadcasted_iota(jnp.int32, (8, LANES), 0) < 4
    for index, (tap, ob) in enumerate(taps):
        dy, dx = lax.div(tap, 3), lax.rem(tap, 3)
        for target in range(8):
            at = spot(4 * (target // 2) + row + dy, 4 * (target % 2) + dx)
            to = index * 128 + target * 16
            for o in range(blocks):
                for two in range(2):
                    first = xg[o, pl.ds(pl.multiple_of(at + two * 16, 8), 8), :]
                    second = xg[o, pl.ds(pl.multiple_of(at + two * 16 + 8, 8), 8), :]
                    both = jnp.where(early, first, pltpu.roll(second, 4, axis=0))
                    picked[o, to + two * 8 : to + two * 8 + 8, :] = both
    for o in range(blocks):
        rows_ref[:, lane_block(o)] = picked[o].astype(BF16)

    each = weight_ref.shape[1]
    for source in range(weight_ref.shape[0]):
        wf[source * each : (source + 1) * each, :] = weight_ref[source].astype(F32)
    for index in range(PAIRS):
        wc[:, lane_block(index)] = wf[pl.ds(index, chans, stride=PAIRS), :].astype(BF16)

    chunk = 256
    total = jnp.zeros((8, chans), F32)
    for start in range(0, lhs_ref.shape[0], chunk):
        value = lax.dot_general(
            lhs_ref[start : start + chunk, :], wc[...], (((1,), (1,)), ((), ())), preferred_element_type=F32
        )
        value = value * slope_ref[start : start + chunk, :].astype(F32)
        total = total + jnp.sum(value.reshape(chunk // 8, 8, chans), axis=0)
    lanes = total[:, lane_block(0)]
    for o in range(1, blocks):
        lanes = lanes + total[:, lane_block(o)]
    lanes = lanes + pltpu.roll(lanes, 4, axis=0)

    velocity[...] = jnp.zeros(velocity.shape, F32)
    for index in range(PAIRS):
        ob = jnp.minimum(taps[index][1], blocks - 1)
        part = jnp.dot(
            rows_ref[index * 128 : index * 128 + 128, :], wc[:, lane_block(index)], preferred_element_type=F32
        )
        velocity[ob] = velocity[ob] + part
    for target in range(8):
        for o in range(blocks):
            out_ref[target, o * 16 : o * 16 + 16, :] = velocity[o, target * 16 : target * 16 + 16, :]
        out_ref[target, blocks * 16 : blocks * 16 + 8, :] = lanes


def step_kernel(parts_ref, state_ref, bias_ref, rows_ref, mass_ref, lines):
    blocks = bias_ref.shape[1] // LANES
    total = parts_ref[0]
    for source in range(1, 8):
        total = total + parts_ref[source]
    mass = jnp.sum(total[blocks * 16 : blocks * 16 + 8, :], axis=1, keepdims=True)
    lane = lax.broadcasted_iota(jnp.int32, (8, LANES), 1)
    latents = lax.broadcasted_iota(jnp.int32, (8, LANES), 0)
    line = jnp.sum(jnp.where(lane == latents, mass, 0.0), axis=0, keepdims=True)
    mass_ref[...] = jnp.broadcast_to(line, mass_ref.shape)
    row = quarter()
    for b in range(4):
        here = state_ref[b, row].astype(F32)
        for o in range(blocks):
            lines[o, pl.ds(b, 4, stride=4), :] = here[:, lane_block(o)]
    for o in range(blocks):
        value = lines[o] + 0.25 * (total[o * 16 : o * 16 + 16, :] + bias_ref[:, lane_block(o)])
        rows_ref[:, lane_block(o)] = value.astype(BF16)


def final_kernel(scale, mass_ref, rows0, rows1, rows2, rows3, next_ref, out_ref, lines):
    blocks = lines.shape[0]
    total = jnp.sum(mass_ref[...], axis=0, keepdims=True)
    lane = lax.broadcasted_iota(jnp.int32, (1, LANES), 1)
    for b in range(4):
        out_ref[b] = scale * jnp.sum(jnp.where(lane == b, total, 0.0))
    for code, rows in enumerate((rows0, rows1, rows2, rows3)):
        tall, wide = lax.axis_index("probe_0") + code // 2, lax.axis_index("probe_1") + code % 2
        row = 2 * lax.rem(tall, 2) + lax.rem(wide, 2)
        for o in range(blocks):
            lines[o] = rows[:, lane_block(o)].astype(F32)
        for o in range(blocks):
            for b in range(4):
                next_ref[b, row, :, lane_block(o)] = lines[o, pl.ds(b, 4, stride=4), :].astype(BF16)


def shape(dims, kind):
    return jax.ShapeDtypeStruct(dims, kind)


def body(state, probe_signs, timesteps, time_table, gn_gain, gn_shift, conv_weight, conv_bias):
    chans = state.shape[3]
    blocks = chans // LANES
    each = conv_weight.shape[1] * PAIRS
    params = pltpu.CompilerParams(vmem_limit_bytes=40 * 1024 * 1024)
    far = lambda array: pltpu.with_memory_space_constraint(array, pltpu.HBM)
    wsend, main, rim, offset = pl.pallas_call(
        pack_kernel,
        out_shape=(
            shape((32, each, LANES), BF16),
            shape((192, chans), BF16),
            shape((56, chans), BF16),
            shape((8, chans), F32),
        ),
        in_specs=[SMEM] + [HBM] * 4 + [VMEM],
        out_specs=(VMEM,) * 4,
        scratch_shapes=[
            pltpu.VMEM(probe_signs.shape, jnp.int32),
            pltpu.VMEM(state.shape, BF16),
            pltpu.VMEM(conv_weight.shape, BF16),
            pltpu.VMEM((4, 8, chans), F32),
            pltpu.VMEM((blocks, 128, LANES), F32),
            pltpu.VMEM((blocks, 64, LANES), F32),
            pltpu.VMEM((each, LANES), F32),
            pltpu.VMEM((56, chans), F32),
            pltpu.VMEM((32, chans), F32),
            pltpu.SemaphoreType.DMA((3,)),
            pltpu.SemaphoreType.DMA((4,)),
        ],
        compiler_params=params,
        name="pack",
    )(timesteps, far(probe_signs), far(state), far(conv_weight), far(time_table), gn_shift[None])

    across = [(a * 2 + b, (1 - a) * 2 + 1 - b) for a in range(2) for b in range(2)]
    facing = lax.ppermute(rim, GX, across)
    weights = lax.all_to_all(wsend, PROBE, 0, 0, tiled=True)
    block = jnp.concatenate([main, facing, rim[48:56]], axis=0)
    down = [(i, (i + 1) % 4) for i in range(4)]
    up = [(i, (i + 3) % 4) for i in range(4)]
    above = lax.ppermute(block, "gy", down)
    below = lax.ppermute(block, "gy", up)
    upper = lax.ppermute(above[:128], "gy", down)
    lower = lax.ppermute(below[128:], "gy", up)
    own = [block, above, below, upper, lower]
    other = [lax.ppermute(tile, "gx_1", [(0, 1), (1, 0)]) for tile in own]

    partial = pl.pallas_call(
        mix_kernel,
        out_shape=shape((8, blocks * 16 + 8, LANES), F32),
        in_specs=[VMEM] * 13,
        out_specs=VMEM,
        scratch_shapes=[
            pltpu.VMEM((blocks, 1440, LANES), F32),
            pltpu.VMEM((blocks, 1440, LANES), F32),
            pltpu.VMEM((blocks, PAIRS * 128, LANES), F32),
            pltpu.VMEM((1024, PAIRS * LANES), BF16),
            pltpu.VMEM((1024, chans), BF16),
            pltpu.VMEM((PAIRS * 128, chans), BF16),
            pltpu.VMEM((32 * each, LANES), F32),
            pltpu.VMEM((chans, PAIRS * LANES), BF16),
            pltpu.VMEM((blocks, 128, LANES), F32),
        ],
        compiler_params=params,
        name="mix",
    )(*own, *other, weights, gn_gain[None], offset)

    partial = lax.all_to_all(partial, ("gy", "gx_1"), 0, 0, tiled=True)
    rows, mass = pl.pallas_call(
        step_kernel,
        out_shape=(shape((16, chans), BF16), shape((64, LANES), F32)),
        in_specs=[VMEM] * 3,
        out_specs=(VMEM,) * 2,
        scratch_shapes=[pltpu.VMEM((blocks, 16, LANES), F32)],
        compiler_params=params,
        name="step",
    )(partial, state, conv_bias[None])
    mass = lax.all_to_all(mass.reshape(64, 1, LANES), ("gx_0",) + PROBE, 0, 0, tiled=True)
    quarters = [rows]
    tall, wide = lax.axis_size("probe_0"), lax.axis_size("probe_1")
    for code in (1, 2, 3):
        swap = [(y * wide + z, (y ^ (code // 2)) * wide + (z ^ (code % 2))) for y in range(tall) for z in range(wide)]
        quarters.append(lax.ppermute(rows, PROBE, swap))
    scale = -0.25 / (probe_signs.shape[0] * lax.axis_size(PROBE))
    return pl.pallas_call(
        lambda *refs: final_kernel(scale, *refs),
        out_shape=(shape(state.shape, BF16), shape((4,), F32)),
        in_specs=[VMEM] * 5,
        out_specs=(VMEM, SMEM),
        scratch_shapes=[pltpu.VMEM((blocks, 16, LANES), F32)],
        compiler_params=params,
        name="final",
    )(mass.reshape(64, LANES), *quarters)


def solution(mesh):
    split = Mesh(
        mesh.devices.reshape(mesh.shape["gy"], 2, 2, 8, 4),
        ("gy", "gx_0", "gx_1", "probe_0", "probe_1"),
    )
    return jax.shard_map(
        body,
        mesh=split,
        in_specs=(
            P(None, "gy", GX, None),
            P(PROBE, None, "gy", GX, None),
            P(),
            P(),
            P(),
            P(),
            P(None, PROBE, None),
            P(),
        ),
        out_specs=(P(None, "gy", GX, None), P()),
        check_vma=False,
    )
```

```python
import jax
import jax.numpy as jnp
from jax import lax
from jax.experimental import pallas as pl
from jax.experimental.pallas import tpu as pltpu
from jax.sharding import Mesh
from jax.sharding import PartitionSpec as P


GROUPS = 32
GX = ("gx_0", "gx_1")
PROBE = ("probe_0", "probe_1")
LANES = 128
PAIRS = 6
F32 = jnp.float32
BF16 = jnp.bfloat16
VMEM = pl.BlockSpec(memory_space=pltpu.VMEM)
SMEM = pl.BlockSpec(memory_space=pltpu.SMEM)
HBM = pl.BlockSpec(memory_space=pltpu.HBM)


def three_parts(value):
    high = value.astype(BF16)
    rest = value - high.astype(F32)
    mid = rest.astype(BF16)
    low = (rest - mid.astype(F32)).astype(BF16)
    return high, mid, low


def lane_block(index):
    return slice(index * LANES, (index + 1) * LANES)


def doubled_rows(rows):
    turned = pltpu.roll(rows, 4, axis=0)
    upper = lax.broadcasted_iota(jnp.int32, rows.shape, 0) < 4
    return jnp.where(upper, rows, turned), jnp.where(upper, turned, rows)


def half_rows():
    return 2 * lax.rem(lax.axis_index("probe_0"), 2)


def first_block(member):
    return member * PAIRS // 9


def pair_of(index):
    member = lax.axis_index("gy") * 2 + lax.axis_index("gx_1")
    number = member * PAIRS + index
    return lax.rem(number, 9), lax.div(number, 9)


def spread_kernel(weight_ref, wsend_ref, wf):
    for index in range(PAIRS):
        tap, ob = pair_of(index)
        rows = weight_ref[tap].astype(F32)
        picked = jnp.zeros((rows.shape[0], LANES), F32)
        for o in range(rows.shape[1] // LANES):
            picked = picked + jnp.where(ob == o, rows[:, lane_block(o)], 0.0)
        wf[pl.ds(index, rows.shape[0], stride=PAIRS), :] = picked
    packed = wf[...].astype(BF16)
    for target in range(wsend_ref.shape[0]):
        wsend_ref[target] = packed


def lookup_kernel(step_ref, table_hbm, shift_ref, offset_ref, table, found):
    steps = [step_ref[b] for b in range(4)]
    finds = [
        pltpu.make_async_copy(
            table_hbm.at[pl.ds(pl.multiple_of(lax.div(steps[b], 8) * 8, 8), 8), :], table.at[b], found.at[b]
        )
        for b in range(4)
    ]
    for find in finds:
        find.start()
    for b in range(4):
        finds[b].wait()
        line = table[b, pl.ds(lax.rem(steps[b], 8), 1), :] + shift_ref[...]
        offset_ref[b : b + 1, :] = line
        offset_ref[b + 4 : b + 5, :] = line


def pack_kernel(signs_hbm, state_hbm, main_ref, rim_ref, signs_ref, state_ref, uf, xf, rim, sums, arrived):
    blocks = uf.shape[0]
    loads = [
        pltpu.make_async_copy(src, dst, arrived.at[index])
        for index, (src, dst) in enumerate(((signs_hbm, signs_ref), (state_hbm, state_ref)))
    ]
    for load in loads:
        load.start()
    for load in loads:
        load.wait()
    for p in range(2):
        for b in range(4):
            for r in range(4):
                line = signs_ref[p, b, r].astype(F32)
                for o in range(blocks):
                    uf[o, pl.ds(r * 32 + p * 4 + b, 4, stride=8), :] = line[:, lane_block(o)]
    for b in range(4):
        for r in range(4):
            line = state_ref[b, r].astype(F32)
            for o in range(blocks):
                xf[o, pl.ds(r * 16 + b, 4, stride=4), :] = line[:, lane_block(o)]

    edge = jnp.where(lax.axis_index("gx_0") == 0, 3, 0)
    for o in range(blocks):
        sum_u = jnp.zeros((8, LANES), F32)
        cross = jnp.zeros((8, LANES), F32)
        sum_x = jnp.zeros((8, LANES), F32)
        sum_xx = jnp.zeros((8, LANES), F32)
        for two in range(8):
            pair = doubled_rows(xf[o, two * 8 : two * 8 + 8, :])
            for half in range(2):
                cell = two * 2 + half
                x = pair[half]
                u = uf[o, cell * 8 : cell * 8 + 8, :]
                sum_u, cross = sum_u + u, cross + u * x
                sum_x, sum_xx = sum_x + x, sum_xx + x * x
        for kind, part in enumerate((sum_u, cross, sum_x, sum_xx)):
            sums[kind * 8 : kind * 8 + 8, lane_block(o)] = part
        for r in range(4):
            rim[r * 8 : r * 8 + 8, lane_block(o)] = uf[o, pl.ds(pl.multiple_of((r * 4 + edge) * 8, 8), 8), :]
            rim[32 + r * 4 : 36 + r * 4, lane_block(o)] = xf[o, pl.ds((r * 4 + edge) * 4, 4), :]

    width = sums.shape[1] // GROUPS
    row = lax.broadcasted_iota(jnp.int32, (sums.shape[1], LANES), 0)
    first = lax.broadcasted_iota(jnp.int32, (sums.shape[1], LANES), 1) * width
    member = jnp.where((row >= first) & (row < first + width), 1.0, 0.0).astype(BF16)
    grouped = jnp.zeros((32, LANES), F32)
    for part in three_parts(sums[...]):
        grouped = grouped + jnp.dot(part, member, preferred_element_type=F32)
    stats = grouped[0:8]
    for kind in range(1, 4):
        stats = stats + pltpu.roll(grouped[kind * 8 : kind * 8 + 8], GROUPS * kind, axis=1)
    rim[48:56, :] = jnp.zeros((8, rim.shape[1]), F32)
    for index, part in enumerate(three_parts(stats)):
        rim[48:56, lane_block(index)] = part.astype(F32)

    for o in range(blocks):
        main_ref[0:128, lane_block(o)] = uf[o].astype(BF16)
        main_ref[128:192, lane_block(o)] = xf[o].astype(BF16)
    rim_ref[...] = rim[...].astype(BF16)


def mix_kernel(
    own0, own1, own3, own2, other0, other1, other3, other2, weight_hbm, gain_ref, offset_ref,
    out_ref, ug, xg, picked, lhs_ref, slope_ref, rows_ref, weight_ref, wf, wc, velocity, arrived,
):
    load = pltpu.make_async_copy(weight_hbm, weight_ref, arrived)
    load.start()
    blocks = ug.shape[0]
    core = lax.axis_index("gx_1")
    half = lax.axis_index("gx_0")
    chans = own0.shape[1]
    ug[...] = jnp.zeros(ug.shape, F32)
    xg[...] = jnp.zeros(xg.shape, F32)

    def spot(row, col):
        return pl.multiple_of((row * 10 + col) * 8, 8)

    total = jnp.zeros((8, chans), F32)
    rim_here = core == 1 - half
    rim_col = jnp.where(half == 0, 9, 0)
    sources = ((0, own0, other0), (1, own1, other1), (3, own3, other3), (2, own2, other2))
    for back, own_ref, other_ref in sources:
        tile = lax.rem(lax.axis_index("gy") + 4 - back, 4)
        for src, base in ((own_ref, 4 * core), (other_ref, 4 * (1 - core))):
            for r in range(4):
                at = spot(4 * tile + r + 1, base + 1)
                lines = src[r * 32 : r * 32 + 32, :].astype(F32)
                states = src[128 + r * 16 : 144 + r * 16, :].astype(F32)
                for o in range(blocks):
                    ug[o, pl.ds(at, 32), :] = lines[:, lane_block(o)]
                    for two in range(2):
                        pair = doubled_rows(states[two * 8 : two * 8 + 8, lane_block(o)])
                        xg[o, pl.ds(pl.multiple_of(at + two * 16, 8), 8), :] = pair[0]
                        xg[o, pl.ds(pl.multiple_of(at + two * 16 + 8, 8), 8), :] = pair[1]
        mine = own_ref[192:256, :].astype(F32)
        theirs = other_ref[192:256, :].astype(F32)
        total = total + mine[48:56] + mine[56:64] + theirs[48:56] + theirs[56:64]
        rim = jnp.where(rim_here, mine[0:48], theirs[0:48])
        for r in range(4):
            at = spot(4 * tile + r + 1, rim_col)
            for o in range(blocks):
                ug[o, pl.ds(at, 8), :] = rim[r * 8 : r * 8 + 8, lane_block(o)]
        for two in range(2):
            for o in range(blocks):
                pair = doubled_rows(rim[32 + two * 8 : 40 + two * 8, lane_block(o)])
                for one in range(2):
                    at = spot(4 * tile + two * 2 + one + 1, rim_col)
                    xg[o, pl.ds(at, 8), :] = pair[one]

    stats = total[:, lane_block(0)] + total[:, lane_block(1)] + total[:, lane_block(2)]
    width = chans // GROUPS
    lane = lax.broadcasted_iota(jnp.int32, (LANES, chans), 1)
    first = lax.broadcasted_iota(jnp.int32, (LANES, chans), 0) * width
    spread = jnp.where((lane >= first) & (lane < first + width), 1.0, 0.0).astype(BF16)

    def expanded(kind):
        turned = stats if kind == 0 else pltpu.roll(stats, LANES - GROUPS * kind, axis=1)
        out = jnp.zeros((8, chans), F32)
        for part in three_parts(turned):
            out = out + jnp.dot(part, spread, preferred_element_type=F32)
        return out

    count = 256 * width
    sum_u, cross, sum_x, sum_xx = (expanded(kind) for kind in range(4))
    mean = sum_x / count
    sigma = jnp.sqrt(sum_xx / count - mean * mean + 1e-05)
    inverse = 1.0 / sigma
    mean_u = sum_u / count
    mean_cu = (cross - mean * sum_u) / count
    bend = mean_cu / (sigma * sigma * sigma)
    offset = offset_ref[...]
    gain = gain_ref[...]

    def fields(x, o):
        at = lane_block(o)
        centered = x - mean[:, at]
        pre = centered * inverse[:, at] * gain[:, at] + offset[:, at]
        sig = 1.0 / (1.0 + jnp.exp(-pre))
        return centered, pre, sig

    def grid_row(gr, carry):
        at = spot(gr + 1, 1)
        for o in range(blocks):
            ln = lane_block(o)
            x = xg[o, pl.ds(at, 64), :].reshape(8, 8, LANES)
            u = ug[o, pl.ds(at, 64), :].reshape(8, 8, LANES)
            centered, pre, sig = fields(x, o)
            xg[o, pl.ds(at, 64), :] = (pre * sig).reshape(64, LANES)
            slope = sig * (1.0 + pre * (1.0 - sig)) * gain[:, ln]
            direction = (u - mean_u[:, ln]) * inverse[:, ln] - centered * bend[:, ln]
            out = (slope * direction).reshape(64, LANES).astype(BF16)
            slope_ref[pl.ds(pl.multiple_of(gr * 64, 64), 64), ln] = out
            edge = spot(gr + 1, rim_col)
            _, pre, sig = fields(xg[o, pl.ds(edge, 8), :], o)
            xg[o, pl.ds(edge, 8), :] = pre * sig
        return carry

    lax.fori_loop(0, 16, grid_row, 0)

    taps = [pair_of(index) for index in range(PAIRS)]

    def lhs_row(gr, carry):
        for index, (tap, ob) in enumerate(taps):
            dy, dx = lax.div(tap, 3), lax.rem(tap, 3)
            at = spot(gr + 2 - dy, 2 - dx)
            value = ug[jnp.minimum(ob, blocks - 1), pl.ds(at, 64), :]
            lhs_ref[pl.ds(pl.multiple_of(gr * 64, 64), 64), lane_block(index)] = value.astype(BF16)
        return carry

    lax.fori_loop(0, 16, lhs_row, 0)

    early = lax.broadcasted_iota(jnp.int32, (8, LANES), 0) < 4
    for index, (tap, ob) in enumerate(taps):
        dy, dx = lax.div(tap, 3), lax.rem(tap, 3)
        for target in range(8):
            for line in range(2):
                at = spot(4 * (target // 2) + half_rows() + line + dy, 4 * (target % 2) + dx)
                to = index * 256 + target * 32 + line * 16
                for o in range(blocks):
                    for two in range(2):
                        first = xg[o, pl.ds(pl.multiple_of(at + two * 16, 8), 8), :]
                        second = xg[o, pl.ds(pl.multiple_of(at + two * 16 + 8, 8), 8), :]
                        both = jnp.where(early, first, pltpu.roll(second, 4, axis=0))
                        picked[o, to + two * 8 : to + two * 8 + 8, :] = both
    for o in range(blocks):
        rows_ref[:, lane_block(o)] = picked[o].astype(BF16)

    load.wait()
    each = weight_ref.shape[1]
    for source in range(weight_ref.shape[0]):
        wf[source * each : (source + 1) * each, :] = weight_ref[source].astype(F32)
    for index in range(PAIRS):
        wc[:, lane_block(index)] = wf[pl.ds(index, chans, stride=PAIRS), :].astype(BF16)

    chunk = 256
    total = jnp.zeros((8, chans), F32)
    for start in range(0, lhs_ref.shape[0], chunk):
        value = lax.dot_general(
            lhs_ref[start : start + chunk, :], wc[...], (((1,), (1,)), ((), ())), preferred_element_type=F32
        )
        value = value * slope_ref[start : start + chunk, :].astype(F32)
        total = total + jnp.sum(value.reshape(chunk // 8, 8, chans), axis=0)
    lanes = total[:, lane_block(0)]
    for o in range(1, blocks):
        lanes = lanes + total[:, lane_block(o)]
    lanes = lanes + pltpu.roll(lanes, 4, axis=0)

    velocity[...] = jnp.zeros(velocity.shape, F32)
    for index in range(PAIRS):
        slot = taps[index][1] - lax.div((lax.axis_index("gy") * 2 + lax.axis_index("gx_1")) * PAIRS, 9)
        part = jnp.dot(
            rows_ref[index * 256 : index * 256 + 256, :], wc[:, lane_block(index)], preferred_element_type=F32
        )
        velocity[slot] = velocity[slot] + part
    for target in range(8):
        for slot in range(2):
            out_ref[target, slot * 32 : slot * 32 + 32, :] = velocity[slot, target * 32 : target * 32 + 32, :]
        out_ref[target, 64:72, :] = lanes


def step_kernel(parts_ref, state_ref, bias_ref, rows_ref, mass_ref, lines):
    blocks = bias_ref.shape[1] // LANES
    total = parts_ref[0, 64:72, :]
    for source in range(1, 8):
        total = total + parts_ref[source, 64:72, :]
    mass = jnp.sum(total, axis=1, keepdims=True)
    lane = lax.broadcasted_iota(jnp.int32, (8, LANES), 1)
    latents = lax.broadcasted_iota(jnp.int32, (8, LANES), 0)
    line = jnp.sum(jnp.where(lane == latents, mass, 0.0), axis=0, keepdims=True)
    mass_ref[...] = jnp.broadcast_to(line, mass_ref.shape)
    for b in range(4):
        for r in range(2):
            here = state_ref[b, half_rows() + r].astype(F32)
            for o in range(blocks):
                lines[o, pl.ds(r * 16 + b, 4, stride=4), :] = here[:, lane_block(o)]
    velocity = [jnp.broadcast_to(bias_ref[:, lane_block(o)], (32, LANES)) for o in range(blocks)]
    for source in range(8):
        for slot in range(2):
            o = first_block(source) + slot
            if o < blocks:
                velocity[o] = velocity[o] + parts_ref[source, slot * 32 : slot * 32 + 32, :]
    for o in range(blocks):
        rows_ref[:, lane_block(o)] = (lines[o] + 0.25 * velocity[o]).astype(BF16)


def final_kernel(scale, mass_ref, rows0, rows1, next_ref, out_ref, lines):
    blocks = lines.shape[0]
    total = jnp.sum(mass_ref[...], axis=0, keepdims=True)
    lane = lax.broadcasted_iota(jnp.int32, (1, LANES), 1)
    for b in range(4):
        out_ref[b] = scale * jnp.sum(jnp.where(lane == b, total, 0.0))
    for start, rows in ((half_rows(), rows0), (2 - half_rows(), rows1)):
        for o in range(blocks):
            lines[o] = rows[:, lane_block(o)].astype(F32)
        for o in range(blocks):
            for b in range(4):
                for r in range(2):
                    value = lines[o, pl.ds(r * 16 + b, 4, stride=4), :].astype(BF16)
                    next_ref[b, start + r, :, lane_block(o)] = value


def shape(dims, kind):
    return jax.ShapeDtypeStruct(dims, kind)


def body(state, probe_signs, timesteps, time_table, gn_gain, gn_shift, conv_weight, conv_bias):
    chans = state.shape[3]
    blocks = chans // LANES
    each = conv_weight.shape[1] * PAIRS
    params = pltpu.CompilerParams(vmem_limit_bytes=40 * 1024 * 1024)
    far = lambda array: pltpu.with_memory_space_constraint(array, pltpu.HBM)
    main, rim = pl.pallas_call(
        pack_kernel,
        out_shape=(shape((192, chans), BF16), shape((56, chans), BF16)),
        in_specs=[HBM] * 2,
        out_specs=(VMEM,) * 2,
        scratch_shapes=[
            pltpu.VMEM(probe_signs.shape, jnp.int32),
            pltpu.VMEM(state.shape, BF16),
            pltpu.VMEM((blocks, 128, LANES), F32),
            pltpu.VMEM((blocks, 64, LANES), F32),
            pltpu.VMEM((56, chans), F32),
            pltpu.VMEM((32, chans), F32),
            pltpu.SemaphoreType.DMA((2,)),
        ],
        compiler_params=params,
        name="pack",
    )(far(probe_signs), far(state))
    wsend = pl.pallas_call(
        spread_kernel,
        out_shape=shape((32, each, LANES), BF16),
        in_specs=[VMEM],
        out_specs=VMEM,
        scratch_shapes=[pltpu.VMEM((each, LANES), F32)],
        compiler_params=params,
        name="deal",
    )(conv_weight)
    offset = pl.pallas_call(
        lookup_kernel,
        out_shape=shape((8, chans), F32),
        in_specs=[SMEM, HBM, VMEM],
        out_specs=VMEM,
        scratch_shapes=[pltpu.VMEM((4, 8, chans), F32), pltpu.SemaphoreType.DMA((4,))],
        compiler_params=params,
        name="lookup",
    )(timesteps, far(time_table), gn_shift[None])

    across = [(a * 2 + b, (1 - a) * 2 + 1 - b) for a in range(2) for b in range(2)]
    facing = lax.ppermute(rim, GX, across)
    weights = lax.all_to_all(wsend, PROBE, 0, 0, tiled=True)
    block = jnp.concatenate([main, facing, rim[48:56]], axis=0)
    down = [(i, (i + 1) % 4) for i in range(4)]
    up = [(i, (i + 3) % 4) for i in range(4)]
    above = lax.ppermute(block, "gy", down)
    below = lax.ppermute(block, "gy", up)
    onward = [(x * 2 + c, (x + 1 - 2 * c) % 4 * 2 + c) for x in range(4) for c in range(2)]
    beyond = lax.ppermute(jnp.where(lax.axis_index("gx_1") == 0, above, below), ("gy", "gx_1"), onward)
    own = [block, above, below, beyond]
    other = [lax.ppermute(tile, "gx_1", [(0, 1), (1, 0)]) for tile in own]

    partial = pl.pallas_call(
        mix_kernel,
        out_shape=shape((8, 72, LANES), F32),
        in_specs=[VMEM] * 8 + [HBM] + [VMEM] * 2,
        out_specs=VMEM,
        scratch_shapes=[
            pltpu.VMEM((blocks, 1440, LANES), F32),
            pltpu.VMEM((blocks, 1440, LANES), F32),
            pltpu.VMEM((blocks, PAIRS * 256, LANES), F32),
            pltpu.VMEM((1024, PAIRS * LANES), BF16),
            pltpu.VMEM((1024, chans), BF16),
            pltpu.VMEM((PAIRS * 256, chans), BF16),
            pltpu.VMEM((32, each, LANES), BF16),
            pltpu.VMEM((32 * each, LANES), F32),
            pltpu.VMEM((chans, PAIRS * LANES), BF16),
            pltpu.VMEM((2, 256, LANES), F32),
            pltpu.SemaphoreType.DMA,
        ],
        compiler_params=params,
        name="mix",
    )(*own, *other, far(weights), gn_gain[None], offset)

    partial = lax.all_to_all(partial, ("gy", "gx_1"), 0, 0, tiled=True)
    rows, mass = pl.pallas_call(
        step_kernel,
        out_shape=(shape((32, chans), BF16), shape((64, LANES), F32)),
        in_specs=[VMEM] * 3,
        out_specs=(VMEM,) * 2,
        scratch_shapes=[pltpu.VMEM((blocks, 32, LANES), F32)],
        compiler_params=params,
        name="step",
    )(partial, state, conv_bias[None])
    mass = lax.all_to_all(mass.reshape(64, 1, LANES), ("gx_0",) + PROBE, 0, 0, tiled=True)
    tall = lax.axis_size("probe_0")
    facing_rows = lax.ppermute(rows, "probe_0", [(y, y ^ 1) for y in range(tall)])
    scale = -0.25 / (probe_signs.shape[0] * lax.axis_size(PROBE))
    return pl.pallas_call(
        lambda *refs: final_kernel(scale, *refs),
        out_shape=(shape(state.shape, BF16), shape((4,), F32)),
        in_specs=[VMEM] * 3,
        out_specs=(VMEM, SMEM),
        scratch_shapes=[pltpu.VMEM((blocks, 32, LANES), F32)],
        compiler_params=params,
        name="final",
    )(mass.reshape(64, LANES), rows, facing_rows)


def solution(mesh):
    split = Mesh(
        mesh.devices.reshape(mesh.shape["gy"], 2, 2, 8, 4),
        ("gy", "gx_0", "gx_1", "probe_0", "probe_1"),
    )
    return jax.shard_map(
        body,
        mesh=split,
        in_specs=(
            P(None, "gy", GX, None),
            P(PROBE, None, "gy", GX, None),
            P(),
            P(),
            P(),
            P(),
            P(None, PROBE, None),
            P(),
        ),
        out_specs=(P(None, "gy", GX, None), P()),
        check_vma=False,
    )
```

```python
import jax
import jax.numpy as jnp
from jax import lax
from jax.experimental import pallas as pl
from jax.experimental.pallas import tpu as pltpu
from jax.sharding import Mesh
from jax.sharding import PartitionSpec as P


GROUPS = 32
GX = ("gx_0", "gx_1")
PROBE = ("probe_0", "probe_1")
LANES = 128
PAIRS = 6
F32 = jnp.float32
BF16 = jnp.bfloat16
VMEM = pl.BlockSpec(memory_space=pltpu.VMEM)
SMEM = pl.BlockSpec(memory_space=pltpu.SMEM)
HBM = pl.BlockSpec(memory_space=pltpu.HBM)


def three_parts(value):
    high = value.astype(BF16)
    rest = value - high.astype(F32)
    mid = rest.astype(BF16)
    low = (rest - mid.astype(F32)).astype(BF16)
    return high, mid, low


def lane_block(index):
    return slice(index * LANES, (index + 1) * LANES)


def doubled_rows(rows):
    turned = pltpu.roll(rows, 4, axis=0)
    upper = lax.broadcasted_iota(jnp.int32, rows.shape, 0) < 4
    return jnp.where(upper, rows, turned), jnp.where(upper, turned, rows)


def half_rows():
    return 2 * lax.rem(lax.axis_index("probe_0"), 2)


def first_block(member):
    return member * PAIRS // 9


def pair_of(index):
    member = lax.axis_index("gy") * 2 + lax.axis_index("gx_1")
    number = member * PAIRS + index
    return lax.rem(number, 9), lax.div(number, 9)


def spread_kernel(weight_ref, wsend_ref, wf):
    for index in range(PAIRS):
        tap, ob = pair_of(index)
        rows = weight_ref[tap].astype(F32)
        picked = jnp.zeros((rows.shape[0], LANES), F32)
        for o in range(rows.shape[1] // LANES):
            picked = picked + jnp.where(ob == o, rows[:, lane_block(o)], 0.0)
        wf[pl.ds(index, rows.shape[0], stride=PAIRS), :] = picked
    packed = wf[...].astype(BF16)
    for target in range(wsend_ref.shape[0]):
        wsend_ref[target] = packed


def lookup_kernel(step_ref, table_hbm, shift_ref, bias_ref, base_ref, offset_ref, start_ref, table, found):
    steps = [step_ref[b] for b in range(4)]
    finds = [
        pltpu.make_async_copy(
            table_hbm.at[pl.ds(pl.multiple_of(lax.div(steps[b], 8) * 8, 8), 8), :], table.at[b], found.at[b]
        )
        for b in range(4)
    ]
    for find in finds:
        find.start()
    start_ref[...] = base_ref[...] + 0.25 * bias_ref[...]
    for b in range(4):
        finds[b].wait()
        line = table[b, pl.ds(lax.rem(steps[b], 8), 1), :] + shift_ref[...]
        offset_ref[b : b + 1, :] = line
        offset_ref[b + 4 : b + 5, :] = line


def pack_kernel(signs_hbm, state_hbm, main_ref, rim_ref, base_ref, signs_ref, state_ref, uf, xf, rim, sums, arrived):
    blocks = uf.shape[0]
    loads = [
        pltpu.make_async_copy(src, dst, arrived.at[index])
        for index, (src, dst) in enumerate(((signs_hbm, signs_ref), (state_hbm, state_ref)))
    ]
    for load in loads:
        load.start()
    for load in loads:
        load.wait()
    for p in range(2):
        for b in range(4):
            for r in range(4):
                line = signs_ref[p, b, r].astype(F32)
                for o in range(blocks):
                    uf[o, pl.ds(r * 32 + p * 4 + b, 4, stride=8), :] = line[:, lane_block(o)]
    for b in range(4):
        for r in range(4):
            line = state_ref[b, r].astype(F32)
            for o in range(blocks):
                xf[o, pl.ds(r * 16 + b, 4, stride=4), :] = line[:, lane_block(o)]

    for o in range(blocks):
        base_ref[:, lane_block(o)] = xf[o, pl.ds(pl.multiple_of(half_rows() * 16, 8), 32), :]
    edge = jnp.where(lax.axis_index("gx_0") == 0, 3, 0)
    for o in range(blocks):
        sum_u = jnp.zeros((8, LANES), F32)
        cross = jnp.zeros((8, LANES), F32)
        sum_x = jnp.zeros((8, LANES), F32)
        sum_xx = jnp.zeros((8, LANES), F32)
        for two in range(8):
            pair = doubled_rows(xf[o, two * 8 : two * 8 + 8, :])
            for half in range(2):
                cell = two * 2 + half
                x = pair[half]
                u = uf[o, cell * 8 : cell * 8 + 8, :]
                sum_u, cross = sum_u + u, cross + u * x
                sum_x, sum_xx = sum_x + x, sum_xx + x * x
        for kind, part in enumerate((sum_u, cross, sum_x, sum_xx)):
            sums[kind * 8 : kind * 8 + 8, lane_block(o)] = part
        for r in range(4):
            rim[r * 8 : r * 8 + 8, lane_block(o)] = uf[o, pl.ds(pl.multiple_of((r * 4 + edge) * 8, 8), 8), :]
            rim[32 + r * 4 : 36 + r * 4, lane_block(o)] = xf[o, pl.ds((r * 4 + edge) * 4, 4), :]

    width = sums.shape[1] // GROUPS
    row = lax.broadcasted_iota(jnp.int32, (sums.shape[1], LANES), 0)
    first = lax.broadcasted_iota(jnp.int32, (sums.shape[1], LANES), 1) * width
    member = jnp.where((row >= first) & (row < first + width), 1.0, 0.0).astype(BF16)
    grouped = jnp.zeros((32, LANES), F32)
    for part in three_parts(sums[...]):
        grouped = grouped + jnp.dot(part, member, preferred_element_type=F32)
    stats = grouped[0:8]
    for kind in range(1, 4):
        stats = stats + pltpu.roll(grouped[kind * 8 : kind * 8 + 8], GROUPS * kind, axis=1)
    rim[48:56, :] = jnp.zeros((8, rim.shape[1]), F32)
    for index, part in enumerate(three_parts(stats)):
        rim[48:56, lane_block(index)] = part.astype(F32)

    for o in range(blocks):
        main_ref[0:128, lane_block(o)] = uf[o].astype(BF16)
        main_ref[128:192, lane_block(o)] = xf[o].astype(BF16)
    rim_ref[...] = rim[...].astype(BF16)


def mix_kernel(
    own0, own1, own3, own2, other0, other1, other3, other2, weight_hbm, gain_ref, offset_ref,
    out_ref, ug, xg, lhs_ref, slope_ref, rows_ref, weight_ref, wf, wc, velocity, arrived,
):
    load = pltpu.make_async_copy(weight_hbm, weight_ref, arrived)
    load.start()
    blocks = ug.shape[0]
    core = lax.axis_index("gx_1")
    half = lax.axis_index("gx_0")
    chans = own0.shape[1]

    def spot(row, col):
        return pl.multiple_of((row * 10 + col) * 8, 8)

    def small(row, col):
        return pl.multiple_of((row * 10 + col) * 4, 4)

    for o in range(blocks):
        for row in (0, 17):
            ug[o, row * 80 : row * 80 + 80, :] = jnp.zeros((80, LANES), F32)
            xg[o, row * 40 : row * 40 + 40, :] = jnp.zeros((40, LANES), F32)
        for row in range(1, 17):
            for col in (0, 9):
                ug[o, row * 80 + col * 8 : row * 80 + col * 8 + 8, :] = jnp.zeros((8, LANES), F32)
                xg[o, row * 40 + col * 4 : row * 40 + col * 4 + 4, :] = jnp.zeros((4, LANES), F32)

    total = jnp.zeros((8, chans), F32)
    rim_here = core == 1 - half
    rim_col = jnp.where(half == 0, 9, 0)
    sources = ((0, own0, other0), (1, own1, other1), (3, own3, other3), (2, own2, other2))
    for back, own_ref, other_ref in sources:
        tile = lax.rem(lax.axis_index("gy") + 4 - back, 4)
        for src, base in ((own_ref, 4 * core), (other_ref, 4 * (1 - core))):
            for r in range(4):
                at = spot(4 * tile + r + 1, base + 1)
                lines = src[r * 32 : r * 32 + 32, :].astype(F32)
                states = src[128 + r * 16 : 144 + r * 16, :].astype(F32)
                for o in range(blocks):
                    ug[o, pl.ds(at, 32), :] = lines[:, lane_block(o)]
                    xg[o, pl.ds(small(4 * tile + r + 1, base + 1), 16), :] = states[:, lane_block(o)]
        mine = own_ref[192:256, :].astype(F32)
        theirs = other_ref[192:256, :].astype(F32)
        total = total + mine[48:56] + mine[56:64] + theirs[48:56] + theirs[56:64]
        rim = jnp.where(rim_here, mine[0:48], theirs[0:48])
        for r in range(4):
            at = spot(4 * tile + r + 1, rim_col)
            for o in range(blocks):
                ug[o, pl.ds(at, 8), :] = rim[r * 8 : r * 8 + 8, lane_block(o)]
                xg[o, pl.ds(small(4 * tile + r + 1, rim_col), 4), :] = rim[32 + r * 4 : 36 + r * 4, lane_block(o)]

    stats = total[:, lane_block(0)] + total[:, lane_block(1)] + total[:, lane_block(2)]
    width = chans // GROUPS
    lane = lax.broadcasted_iota(jnp.int32, (LANES, chans), 1)
    first = lax.broadcasted_iota(jnp.int32, (LANES, chans), 0) * width
    spread = jnp.where((lane >= first) & (lane < first + width), 1.0, 0.0).astype(BF16)

    def expanded(kind):
        turned = stats if kind == 0 else pltpu.roll(stats, LANES - GROUPS * kind, axis=1)
        out = jnp.zeros((8, chans), F32)
        for part in three_parts(turned):
            out = out + jnp.dot(part, spread, preferred_element_type=F32)
        return out

    count = 256 * width
    sum_u, cross, sum_x, sum_xx = (expanded(kind) for kind in range(4))
    mean = sum_x / count
    sigma = jnp.sqrt(sum_xx / count - mean * mean + 1e-05)
    inverse = 1.0 / sigma
    mean_u = sum_u / count
    mean_cu = (cross - mean * sum_u) / count
    bend = mean_cu / (sigma * sigma * sigma)
    offset = offset_ref[...]
    gain = gain_ref[...]

    scale = inverse * gain
    tilt = gain * inverse

    def fields(x, o, rows):
        at = lane_block(o)
        centered = x - mean[:rows, at]
        pre = centered * scale[:rows, at] + offset[:rows, at]
        sig = 1.0 / (1.0 + jnp.exp(-pre))
        return centered, pre, sig

    def grid_row(gr, carry):
        at = spot(gr + 1, 1)
        near = small(gr + 1, 1)
        edge = small(gr + 1, rim_col)
        for o in range(blocks):
            ln = lane_block(o)
            x = xg[o, pl.ds(near, 32), :].reshape(4, 8, LANES)
            centered, pre, sig = fields(x, o, 8)
            xg[o, pl.ds(near, 32), :] = (pre * sig).reshape(32, LANES)
            slope = sig * (1.0 + pre * (1.0 - sig))
            along = slope * tilt[:, ln]
            across = slope * gain[:, ln] * centered
            for two in range(4):
                spans = zip(doubled_rows(along[two]), doubled_rows(across[two]))
                for half_cell, (first, second) in enumerate(spans):
                    cell = two * 2 + half_cell
                    u = ug[o, pl.ds(pl.multiple_of(at + cell * 8, 8), 8), :]
                    out = first * (u - mean_u[:, ln]) - second * bend[:, ln]
                    slope_ref[pl.ds(pl.multiple_of(gr * 64 + cell * 8, 8), 8), ln] = out
            _, pre, sig = fields(xg[o, pl.ds(edge, 4), :], o, 4)
            xg[o, pl.ds(edge, 4), :] = pre * sig
        return carry

    lax.fori_loop(0, 16, grid_row, 0)

    taps = [pair_of(index) for index in range(PAIRS)]

    def lhs_row(gr, carry):
        for index, (tap, ob) in enumerate(taps):
            dy, dx = lax.div(tap, 3), lax.rem(tap, 3)
            at = spot(gr + 2 - dy, 2 - dx)
            value = ug[jnp.minimum(ob, blocks - 1), pl.ds(at, 64), :]
            lhs_ref[pl.ds(pl.multiple_of(gr * 64, 64), 64), lane_block(index)] = value.astype(BF16)
        return carry

    lax.fori_loop(0, 16, lhs_row, 0)

    for index, (tap, ob) in enumerate(taps):
        dy, dx = lax.div(tap, 3), lax.rem(tap, 3)
        for target in range(8):
            for line in range(2):
                at = small(4 * (target // 2) + half_rows() + line + dy, 4 * (target % 2) + dx)
                to = index * 256 + target * 32 + line * 16
                for o in range(blocks):
                    rows_ref[to : to + 16, lane_block(o)] = xg[o, pl.ds(at, 16), :].astype(BF16)

    load.wait()
    each = weight_ref.shape[1]
    for source in range(weight_ref.shape[0]):
        wf[source * each : (source + 1) * each, :] = weight_ref[source].astype(F32)
    for index in range(PAIRS):
        wc[:, lane_block(index)] = wf[pl.ds(index, chans, stride=PAIRS), :].astype(BF16)

    chunk = 256
    total = jnp.zeros((8, chans), F32)
    for start in range(0, lhs_ref.shape[0], chunk):
        value = lax.dot_general(
            lhs_ref[start : start + chunk, :], wc[...], (((1,), (1,)), ((), ())), preferred_element_type=F32
        )
        value = value * slope_ref[start : start + chunk, :]
        total = total + jnp.sum(value.reshape(chunk // 8, 8, chans), axis=0)
    lanes = total[:, lane_block(0)]
    for o in range(1, blocks):
        lanes = lanes + total[:, lane_block(o)]
    lanes = lanes + pltpu.roll(lanes, 4, axis=0)

    velocity[...] = jnp.zeros(velocity.shape, F32)
    for index in range(PAIRS):
        slot = taps[index][1] - lax.div((lax.axis_index("gy") * 2 + lax.axis_index("gx_1")) * PAIRS, 9)
        part = jnp.dot(
            rows_ref[index * 256 : index * 256 + 256, :], wc[:, lane_block(index)], preferred_element_type=F32
        )
        velocity[slot] = velocity[slot] + part
    for target in range(8):
        for slot in range(2):
            out_ref[target, slot * 32 : slot * 32 + 32, :] = velocity[slot, target * 32 : target * 32 + 32, :]
        out_ref[target, 64:72, :] = lanes


def step_kernel(parts_ref, start_ref, rows_ref, mass_ref):
    blocks = start_ref.shape[1] // LANES
    total = parts_ref[0, 64:72, :]
    for source in range(1, 8):
        total = total + parts_ref[source, 64:72, :]
    mass = jnp.sum(total, axis=1, keepdims=True)
    lane = lax.broadcasted_iota(jnp.int32, (8, LANES), 1)
    latents = lax.broadcasted_iota(jnp.int32, (8, LANES), 0)
    line = jnp.sum(jnp.where(lane == latents, mass, 0.0), axis=0, keepdims=True)
    mass_ref[...] = jnp.broadcast_to(line, mass_ref.shape)
    velocity = [jnp.zeros((32, LANES), F32) for _ in range(blocks)]
    for source in range(8):
        for slot in range(2):
            o = first_block(source) + slot
            if o < blocks:
                velocity[o] = velocity[o] + parts_ref[source, slot * 32 : slot * 32 + 32, :]
    for o in range(blocks):
        rows_ref[:, lane_block(o)] = (start_ref[:, lane_block(o)] + 0.25 * velocity[o]).astype(BF16)


def final_kernel(scale, mass_ref, rows0, rows1, next_ref, out_ref, lines):
    blocks = lines.shape[0]
    total = jnp.sum(mass_ref[...], axis=0, keepdims=True)
    lane = lax.broadcasted_iota(jnp.int32, (1, LANES), 1)
    for b in range(4):
        out_ref[b] = scale * jnp.sum(jnp.where(lane == b, total, 0.0))
    for start, rows in ((half_rows(), rows0), (2 - half_rows(), rows1)):
        for o in range(blocks):
            lines[o] = rows[:, lane_block(o)].astype(F32)
        for o in range(blocks):
            for b in range(4):
                for r in range(2):
                    value = lines[o, pl.ds(r * 16 + b, 4, stride=4), :].astype(BF16)
                    next_ref[b, start + r, :, lane_block(o)] = value


def shape(dims, kind):
    return jax.ShapeDtypeStruct(dims, kind)


def body(state, probe_signs, timesteps, time_table, gn_gain, gn_shift, conv_weight, conv_bias):
    chans = state.shape[3]
    blocks = chans // LANES
    each = conv_weight.shape[1] * PAIRS
    params = pltpu.CompilerParams(vmem_limit_bytes=40 * 1024 * 1024)
    far = lambda array: pltpu.with_memory_space_constraint(array, pltpu.HBM)
    main, rim, base = pl.pallas_call(
        pack_kernel,
        out_shape=(shape((192, chans), BF16), shape((56, chans), BF16), shape((32, chans), F32)),
        in_specs=[HBM] * 2,
        out_specs=(VMEM,) * 3,
        scratch_shapes=[
            pltpu.VMEM(probe_signs.shape, jnp.int32),
            pltpu.VMEM(state.shape, BF16),
            pltpu.VMEM((blocks, 128, LANES), F32),
            pltpu.VMEM((blocks, 64, LANES), F32),
            pltpu.VMEM((56, chans), F32),
            pltpu.VMEM((32, chans), F32),
            pltpu.SemaphoreType.DMA((2,)),
        ],
        compiler_params=params,
        name="pack",
    )(far(probe_signs), far(state))
    wsend = pl.pallas_call(
        spread_kernel,
        out_shape=shape((32, each, LANES), BF16),
        in_specs=[VMEM],
        out_specs=VMEM,
        scratch_shapes=[pltpu.VMEM((each, LANES), F32)],
        compiler_params=params,
        name="deal",
    )(conv_weight)
    offset, start = pl.pallas_call(
        lookup_kernel,
        out_shape=(shape((8, chans), F32), shape((32, chans), F32)),
        in_specs=[SMEM, HBM, VMEM, VMEM, VMEM],
        out_specs=(VMEM,) * 2,
        scratch_shapes=[pltpu.VMEM((4, 8, chans), F32), pltpu.SemaphoreType.DMA((4,))],
        compiler_params=params,
        name="lookup",
    )(timesteps, far(time_table), gn_shift[None], conv_bias[None], base)

    across = [(a * 2 + b, (1 - a) * 2 + 1 - b) for a in range(2) for b in range(2)]
    facing = lax.ppermute(rim, GX, across)
    weights = lax.all_to_all(wsend, PROBE, 0, 0, tiled=True)
    block = jnp.concatenate([main, facing, rim[48:56]], axis=0)
    down = [(i, (i + 1) % 4) for i in range(4)]
    up = [(i, (i + 3) % 4) for i in range(4)]
    above = lax.ppermute(block, "gy", down)
    below = lax.ppermute(block, "gy", up)
    onward = [(x * 2 + c, (x + 1 - 2 * c) % 4 * 2 + c) for x in range(4) for c in range(2)]
    beyond = lax.ppermute(jnp.where(lax.axis_index("gx_1") == 0, above, below), ("gy", "gx_1"), onward)
    own = [block, above, below, beyond]
    swap = [(0, 1), (1, 0)]
    other = [lax.ppermute(block, "gx_1", swap)]
    other += [lax.ppermute(tile, "gx_1", swap) for tile in own[1:]]

    partial = pl.pallas_call(
        mix_kernel,
        out_shape=shape((8, 72, LANES), F32),
        in_specs=[VMEM] * 8 + [HBM] + [VMEM] * 2,
        out_specs=VMEM,
        scratch_shapes=[
            pltpu.VMEM((blocks, 1440, LANES), F32),
            pltpu.VMEM((blocks, 720, LANES), F32),
            pltpu.VMEM((1024, PAIRS * LANES), BF16),
            pltpu.VMEM((1024, chans), F32),
            pltpu.VMEM((PAIRS * 256, chans), BF16),
            pltpu.VMEM((32, each, LANES), BF16),
            pltpu.VMEM((32 * each, LANES), F32),
            pltpu.VMEM((chans, PAIRS * LANES), BF16),
            pltpu.VMEM((2, 256, LANES), F32),
            pltpu.SemaphoreType.DMA,
        ],
        compiler_params=params,
        name="mix",
    )(*own, *other, far(weights), gn_gain[None], offset)

    partial = lax.all_to_all(partial, ("gy", "gx_1"), 0, 0, tiled=True)
    rows, mass = pl.pallas_call(
        step_kernel,
        out_shape=(shape((32, chans), BF16), shape((64, LANES), F32)),
        in_specs=[VMEM] * 2,
        out_specs=(VMEM,) * 2,
        compiler_params=params,
        name="step",
    )(partial, start)
    tall = lax.axis_size("probe_0")
    facing_rows = lax.ppermute(rows, "probe_0", [(y, y ^ 1) for y in range(tall)])
    mass = lax.all_to_all(mass.reshape(64, 1, LANES), ("gx_0",) + PROBE, 0, 0, tiled=True)
    scale = -0.25 / (probe_signs.shape[0] * lax.axis_size(PROBE))
    return pl.pallas_call(
        lambda *refs: final_kernel(scale, *refs),
        out_shape=(shape(state.shape, BF16), shape((4,), F32)),
        in_specs=[VMEM] * 3,
        out_specs=(VMEM, SMEM),
        scratch_shapes=[pltpu.VMEM((blocks, 32, LANES), F32)],
        compiler_params=params,
        name="final",
    )(mass.reshape(64, LANES), rows, facing_rows)


def solution(mesh):
    split = Mesh(
        mesh.devices.reshape(mesh.shape["gy"], 2, 2, 8, 4),
        ("gy", "gx_0", "gx_1", "probe_0", "probe_1"),
    )
    return jax.shard_map(
        body,
        mesh=split,
        in_specs=(
            P(None, "gy", GX, None),
            P(PROBE, None, "gy", GX, None),
            P(),
            P(),
            P(),
            P(),
            P(None, PROBE, None),
            P(),
        ),
        out_specs=(P(None, "gy", GX, None), P()),
        check_vma=False,
    )
```

```python
import jax
import jax.numpy as jnp
from jax import lax
from jax.experimental import pallas as pl
from jax.experimental.pallas import tpu as pltpu
from jax.sharding import Mesh
from jax.sharding import PartitionSpec as P


GROUPS = 32
GX = ("gx_0", "gx_1")
PROBE = ("probe_0", "probe_1")
LANES = 128
PAIRS = 6
F32 = jnp.float32
BF16 = jnp.bfloat16
VMEM = pl.BlockSpec(memory_space=pltpu.VMEM)
SMEM = pl.BlockSpec(memory_space=pltpu.SMEM)
HBM = pl.BlockSpec(memory_space=pltpu.HBM)


def three_parts(value):
    high = value.astype(BF16)
    rest = value - high.astype(F32)
    mid = rest.astype(BF16)
    low = (rest - mid.astype(F32)).astype(BF16)
    return high, mid, low


def lane_block(index):
    return slice(index * LANES, (index + 1) * LANES)


def doubled_rows(rows):
    turned = pltpu.roll(rows, 4, axis=0)
    upper = lax.broadcasted_iota(jnp.int32, rows.shape, 0) < 4
    return jnp.where(upper, rows, turned), jnp.where(upper, turned, rows)


def half_rows():
    return 2 * lax.rem(lax.axis_index("probe_0"), 2)


def first_block(member):
    return member * PAIRS // 9


def pair_of(index):
    member = lax.axis_index("gy") * 2 + lax.axis_index("gx_1")
    number = member * PAIRS + index
    return lax.rem(number, 9), lax.div(number, 9)


def spread_kernel(weight_ref, wsend_ref, wf):
    for index in range(PAIRS):
        tap, ob = pair_of(index)
        rows = weight_ref[tap].astype(F32)
        picked = jnp.zeros((rows.shape[0], LANES), F32)
        for o in range(rows.shape[1] // LANES):
            picked = picked + jnp.where(ob == o, rows[:, lane_block(o)], 0.0)
        wf[pl.ds(index, rows.shape[0], stride=PAIRS), :] = picked
    packed = wf[...].astype(BF16)
    for target in range(wsend_ref.shape[0]):
        wsend_ref[target] = packed


def lookup_kernel(step_ref, table_hbm, shift_ref, bias_ref, base_ref, offset_ref, start_ref, table, found):
    steps = [step_ref[b] for b in range(4)]
    finds = [
        pltpu.make_async_copy(
            table_hbm.at[pl.ds(pl.multiple_of(lax.div(steps[b], 8) * 8, 8), 8), :], table.at[b], found.at[b]
        )
        for b in range(4)
    ]
    for find in finds:
        find.start()
    start_ref[...] = base_ref[...] + 0.25 * bias_ref[...]
    for b in range(4):
        finds[b].wait()
        line = table[b, pl.ds(lax.rem(steps[b], 8), 1), :] + shift_ref[...]
        offset_ref[b : b + 1, :] = line
        offset_ref[b + 4 : b + 5, :] = line


def pack_kernel(signs_hbm, state_hbm, main_ref, rim_ref, base_ref, signs_ref, state_ref, uf, xf, rim, sums, arrived):
    blocks = uf.shape[0]
    loads = [
        pltpu.make_async_copy(src, dst, arrived.at[index])
        for index, (src, dst) in enumerate(((signs_hbm, signs_ref), (state_hbm, state_ref)))
    ]
    for load in loads:
        load.start()
    for load in loads:
        load.wait()
    for p in range(2):
        for b in range(4):
            for r in range(4):
                line = signs_ref[p, b, r].astype(F32)
                for o in range(blocks):
                    uf[o, pl.ds(r * 32 + p * 4 + b, 4, stride=8), :] = line[:, lane_block(o)]
    for b in range(4):
        for r in range(4):
            line = state_ref[b, r].astype(F32)
            for o in range(blocks):
                xf[o, pl.ds(r * 16 + b, 4, stride=4), :] = line[:, lane_block(o)]

    for o in range(blocks):
        base_ref[:, lane_block(o)] = xf[o, pl.ds(pl.multiple_of(half_rows() * 16, 8), 32), :]
    edge = jnp.where(lax.axis_index("gx_0") == 0, 3, 0)
    for o in range(blocks):
        sum_u = jnp.zeros((8, LANES), F32)
        cross = jnp.zeros((8, LANES), F32)
        sum_x = jnp.zeros((8, LANES), F32)
        sum_xx = jnp.zeros((8, LANES), F32)
        for two in range(8):
            pair = doubled_rows(xf[o, two * 8 : two * 8 + 8, :])
            for half in range(2):
                cell = two * 2 + half
                x = pair[half]
                u = uf[o, cell * 8 : cell * 8 + 8, :]
                sum_u, cross = sum_u + u, cross + u * x
                sum_x, sum_xx = sum_x + x, sum_xx + x * x
        for kind, part in enumerate((sum_u, cross, sum_x, sum_xx)):
            sums[kind * 8 : kind * 8 + 8, lane_block(o)] = part
        for r in range(4):
            rim[r * 8 : r * 8 + 8, lane_block(o)] = uf[o, pl.ds(pl.multiple_of((r * 4 + edge) * 8, 8), 8), :]
            rim[32 + r * 4 : 36 + r * 4, lane_block(o)] = xf[o, pl.ds((r * 4 + edge) * 4, 4), :]

    width = sums.shape[1] // GROUPS
    row = lax.broadcasted_iota(jnp.int32, (sums.shape[1], LANES), 0)
    first = lax.broadcasted_iota(jnp.int32, (sums.shape[1], LANES), 1) * width
    member = jnp.where((row >= first) & (row < first + width), 1.0, 0.0).astype(BF16)
    grouped = jnp.zeros((32, LANES), F32)
    for part in three_parts(sums[...]):
        grouped = grouped + jnp.dot(part, member, preferred_element_type=F32)
    stats = grouped[0:8]
    for kind in range(1, 4):
        stats = stats + pltpu.roll(grouped[kind * 8 : kind * 8 + 8], GROUPS * kind, axis=1)
    rim[48:56, :] = jnp.zeros((8, rim.shape[1]), F32)
    for index, part in enumerate(three_parts(stats)):
        rim[48:56, lane_block(index)] = part.astype(F32)

    for o in range(blocks):
        main_ref[0:128, lane_block(o)] = uf[o].astype(BF16)
        main_ref[128:192, lane_block(o)] = xf[o].astype(BF16)
    rim_ref[...] = rim[...].astype(BF16)


def mix_kernel(
    own0, own1, own3, own2, other0, other1, other3, other2, weight_hbm, gain_ref, offset_ref,
    out_ref, ug, xg, lhs_ref, slope_ref, rows_ref, weight_ref, wf, wc, velocity, arrived,
):
    load = pltpu.make_async_copy(weight_hbm, weight_ref, arrived)
    load.start()
    blocks = ug.shape[0]
    core = lax.axis_index("gx_1")
    half = lax.axis_index("gx_0")
    chans = own0.shape[1]

    def spot(row, col):
        return pl.multiple_of((row * 10 + col) * 8, 8)

    def small(row, col):
        return pl.multiple_of((row * 10 + col) * 4, 4)

    for o in range(blocks):
        for row in (0, 17):
            ug[o, row * 80 : row * 80 + 80, :] = jnp.zeros((80, LANES), F32)
            xg[o, row * 40 : row * 40 + 40, :] = jnp.zeros((40, LANES), F32)
        for row in range(1, 17):
            for col in (0, 9):
                ug[o, row * 80 + col * 8 : row * 80 + col * 8 + 8, :] = jnp.zeros((8, LANES), F32)
                xg[o, row * 40 + col * 4 : row * 40 + col * 4 + 4, :] = jnp.zeros((4, LANES), F32)

    total = jnp.zeros((8, chans), F32)
    rim_here = core == 1 - half
    rim_col = jnp.where(half == 0, 9, 0)
    sources = ((0, own0, other0), (1, own1, other1), (3, own3, other3), (2, own2, other2))
    for back, own_ref, other_ref in sources:
        tile = lax.rem(lax.axis_index("gy") + 4 - back, 4)
        for src, base in ((own_ref, 4 * core), (other_ref, 4 * (1 - core))):
            for r in range(4):
                at = spot(4 * tile + r + 1, base + 1)
                lines = src[r * 32 : r * 32 + 32, :].astype(F32)
                states = src[128 + r * 16 : 144 + r * 16, :].astype(F32)
                for o in range(blocks):
                    ug[o, pl.ds(at, 32), :] = lines[:, lane_block(o)]
                    xg[o, pl.ds(small(4 * tile + r + 1, base + 1), 16), :] = states[:, lane_block(o)]
        mine = own_ref[192:256, :].astype(F32)
        theirs = other_ref[192:256, :].astype(F32)
        total = total + mine[48:56] + mine[56:64] + theirs[48:56] + theirs[56:64]
        rim = jnp.where(rim_here, mine[0:48], theirs[0:48])
        for r in range(4):
            at = spot(4 * tile + r + 1, rim_col)
            for o in range(blocks):
                ug[o, pl.ds(at, 8), :] = rim[r * 8 : r * 8 + 8, lane_block(o)]
                xg[o, pl.ds(small(4 * tile + r + 1, rim_col), 4), :] = rim[32 + r * 4 : 36 + r * 4, lane_block(o)]

    stats = total[:, lane_block(0)] + total[:, lane_block(1)] + total[:, lane_block(2)]
    width = chans // GROUPS
    lane = lax.broadcasted_iota(jnp.int32, (LANES, chans), 1)
    first = lax.broadcasted_iota(jnp.int32, (LANES, chans), 0) * width
    spread = jnp.where((lane >= first) & (lane < first + width), 1.0, 0.0).astype(BF16)

    def expanded(kind):
        turned = stats if kind == 0 else pltpu.roll(stats, LANES - GROUPS * kind, axis=1)
        out = jnp.zeros((8, chans), F32)
        for part in three_parts(turned):
            out = out + jnp.dot(part, spread, preferred_element_type=F32)
        return out

    count = 256 * width
    sum_u, cross, sum_x, sum_xx = (expanded(kind) for kind in range(4))
    mean = sum_x / count
    sigma = jnp.sqrt(sum_xx / count - mean * mean + 1e-05)
    inverse = 1.0 / sigma
    mean_u = sum_u / count
    mean_cu = (cross - mean * sum_u) / count
    bend = mean_cu / (sigma * sigma * sigma)
    offset = offset_ref[...]
    gain = gain_ref[...]

    scale = inverse * gain
    tilt = gain * inverse

    def fields(x, o, rows):
        at = lane_block(o)
        centered = x - mean[:rows, at]
        pre = centered * scale[:rows, at] + offset[:rows, at]
        sig = 1.0 / (1.0 + jnp.exp(-pre))
        return centered, pre, sig

    def grid_row(gr, carry):
        at = spot(gr + 1, 1)
        near = small(gr + 1, 1)
        edge = small(gr + 1, rim_col)
        for o in range(blocks):
            ln = lane_block(o)
            x = xg[o, pl.ds(near, 32), :].reshape(4, 8, LANES)
            centered, pre, sig = fields(x, o, 8)
            xg[o, pl.ds(near, 32), :] = (pre * sig).reshape(32, LANES)
            slope = sig * (1.0 + pre * (1.0 - sig))
            along = slope * tilt[:, ln]
            across = slope * gain[:, ln] * centered
            for two in range(4):
                spans = zip(doubled_rows(along[two]), doubled_rows(across[two]))
                for half_cell, (first, second) in enumerate(spans):
                    cell = two * 2 + half_cell
                    u = ug[o, pl.ds(pl.multiple_of(at + cell * 8, 8), 8), :]
                    out = first * (u - mean_u[:, ln]) - second * bend[:, ln]
                    slope_ref[pl.ds(pl.multiple_of(gr * 64 + cell * 8, 8), 8), ln] = out.astype(BF16).astype(F32)
            _, pre, sig = fields(xg[o, pl.ds(edge, 4), :], o, 4)
            xg[o, pl.ds(edge, 4), :] = pre * sig
        return carry

    lax.fori_loop(0, 16, grid_row, 0)

    taps = [pair_of(index) for index in range(PAIRS)]

    def lhs_row(gr, carry):
        for index, (tap, ob) in enumerate(taps):
            dy, dx = lax.div(tap, 3), lax.rem(tap, 3)
            at = spot(gr + 2 - dy, 2 - dx)
            value = ug[jnp.minimum(ob, blocks - 1), pl.ds(at, 64), :]
            lhs_ref[pl.ds(pl.multiple_of(gr * 64, 64), 64), lane_block(index)] = value.astype(BF16)
        return carry

    lax.fori_loop(0, 16, lhs_row, 0)

    for index, (tap, ob) in enumerate(taps):
        dy, dx = lax.div(tap, 3), lax.rem(tap, 3)
        for target in range(8):
            for line in range(2):
                at = small(4 * (target // 2) + half_rows() + line + dy, 4 * (target % 2) + dx)
                to = index * 256 + target * 32 + line * 16
                for o in range(blocks):
                    rows_ref[to : to + 16, lane_block(o)] = xg[o, pl.ds(at, 16), :].astype(BF16)

    load.wait()
    each = weight_ref.shape[1]
    for source in range(weight_ref.shape[0]):
        wf[source * each : (source + 1) * each, :] = weight_ref[source].astype(F32)
    for index in range(PAIRS):
        wc[:, lane_block(index)] = wf[pl.ds(index, chans, stride=PAIRS), :].astype(BF16)

    chunk = 256
    total = jnp.zeros((8, chans), F32)
    for start in range(0, lhs_ref.shape[0], chunk):
        value = lax.dot_general(
            lhs_ref[start : start + chunk, :], wc[...], (((1,), (1,)), ((), ())), preferred_element_type=F32
        )
        value = value * slope_ref[start : start + chunk, :]
        total = total + jnp.sum(value.reshape(chunk // 8, 8, chans), axis=0)
    lanes = total[:, lane_block(0)]
    for o in range(1, blocks):
        lanes = lanes + total[:, lane_block(o)]
    lanes = lanes + pltpu.roll(lanes, 4, axis=0)

    velocity[...] = jnp.zeros(velocity.shape, F32)
    for index in range(PAIRS):
        slot = taps[index][1] - lax.div((lax.axis_index("gy") * 2 + lax.axis_index("gx_1")) * PAIRS, 9)
        part = jnp.dot(
            rows_ref[index * 256 : index * 256 + 256, :], wc[:, lane_block(index)], preferred_element_type=F32
        )
        velocity[slot] = velocity[slot] + part
    for target in range(8):
        for slot in range(2):
            out_ref[target, slot * 32 : slot * 32 + 32, :] = velocity[slot, target * 32 : target * 32 + 32, :]
        out_ref[target, 64:72, :] = lanes


def step_kernel(parts_ref, start_ref, rows_ref, mass_ref):
    blocks = start_ref.shape[1] // LANES
    total = parts_ref[0, 64:72, :]
    for source in range(1, 8):
        total = total + parts_ref[source, 64:72, :]
    mass = jnp.sum(total, axis=1, keepdims=True)
    lane = lax.broadcasted_iota(jnp.int32, (8, LANES), 1)
    latents = lax.broadcasted_iota(jnp.int32, (8, LANES), 0)
    line = jnp.sum(jnp.where(lane == latents, mass, 0.0), axis=0, keepdims=True)
    mass_ref[...] = jnp.broadcast_to(line, mass_ref.shape)
    velocity = [jnp.zeros((32, LANES), F32) for _ in range(blocks)]
    for source in range(8):
        for slot in range(2):
            o = first_block(source) + slot
            if o < blocks:
                velocity[o] = velocity[o] + parts_ref[source, slot * 32 : slot * 32 + 32, :]
    for o in range(blocks):
        rows_ref[:, lane_block(o)] = (start_ref[:, lane_block(o)] + 0.25 * velocity[o]).astype(BF16)


def tally_kernel(scale, mass_ref, out_ref):
    total = jnp.sum(mass_ref[...], axis=0, keepdims=True)
    lane = lax.broadcasted_iota(jnp.int32, (1, LANES), 1)
    for b in range(4):
        out_ref[b] = scale * jnp.sum(jnp.where(lane == b, total, 0.0))


def final_kernel(rows0, rows1, next_ref, lines):
    blocks = lines.shape[0]
    for start, rows in ((half_rows(), rows0), (2 - half_rows(), rows1)):
        for o in range(blocks):
            lines[o] = rows[:, lane_block(o)].astype(F32)
        for o in range(blocks):
            for b in range(4):
                for r in range(2):
                    value = lines[o, pl.ds(r * 16 + b, 4, stride=4), :].astype(BF16)
                    next_ref[b, start + r, :, lane_block(o)] = value


def shape(dims, kind):
    return jax.ShapeDtypeStruct(dims, kind)


def body(state, probe_signs, timesteps, time_table, gn_gain, gn_shift, conv_weight, conv_bias):
    chans = state.shape[3]
    blocks = chans // LANES
    each = conv_weight.shape[1] * PAIRS
    params = pltpu.CompilerParams(vmem_limit_bytes=40 * 1024 * 1024)
    far = lambda array: pltpu.with_memory_space_constraint(array, pltpu.HBM)
    main, rim, base = pl.pallas_call(
        pack_kernel,
        out_shape=(shape((192, chans), BF16), shape((56, chans), BF16), shape((32, chans), F32)),
        in_specs=[HBM] * 2,
        out_specs=(VMEM,) * 3,
        scratch_shapes=[
            pltpu.VMEM(probe_signs.shape, jnp.int32),
            pltpu.VMEM(state.shape, BF16),
            pltpu.VMEM((blocks, 128, LANES), F32),
            pltpu.VMEM((blocks, 64, LANES), F32),
            pltpu.VMEM((56, chans), F32),
            pltpu.VMEM((32, chans), F32),
            pltpu.SemaphoreType.DMA((2,)),
        ],
        compiler_params=params,
        name="pack",
    )(far(probe_signs), far(state))
    wsend = pl.pallas_call(
        spread_kernel,
        out_shape=shape((32, each, LANES), BF16),
        in_specs=[VMEM],
        out_specs=VMEM,
        scratch_shapes=[pltpu.VMEM((each, LANES), F32)],
        compiler_params=params,
        name="deal",
    )(conv_weight)
    offset, start = pl.pallas_call(
        lookup_kernel,
        out_shape=(shape((8, chans), F32), shape((32, chans), F32)),
        in_specs=[SMEM, HBM, VMEM, VMEM, VMEM],
        out_specs=(VMEM,) * 2,
        scratch_shapes=[pltpu.VMEM((4, 8, chans), F32), pltpu.SemaphoreType.DMA((4,))],
        compiler_params=params,
        name="lookup",
    )(timesteps, far(time_table), gn_shift[None], conv_bias[None], base)

    facing = lax.ppermute(rim, GX, [(1, 2), (2, 1)])
    outer = lax.ppermute(rim[48:56], GX, [(0, 3), (3, 0)])
    weights = lax.all_to_all(wsend, PROBE, 0, 0, tiled=True)
    block = jnp.concatenate([main, facing[:48], facing[48:] + outer, rim[48:56]], axis=0)
    down = [(i, (i + 1) % 4) for i in range(4)]
    up = [(i, (i + 3) % 4) for i in range(4)]
    above = lax.ppermute(block, "gy", down)
    below = lax.ppermute(block, "gy", up)
    onward = [(x * 2 + c, (x + 1 - 2 * c) % 4 * 2 + c) for x in range(4) for c in range(2)]
    beyond = lax.ppermute(jnp.where(lax.axis_index("gx_1") == 0, above, below), ("gy", "gx_1"), onward)
    own = [block, above, below, beyond]
    swap = [(0, 1), (1, 0)]
    other = [lax.ppermute(block, "gx_1", swap)]
    other += [lax.ppermute(tile, "gx_1", swap) for tile in own[1:]]

    partial = pl.pallas_call(
        mix_kernel,
        out_shape=shape((8, 72, LANES), F32),
        in_specs=[VMEM] * 8 + [HBM] + [VMEM] * 2,
        out_specs=VMEM,
        scratch_shapes=[
            pltpu.VMEM((blocks, 1440, LANES), F32),
            pltpu.VMEM((blocks, 720, LANES), F32),
            pltpu.VMEM((1024, PAIRS * LANES), BF16),
            pltpu.VMEM((1024, chans), F32),
            pltpu.VMEM((PAIRS * 256, chans), BF16),
            pltpu.VMEM((32, each, LANES), BF16),
            pltpu.VMEM((32 * each, LANES), F32),
            pltpu.VMEM((chans, PAIRS * LANES), BF16),
            pltpu.VMEM((2, 256, LANES), F32),
            pltpu.SemaphoreType.DMA,
        ],
        compiler_params=params,
        name="mix",
    )(*own, *other, far(weights), gn_gain[None], offset)

    partial = lax.all_to_all(partial, ("gy", "gx_1"), 0, 0, tiled=True)
    rows, mass = pl.pallas_call(
        step_kernel,
        out_shape=(shape((32, chans), BF16), shape((64, LANES), F32)),
        in_specs=[VMEM] * 2,
        out_specs=(VMEM,) * 2,
        compiler_params=params,
        name="step",
    )(partial, start)
    tall = lax.axis_size("probe_0")
    facing_rows = lax.ppermute(rows, "probe_0", [(y, y ^ 1) for y in range(tall)])
    mass = lax.all_to_all(mass.reshape(64, 1, LANES), ("gx_0",) + PROBE, 0, 0, tiled=True)
    scale = -0.25 / (probe_signs.shape[0] * lax.axis_size(PROBE))
    total = pl.pallas_call(
        lambda *refs: tally_kernel(scale, *refs),
        out_shape=shape((4,), F32),
        in_specs=[VMEM],
        out_specs=SMEM,
        compiler_params=params,
        name="tally",
    )(mass.reshape(64, LANES))
    following = pl.pallas_call(
        final_kernel,
        out_shape=shape(state.shape, BF16),
        in_specs=[VMEM] * 2,
        out_specs=VMEM,
        scratch_shapes=[pltpu.VMEM((blocks, 32, LANES), F32)],
        compiler_params=params,
        name="final",
    )(rows, facing_rows)
    return following, total


def solution(mesh):
    split = Mesh(
        mesh.devices.reshape(mesh.shape["gy"], 2, 2, 8, 4),
        ("gy", "gx_0", "gx_1", "probe_0", "probe_1"),
    )
    return jax.shard_map(
        body,
        mesh=split,
        in_specs=(
            P(None, "gy", GX, None),
            P(PROBE, None, "gy", GX, None),
            P(),
            P(),
            P(),
            P(),
            P(None, PROBE, None),
            P(),
        ),
        out_specs=(P(None, "gy", GX, None), P()),
        check_vma=False,
    )
```

```python
import jax
import jax.numpy as jnp
from jax import lax
from jax.experimental import pallas as pl
from jax.experimental.pallas import tpu as pltpu
from jax.sharding import Mesh
from jax.sharding import PartitionSpec as P


GROUPS = 32
GX = ("gx_0", "gx_1")
PROBE = ("probe_0", "probe_1")
LANES = 128
PAIRS = 6
F32 = jnp.float32
BF16 = jnp.bfloat16
VMEM = pl.BlockSpec(memory_space=pltpu.VMEM)
SMEM = pl.BlockSpec(memory_space=pltpu.SMEM)
HBM = pl.BlockSpec(memory_space=pltpu.HBM)


def three_parts(value):
    high = value.astype(BF16)
    rest = value - high.astype(F32)
    mid = rest.astype(BF16)
    low = (rest - mid.astype(F32)).astype(BF16)
    return high, mid, low


def lane_block(index):
    return slice(index * LANES, (index + 1) * LANES)


def doubled_rows(rows):
    turned = pltpu.roll(rows, 4, axis=0)
    upper = lax.broadcasted_iota(jnp.int32, rows.shape, 0) < 4
    return jnp.where(upper, rows, turned), jnp.where(upper, turned, rows)


def half_rows():
    return 2 * lax.rem(lax.axis_index("probe_0"), 2)


def first_block(member):
    return member * PAIRS // 9


def pair_of(index):
    member = lax.axis_index("gy") * 2 + lax.axis_index("gx_1")
    number = member * PAIRS + index
    return lax.rem(number, 9), lax.div(number, 9)


def lookup_kernel(step_ref, table_hbm, shift_ref, bias_ref, base_ref, offset_ref, start_ref, table, found):
    steps = [step_ref[b] for b in range(4)]
    finds = [
        pltpu.make_async_copy(
            table_hbm.at[pl.ds(pl.multiple_of(lax.div(steps[b], 8) * 8, 8), 8), :], table.at[b], found.at[b]
        )
        for b in range(4)
    ]
    for find in finds:
        find.start()
    start_ref[...] = base_ref[...] + 0.25 * bias_ref[...]
    for b in range(4):
        finds[b].wait()
        line = table[b, pl.ds(lax.rem(steps[b], 8), 1), :] + shift_ref[...]
        offset_ref[b : b + 1, :] = line
        offset_ref[b + 4 : b + 5, :] = line


def pack_kernel(
    weight_hbm, state_hbm, signs_hbm, main_ref, rim_ref, base_ref, wsend_hbm,
    weight_ref, state_ref, signs_ref, uf, xf, wf, wsend_ref, rim, sums, arrived, left,
):
    blocks = uf.shape[0]
    loads = [
        pltpu.make_async_copy(src, dst, arrived.at[index])
        for index, (src, dst) in enumerate(
            ((weight_hbm, weight_ref), (state_hbm, state_ref), (signs_hbm, signs_ref))
        )
    ]
    for load in loads:
        load.start()
    loads[0].wait()
    for index in range(PAIRS):
        tap, ob = pair_of(index)
        rows = weight_ref[tap].astype(F32)
        picked = jnp.zeros((rows.shape[0], LANES), F32)
        for o in range(blocks):
            picked = picked + jnp.where(ob == o, rows[:, lane_block(o)], 0.0)
        wf[pl.ds(index, rows.shape[0], stride=PAIRS), :] = picked
    packed = wf[...].astype(BF16)
    for target in range(wsend_ref.shape[0]):
        wsend_ref[target] = packed
    leave = pltpu.make_async_copy(wsend_ref, wsend_hbm, left)
    leave.start()
    loads[1].wait()
    loads[2].wait()
    for p in range(2):
        for b in range(4):
            for r in range(4):
                line = signs_ref[p, b, r].astype(F32)
                for o in range(blocks):
                    uf[o, pl.ds(r * 32 + p * 4 + b, 4, stride=8), :] = line[:, lane_block(o)]
    for b in range(4):
        for r in range(4):
            line = state_ref[b, r].astype(F32)
            for o in range(blocks):
                xf[o, pl.ds(r * 16 + b, 4, stride=4), :] = line[:, lane_block(o)]

    for o in range(blocks):
        base_ref[:, lane_block(o)] = xf[o, pl.ds(pl.multiple_of(half_rows() * 16, 8), 32), :]
    edge = jnp.where(lax.axis_index("gx_0") == 0, 3, 0)
    for o in range(blocks):
        sum_u = jnp.zeros((8, LANES), F32)
        cross = jnp.zeros((8, LANES), F32)
        sum_x = jnp.zeros((8, LANES), F32)
        sum_xx = jnp.zeros((8, LANES), F32)
        for two in range(8):
            pair = doubled_rows(xf[o, two * 8 : two * 8 + 8, :])
            for half in range(2):
                cell = two * 2 + half
                x = pair[half]
                u = uf[o, cell * 8 : cell * 8 + 8, :]
                sum_u, cross = sum_u + u, cross + u * x
                sum_x, sum_xx = sum_x + x, sum_xx + x * x
        for kind, part in enumerate((sum_u, cross, sum_x, sum_xx)):
            sums[kind * 8 : kind * 8 + 8, lane_block(o)] = part
        for r in range(4):
            rim[r * 8 : r * 8 + 8, lane_block(o)] = uf[o, pl.ds(pl.multiple_of((r * 4 + edge) * 8, 8), 8), :]
            rim[32 + r * 4 : 36 + r * 4, lane_block(o)] = xf[o, pl.ds((r * 4 + edge) * 4, 4), :]

    width = sums.shape[1] // GROUPS
    row = lax.broadcasted_iota(jnp.int32, (sums.shape[1], LANES), 0)
    first = lax.broadcasted_iota(jnp.int32, (sums.shape[1], LANES), 1) * width
    member = jnp.where((row >= first) & (row < first + width), 1.0, 0.0).astype(BF16)
    grouped = jnp.zeros((32, LANES), F32)
    for part in three_parts(sums[...]):
        grouped = grouped + jnp.dot(part, member, preferred_element_type=F32)
    stats = grouped[0:8]
    for kind in range(1, 4):
        stats = stats + pltpu.roll(grouped[kind * 8 : kind * 8 + 8], GROUPS * kind, axis=1)
    rim[48:56, :] = jnp.zeros((8, rim.shape[1]), F32)
    for index, part in enumerate(three_parts(stats)):
        rim[48:56, lane_block(index)] = part.astype(F32)

    for o in range(blocks):
        main_ref[0:128, lane_block(o)] = uf[o].astype(BF16)
        main_ref[128:192, lane_block(o)] = xf[o].astype(BF16)
    rim_ref[...] = rim[...].astype(BF16)
    leave.wait()


def mix_kernel(
    own0, own1, own3, own2, other0, other1, other3, other2, weight_hbm, gain_ref, offset_ref,
    out_ref, ug, xg, lhs_ref, slope_ref, rows_ref, weight_ref, wf, wc, velocity, arrived,
):
    load = pltpu.make_async_copy(weight_hbm, weight_ref, arrived)
    load.start()
    blocks = ug.shape[0]
    core = lax.axis_index("gx_1")
    half = lax.axis_index("gx_0")
    chans = own0.shape[1]

    def spot(row, col):
        return pl.multiple_of((row * 10 + col) * 8, 8)

    def small(row, col):
        return pl.multiple_of((row * 10 + col) * 4, 4)

    for o in range(blocks):
        for row in (0, 17):
            ug[o, row * 80 : row * 80 + 80, :] = jnp.zeros((80, LANES), F32)
            xg[o, row * 40 : row * 40 + 40, :] = jnp.zeros((40, LANES), F32)
        for row in range(1, 17):
            for col in (0, 9):
                ug[o, row * 80 + col * 8 : row * 80 + col * 8 + 8, :] = jnp.zeros((8, LANES), F32)
                xg[o, row * 40 + col * 4 : row * 40 + col * 4 + 4, :] = jnp.zeros((4, LANES), F32)

    total = jnp.zeros((8, chans), F32)
    rim_here = core == 1 - half
    rim_col = jnp.where(half == 0, 9, 0)
    sources = ((0, own0, other0), (1, own1, other1), (3, own3, other3), (2, own2, other2))
    for back, own_ref, other_ref in sources:
        tile = lax.rem(lax.axis_index("gy") + 4 - back, 4)
        for src, base in ((own_ref, 4 * core), (other_ref, 4 * (1 - core))):
            for r in range(4):
                at = spot(4 * tile + r + 1, base + 1)
                lines = src[r * 32 : r * 32 + 32, :].astype(F32)
                states = src[128 + r * 16 : 144 + r * 16, :].astype(F32)
                for o in range(blocks):
                    ug[o, pl.ds(at, 32), :] = lines[:, lane_block(o)]
                    xg[o, pl.ds(small(4 * tile + r + 1, base + 1), 16), :] = states[:, lane_block(o)]
        mine = own_ref[192:256, :].astype(F32)
        theirs = other_ref[192:256, :].astype(F32)
        total = total + mine[48:56] + mine[56:64] + theirs[48:56] + theirs[56:64]
        rim = jnp.where(rim_here, mine[0:48], theirs[0:48])
        for r in range(4):
            at = spot(4 * tile + r + 1, rim_col)
            for o in range(blocks):
                ug[o, pl.ds(at, 8), :] = rim[r * 8 : r * 8 + 8, lane_block(o)]
                xg[o, pl.ds(small(4 * tile + r + 1, rim_col), 4), :] = rim[32 + r * 4 : 36 + r * 4, lane_block(o)]

    stats = total[:, lane_block(0)] + total[:, lane_block(1)] + total[:, lane_block(2)]
    width = chans // GROUPS
    lane = lax.broadcasted_iota(jnp.int32, (LANES, chans), 1)
    first = lax.broadcasted_iota(jnp.int32, (LANES, chans), 0) * width
    spread = jnp.where((lane >= first) & (lane < first + width), 1.0, 0.0).astype(BF16)

    def expanded(kind):
        turned = stats if kind == 0 else pltpu.roll(stats, LANES - GROUPS * kind, axis=1)
        out = jnp.zeros((8, chans), F32)
        for part in three_parts(turned):
            out = out + jnp.dot(part, spread, preferred_element_type=F32)
        return out

    count = 256 * width
    sum_u, cross, sum_x, sum_xx = (expanded(kind) for kind in range(4))
    mean = sum_x / count
    sigma = jnp.sqrt(sum_xx / count - mean * mean + 1e-05)
    inverse = 1.0 / sigma
    mean_u = sum_u / count
    mean_cu = (cross - mean * sum_u) / count
    bend = mean_cu / (sigma * sigma * sigma)
    offset = offset_ref[...]
    gain = gain_ref[...]

    scale = inverse * gain
    tilt = gain * inverse

    def fields(x, o, rows):
        at = lane_block(o)
        centered = x - mean[:rows, at]
        pre = centered * scale[:rows, at] + offset[:rows, at]
        sig = 1.0 / (1.0 + jnp.exp(-pre))
        return centered, pre, sig

    def grid_row(gr, carry):
        at = spot(gr + 1, 1)
        near = small(gr + 1, 1)
        edge = small(gr + 1, rim_col)
        for o in range(blocks):
            ln = lane_block(o)
            x = xg[o, pl.ds(near, 32), :].reshape(4, 8, LANES)
            centered, pre, sig = fields(x, o, 8)
            xg[o, pl.ds(near, 32), :] = (pre * sig).reshape(32, LANES)
            slope = sig * (1.0 + pre * (1.0 - sig))
            along = slope * tilt[:, ln]
            across = slope * gain[:, ln] * centered
            for two in range(4):
                spans = zip(doubled_rows(along[two]), doubled_rows(across[two]))
                for half_cell, (first, second) in enumerate(spans):
                    cell = two * 2 + half_cell
                    u = ug[o, pl.ds(pl.multiple_of(at + cell * 8, 8), 8), :]
                    out = first * (u - mean_u[:, ln]) - second * bend[:, ln]
                    slope_ref[pl.ds(pl.multiple_of(gr * 64 + cell * 8, 8), 8), ln] = out.astype(BF16).astype(F32)
            _, pre, sig = fields(xg[o, pl.ds(edge, 4), :], o, 4)
            xg[o, pl.ds(edge, 4), :] = pre * sig
        return carry

    lax.fori_loop(0, 16, grid_row, 0)

    taps = [pair_of(index) for index in range(PAIRS)]

    def lhs_row(gr, carry):
        for index, (tap, ob) in enumerate(taps):
            dy, dx = lax.div(tap, 3), lax.rem(tap, 3)
            at = spot(gr + 2 - dy, 2 - dx)
            value = ug[jnp.minimum(ob, blocks - 1), pl.ds(at, 64), :]
            lhs_ref[pl.ds(pl.multiple_of(gr * 64, 64), 64), lane_block(index)] = value.astype(BF16)
        return carry

    lax.fori_loop(0, 16, lhs_row, 0)

    for index, (tap, ob) in enumerate(taps):
        dy, dx = lax.div(tap, 3), lax.rem(tap, 3)
        for target in range(8):
            for line in range(2):
                at = small(4 * (target // 2) + half_rows() + line + dy, 4 * (target % 2) + dx)
                to = index * 256 + target * 32 + line * 16
                for o in range(blocks):
                    rows_ref[to : to + 16, lane_block(o)] = xg[o, pl.ds(at, 16), :].astype(BF16)

    load.wait()
    each = weight_ref.shape[1]
    for source in range(weight_ref.shape[0]):
        wf[source * each : (source + 1) * each, :] = weight_ref[source].astype(F32)
    for index in range(PAIRS):
        wc[:, lane_block(index)] = wf[pl.ds(index, chans, stride=PAIRS), :].astype(BF16)

    chunk = 256
    total = jnp.zeros((8, chans), F32)
    for start in range(0, lhs_ref.shape[0], chunk):
        value = lax.dot_general(
            lhs_ref[start : start + chunk, :], wc[...], (((1,), (1,)), ((), ())), preferred_element_type=F32
        )
        value = value * slope_ref[start : start + chunk, :]
        total = total + jnp.sum(value.reshape(chunk // 8, 8, chans), axis=0)
    lanes = total[:, lane_block(0)]
    for o in range(1, blocks):
        lanes = lanes + total[:, lane_block(o)]
    lanes = lanes + pltpu.roll(lanes, 4, axis=0)

    velocity[...] = jnp.zeros(velocity.shape, F32)
    for index in range(PAIRS):
        slot = taps[index][1] - lax.div((lax.axis_index("gy") * 2 + lax.axis_index("gx_1")) * PAIRS, 9)
        part = jnp.dot(
            rows_ref[index * 256 : index * 256 + 256, :], wc[:, lane_block(index)], preferred_element_type=F32
        )
        velocity[slot] = velocity[slot] + part
    for target in range(8):
        for slot in range(2):
            out_ref[target, slot * 32 : slot * 32 + 32, :] = velocity[slot, target * 32 : target * 32 + 32, :]
        out_ref[target, 64:72, :] = lanes


def step_kernel(parts_ref, start_ref, rows_ref, mass_ref):
    blocks = start_ref.shape[1] // LANES
    total = parts_ref[0, 64:72, :]
    for source in range(1, 8):
        total = total + parts_ref[source, 64:72, :]
    mass = jnp.sum(total, axis=1, keepdims=True)
    lane = lax.broadcasted_iota(jnp.int32, (8, LANES), 1)
    latents = lax.broadcasted_iota(jnp.int32, (8, LANES), 0)
    line = jnp.sum(jnp.where(lane == latents, mass, 0.0), axis=0, keepdims=True)
    mass_ref[...] = jnp.broadcast_to(line, mass_ref.shape)
    velocity = [jnp.zeros((32, LANES), F32) for _ in range(blocks)]
    for source in range(8):
        for slot in range(2):
            o = first_block(source) + slot
            if o < blocks:
                velocity[o] = velocity[o] + parts_ref[source, slot * 32 : slot * 32 + 32, :]
    for o in range(blocks):
        rows_ref[:, lane_block(o)] = (start_ref[:, lane_block(o)] + 0.25 * velocity[o]).astype(BF16)


def final_kernel(scale, mass_ref, rows0, rows1, next_ref, out_ref, lines):
    blocks = lines.shape[0]
    total = jnp.sum(mass_ref[...], axis=0, keepdims=True)
    lane = lax.broadcasted_iota(jnp.int32, (1, LANES), 1)
    for b in range(4):
        out_ref[b] = scale * jnp.sum(jnp.where(lane == b, total, 0.0))
    for start, rows in ((half_rows(), rows0), (2 - half_rows(), rows1)):
        for o in range(blocks):
            lines[o] = rows[:, lane_block(o)].astype(F32)
        for o in range(blocks):
            for b in range(4):
                for r in range(2):
                    value = lines[o, pl.ds(r * 16 + b, 4, stride=4), :].astype(BF16)
                    next_ref[b, start + r, :, lane_block(o)] = value


def shape(dims, kind):
    return jax.ShapeDtypeStruct(dims, kind)


def body(state, probe_signs, timesteps, time_table, gn_gain, gn_shift, conv_weight, conv_bias):
    chans = state.shape[3]
    blocks = chans // LANES
    each = conv_weight.shape[1] * PAIRS
    params = pltpu.CompilerParams(vmem_limit_bytes=40 * 1024 * 1024)
    far = lambda array: pltpu.with_memory_space_constraint(array, pltpu.HBM)
    main, rim, base, wsend = pl.pallas_call(
        pack_kernel,
        out_shape=(
            shape((192, chans), BF16),
            shape((56, chans), BF16),
            shape((32, chans), F32),
            pltpu.HBM((32, each, LANES), BF16),
        ),
        in_specs=[HBM] * 3,
        out_specs=(VMEM,) * 3 + (HBM,),
        scratch_shapes=[
            pltpu.VMEM(conv_weight.shape, BF16),
            pltpu.VMEM(state.shape, BF16),
            pltpu.VMEM(probe_signs.shape, jnp.int32),
            pltpu.VMEM((blocks, 128, LANES), F32),
            pltpu.VMEM((blocks, 64, LANES), F32),
            pltpu.VMEM((each, LANES), F32),
            pltpu.VMEM((32, each, LANES), BF16),
            pltpu.VMEM((56, chans), F32),
            pltpu.VMEM((32, chans), F32),
            pltpu.SemaphoreType.DMA((3,)),
            pltpu.SemaphoreType.DMA,
        ],
        compiler_params=params,
        name="pack",
    )(far(conv_weight), far(state), far(probe_signs))
    offset, start = pl.pallas_call(
        lookup_kernel,
        out_shape=(shape((8, chans), F32), shape((32, chans), F32)),
        in_specs=[SMEM, HBM, VMEM, VMEM, VMEM],
        out_specs=(VMEM,) * 2,
        scratch_shapes=[pltpu.VMEM((4, 8, chans), F32), pltpu.SemaphoreType.DMA((4,))],
        compiler_params=params,
        name="lookup",
    )(timesteps, far(time_table), gn_shift[None], conv_bias[None], base)

    facing = lax.ppermute(rim, GX, [(1, 2), (2, 1)])
    outer = lax.ppermute(rim[48:56], GX, [(0, 3), (3, 0)])
    weights = lax.all_to_all(wsend, PROBE, 0, 0, tiled=True)
    block = jnp.concatenate([main, facing[:48], facing[48:] + outer, rim[48:56]], axis=0)
    down = [(i, (i + 1) % 4) for i in range(4)]
    up = [(i, (i + 3) % 4) for i in range(4)]
    above = lax.ppermute(block, "gy", down)
    below = lax.ppermute(block, "gy", up)
    onward = [(x * 2 + c, (x + 1 - 2 * c) % 4 * 2 + c) for x in range(4) for c in range(2)]
    beyond = lax.ppermute(jnp.where(lax.axis_index("gx_1") == 0, above, below), ("gy", "gx_1"), onward)
    own = [block, above, below, beyond]
    swap = [(0, 1), (1, 0)]
    other = [lax.ppermute(block, "gx_1", swap)]
    other += [lax.ppermute(tile, "gx_1", swap) for tile in own[1:]]

    partial = pl.pallas_call(
        mix_kernel,
        out_shape=shape((8, 72, LANES), F32),
        in_specs=[VMEM] * 8 + [HBM] + [VMEM] * 2,
        out_specs=VMEM,
        scratch_shapes=[
            pltpu.VMEM((blocks, 1440, LANES), F32),
            pltpu.VMEM((blocks, 720, LANES), F32),
            pltpu.VMEM((1024, PAIRS * LANES), BF16),
            pltpu.VMEM((1024, chans), F32),
            pltpu.VMEM((PAIRS * 256, chans), BF16),
            pltpu.VMEM((32, each, LANES), BF16),
            pltpu.VMEM((32 * each, LANES), F32),
            pltpu.VMEM((chans, PAIRS * LANES), BF16),
            pltpu.VMEM((2, 256, LANES), F32),
            pltpu.SemaphoreType.DMA,
        ],
        compiler_params=params,
        name="mix",
    )(*own, *other, far(weights), gn_gain[None], offset)

    partial = lax.all_to_all(partial, ("gy", "gx_1"), 0, 0, tiled=True)
    rows, mass = pl.pallas_call(
        step_kernel,
        out_shape=(shape((32, chans), BF16), shape((64, LANES), F32)),
        in_specs=[VMEM] * 2,
        out_specs=(VMEM,) * 2,
        compiler_params=params,
        name="step",
    )(partial, start)
    mass = lax.all_to_all(mass.reshape(64, 1, LANES), ("gx_0",) + PROBE, 0, 0, tiled=True)
    tall = lax.axis_size("probe_0")
    facing_rows = lax.ppermute(rows, "probe_0", [(y, y ^ 1) for y in range(tall)])
    scale = -0.25 / (probe_signs.shape[0] * lax.axis_size(PROBE))
    return pl.pallas_call(
        lambda *refs: final_kernel(scale, *refs),
        out_shape=(shape(state.shape, BF16), shape((4,), F32)),
        in_specs=[VMEM] * 3,
        out_specs=(VMEM, SMEM),
        scratch_shapes=[pltpu.VMEM((blocks, 32, LANES), F32)],
        compiler_params=params,
        name="final",
    )(mass.reshape(64, LANES), rows, facing_rows)


def solution(mesh):
    split = Mesh(
        mesh.devices.reshape(mesh.shape["gy"], 2, 2, 8, 4),
        ("gy", "gx_0", "gx_1", "probe_0", "probe_1"),
    )
    return jax.shard_map(
        body,
        mesh=split,
        in_specs=(
            P(None, "gy", GX, None),
            P(PROBE, None, "gy", GX, None),
            P(),
            P(),
            P(),
            P(),
            P(None, PROBE, None),
            P(),
        ),
        out_specs=(P(None, "gy", GX, None), P()),
        check_vma=False,
    )
```

```python
import jax
import jax.numpy as jnp
from jax import lax
from jax.experimental import pallas as pl
from jax.experimental.pallas import tpu as pltpu
from jax.sharding import Mesh
from jax.sharding import PartitionSpec as P


GROUPS = 32
GX = ("gx_0", "gx_1")
PROBE = ("probe_0", "probe_1")
LANES = 128
PAIRS = 6
F32 = jnp.float32
BF16 = jnp.bfloat16
VMEM = pl.BlockSpec(memory_space=pltpu.VMEM)
SMEM = pl.BlockSpec(memory_space=pltpu.SMEM)
HBM = pl.BlockSpec(memory_space=pltpu.HBM)


def three_parts(value):
    high = value.astype(BF16)
    rest = value - high.astype(F32)
    mid = rest.astype(BF16)
    low = (rest - mid.astype(F32)).astype(BF16)
    return high, mid, low


def lane_block(index):
    return slice(index * LANES, (index + 1) * LANES)


def doubled_rows(rows):
    turned = pltpu.roll(rows, 4, axis=0)
    upper = lax.broadcasted_iota(jnp.int32, rows.shape, 0) < 4
    return jnp.where(upper, rows, turned), jnp.where(upper, turned, rows)


def half_rows():
    return 2 * lax.rem(lax.axis_index("probe_0"), 2)


def first_block(member):
    return member * PAIRS // 9


def pair_of(index):
    member = lax.axis_index("gy") * 2 + lax.axis_index("gx_1")
    number = member * PAIRS + index
    return lax.rem(number, 9), lax.div(number, 9)


def lookup_kernel(step_ref, table_hbm, shift_ref, bias_ref, base_ref, offset_ref, start_ref, table, found):
    steps = [step_ref[b] for b in range(4)]
    finds = [
        pltpu.make_async_copy(
            table_hbm.at[pl.ds(pl.multiple_of(lax.div(steps[b], 8) * 8, 8), 8), :], table.at[b], found.at[b]
        )
        for b in range(4)
    ]
    for find in finds:
        find.start()
    start_ref[...] = base_ref[...] + 0.25 * bias_ref[...]
    for b in range(4):
        finds[b].wait()
        line = table[b, pl.ds(lax.rem(steps[b], 8), 1), :] + shift_ref[...]
        offset_ref[b : b + 1, :] = line
        offset_ref[b + 4 : b + 5, :] = line


def pack_kernel(
    weight_hbm, state_hbm, signs_hbm, main_ref, rim_ref, base_ref, wsend_hbm,
    weight_ref, state_ref, signs_ref, uf, xf, wf, wsend_ref, rim, sums, arrived, left,
):
    blocks = uf.shape[0]
    loads = [
        pltpu.make_async_copy(src, dst, arrived.at[index])
        for index, (src, dst) in enumerate(
            ((weight_hbm, weight_ref), (state_hbm, state_ref), (signs_hbm, signs_ref))
        )
    ]
    for load in loads:
        load.start()
    loads[0].wait()
    for index in range(PAIRS):
        tap, ob = pair_of(index)
        rows = weight_ref[tap].astype(F32)
        picked = jnp.zeros((rows.shape[0], LANES), F32)
        for o in range(blocks):
            picked = picked + jnp.where(ob == o, rows[:, lane_block(o)], 0.0)
        wf[pl.ds(index, rows.shape[0], stride=PAIRS), :] = picked
    packed = wf[...].astype(BF16)
    for target in range(wsend_ref.shape[0]):
        wsend_ref[target] = packed
    leave = pltpu.make_async_copy(wsend_ref, wsend_hbm, left)
    leave.start()
    loads[1].wait()
    loads[2].wait()
    for p in range(2):
        for b in range(4):
            for r in range(4):
                line = signs_ref[p, b, r].astype(F32)
                for o in range(blocks):
                    uf[o, pl.ds(r * 32 + p * 4 + b, 4, stride=8), :] = line[:, lane_block(o)]
    for b in range(4):
        for r in range(4):
            line = state_ref[b, r].astype(F32)
            for o in range(blocks):
                xf[o, pl.ds(r * 16 + b, 4, stride=4), :] = line[:, lane_block(o)]

    for o in range(blocks):
        base_ref[:, lane_block(o)] = xf[o, pl.ds(pl.multiple_of(half_rows() * 16, 8), 32), :]
    edge = jnp.where(lax.axis_index("gx_0") == 0, 3, 0)
    for o in range(blocks):
        sum_u = jnp.zeros((8, LANES), F32)
        cross = jnp.zeros((8, LANES), F32)
        sum_x = jnp.zeros((8, LANES), F32)
        sum_xx = jnp.zeros((8, LANES), F32)
        for two in range(8):
            pair = doubled_rows(xf[o, two * 8 : two * 8 + 8, :])
            for half in range(2):
                cell = two * 2 + half
                x = pair[half]
                u = uf[o, cell * 8 : cell * 8 + 8, :]
                sum_u, cross = sum_u + u, cross + u * x
                sum_x, sum_xx = sum_x + x, sum_xx + x * x
        for kind, part in enumerate((sum_u, cross, sum_x, sum_xx)):
            sums[kind * 8 : kind * 8 + 8, lane_block(o)] = part
        for r in range(4):
            rim[r * 8 : r * 8 + 8, lane_block(o)] = uf[o, pl.ds(pl.multiple_of((r * 4 + edge) * 8, 8), 8), :]
            rim[32 + r * 4 : 36 + r * 4, lane_block(o)] = xf[o, pl.ds((r * 4 + edge) * 4, 4), :]

    width = sums.shape[1] // GROUPS
    row = lax.broadcasted_iota(jnp.int32, (sums.shape[1], LANES), 0)
    first = lax.broadcasted_iota(jnp.int32, (sums.shape[1], LANES), 1) * width
    member = jnp.where((row >= first) & (row < first + width), 1.0, 0.0).astype(BF16)
    grouped = jnp.zeros((32, LANES), F32)
    for part in three_parts(sums[...]):
        grouped = grouped + jnp.dot(part, member, preferred_element_type=F32)
    stats = grouped[0:8]
    for kind in range(1, 4):
        stats = stats + pltpu.roll(grouped[kind * 8 : kind * 8 + 8], GROUPS * kind, axis=1)
    rim[48:56, :] = jnp.zeros((8, rim.shape[1]), F32)
    for index, part in enumerate(three_parts(stats)):
        rim[48:56, lane_block(index)] = part.astype(F32)

    for o in range(blocks):
        main_ref[0:128, lane_block(o)] = uf[o].astype(BF16)
        main_ref[128:192, lane_block(o)] = xf[o].astype(BF16)
    rim_ref[...] = rim[...].astype(BF16)
    leave.wait()


def mix_kernel(
    own0, own1, own3, own2, other0, other1, other3, other2, weight_hbm, gain_ref, offset_ref,
    out_ref, ug, xg, edges, lhs_ref, slope_ref, rows_ref, weight_ref, wf, wc, velocity, arrived,
):
    load = pltpu.make_async_copy(weight_hbm, weight_ref, arrived)
    load.start()
    blocks = ug.shape[0]
    core = lax.axis_index("gx_1")
    half = lax.axis_index("gx_0")
    chans = own0.shape[1]

    def spot(row, col):
        return pl.multiple_of((row * 10 + col) * 8, 8)

    def small(row, col):
        return pl.multiple_of((row * 10 + col) * 4, 4)

    for o in range(blocks):
        for row in (0, 17):
            ug[o, row * 80 : row * 80 + 80, :] = jnp.zeros((80, LANES), F32)
            xg[o, row * 40 : row * 40 + 40, :] = jnp.zeros((40, LANES), F32)
        for row in range(1, 17):
            for col in (0, 9):
                ug[o, row * 80 + col * 8 : row * 80 + col * 8 + 8, :] = jnp.zeros((8, LANES), F32)
                xg[o, row * 40 + col * 4 : row * 40 + col * 4 + 4, :] = jnp.zeros((4, LANES), F32)

    total = jnp.zeros((8, chans), F32)
    rim_here = core == 1 - half
    rim_col = jnp.where(half == 0, 9, 0)
    sources = ((0, own0, other0), (1, own1, other1), (3, own3, other3), (2, own2, other2))
    for back, own_ref, other_ref in sources:
        tile = lax.rem(lax.axis_index("gy") + 4 - back, 4)
        for src, base in ((own_ref, 4 * core), (other_ref, 4 * (1 - core))):
            for r in range(4):
                at = spot(4 * tile + r + 1, base + 1)
                lines = src[r * 32 : r * 32 + 32, :].astype(F32)
                states = src[128 + r * 16 : 144 + r * 16, :].astype(F32)
                for o in range(blocks):
                    ug[o, pl.ds(at, 32), :] = lines[:, lane_block(o)]
                    xg[o, pl.ds(small(4 * tile + r + 1, base + 1), 16), :] = states[:, lane_block(o)]
        mine = own_ref[192:256, :].astype(F32)
        theirs = other_ref[192:256, :].astype(F32)
        total = total + mine[48:56] + mine[56:64] + theirs[48:56] + theirs[56:64]
        rim = jnp.where(rim_here, mine[0:48], theirs[0:48])
        for r in range(4):
            at = spot(4 * tile + r + 1, rim_col)
            for o in range(blocks):
                ug[o, pl.ds(at, 8), :] = rim[r * 8 : r * 8 + 8, lane_block(o)]
        for o in range(blocks):
            edges[o, pl.ds(pl.multiple_of(tile * 16, 16), 16), :] = rim[32:48, lane_block(o)]

    stats = total[:, lane_block(0)] + total[:, lane_block(1)] + total[:, lane_block(2)]
    width = chans // GROUPS
    lane = lax.broadcasted_iota(jnp.int32, (LANES, chans), 1)
    first = lax.broadcasted_iota(jnp.int32, (LANES, chans), 0) * width
    spread = jnp.where((lane >= first) & (lane < first + width), 1.0, 0.0).astype(BF16)

    def expanded(kind):
        turned = stats if kind == 0 else pltpu.roll(stats, LANES - GROUPS * kind, axis=1)
        out = jnp.zeros((8, chans), F32)
        for part in three_parts(turned):
            out = out + jnp.dot(part, spread, preferred_element_type=F32)
        return out

    count = 256 * width
    sum_u, cross, sum_x, sum_xx = (expanded(kind) for kind in range(4))
    mean = sum_x / count
    sigma = jnp.sqrt(sum_xx / count - mean * mean + 1e-05)
    inverse = 1.0 / sigma
    mean_u = sum_u / count
    mean_cu = (cross - mean * sum_u) / count
    bend = mean_cu / (sigma * sigma * sigma)
    offset = offset_ref[...]
    gain = gain_ref[...]

    scale = inverse * gain
    tilt = gain * inverse

    def fields(x, o, rows):
        at = lane_block(o)
        centered = x - mean[:rows, at]
        pre = centered * scale[:rows, at] + offset[:rows, at]
        sig = 0.5 + 0.5 * jnp.tanh(0.5 * pre)
        return centered, pre, sig

    def grid_row(gr, carry):
        at = spot(gr + 1, 1)
        near = small(gr + 1, 1)
        for o in range(blocks):
            ln = lane_block(o)
            x = xg[o, pl.ds(near, 32), :].reshape(4, 8, LANES)
            centered, pre, sig = fields(x, o, 8)
            xg[o, pl.ds(near, 32), :] = (pre * sig).reshape(32, LANES)
            slope = sig * (1.0 + pre * (1.0 - sig))
            along = slope * tilt[:, ln]
            across = slope * gain[:, ln] * centered
            for two in range(4):
                spans = zip(doubled_rows(along[two]), doubled_rows(across[two]))
                cells = []
                for half_cell, (first, second) in enumerate(spans):
                    u = ug[o, pl.ds(pl.multiple_of(at + (two * 2 + half_cell) * 8, 8), 8), :]
                    cells.append(first * (u - mean_u[:, ln]) - second * bend[:, ln])
                out = jnp.concatenate(cells, axis=0).astype(BF16)
                slope_ref[pl.ds(pl.multiple_of(gr * 64 + two * 16, 16), 16), ln] = out
        return carry

    lax.fori_loop(0, 16, grid_row, 0)

    for o in range(blocks):
        _, pre, sig = fields(edges[o].reshape(8, 8, LANES), o, 8)
        edges[o] = (pre * sig).reshape(64, LANES)
        for row in range(16):
            xg[o, pl.ds(small(row + 1, rim_col), 4), :] = edges[o, row * 4 : row * 4 + 4, :]

    taps = [pair_of(index) for index in range(PAIRS)]

    def lhs_row(gr, carry):
        for index, (tap, ob) in enumerate(taps):
            dy, dx = lax.div(tap, 3), lax.rem(tap, 3)
            at = spot(gr + 2 - dy, 2 - dx)
            value = ug[jnp.minimum(ob, blocks - 1), pl.ds(at, 64), :]
            lhs_ref[pl.ds(pl.multiple_of(gr * 64, 64), 64), lane_block(index)] = value.astype(BF16)
        return carry

    lax.fori_loop(0, 16, lhs_row, 0)

    for index, (tap, ob) in enumerate(taps):
        dy, dx = lax.div(tap, 3), lax.rem(tap, 3)
        for target in range(8):
            for line in range(2):
                at = small(4 * (target // 2) + half_rows() + line + dy, 4 * (target % 2) + dx)
                to = index * 256 + target * 32 + line * 16
                for o in range(blocks):
                    rows_ref[to : to + 16, lane_block(o)] = xg[o, pl.ds(at, 16), :].astype(BF16)

    load.wait()
    each = weight_ref.shape[1]
    for source in range(weight_ref.shape[0]):
        wf[source * each : (source + 1) * each, :] = weight_ref[source].astype(F32)
    for index in range(PAIRS):
        wc[:, lane_block(index)] = wf[pl.ds(index, chans, stride=PAIRS), :].astype(BF16)

    chunk = 512
    total = jnp.zeros((8, chans), F32)
    for start in range(0, lhs_ref.shape[0], chunk):
        value = lax.dot_general(
            lhs_ref[start : start + chunk, :], wc[...], (((1,), (1,)), ((), ())), preferred_element_type=F32
        )
        value = value * slope_ref[start : start + chunk, :].astype(F32)
        total = total + jnp.sum(value.reshape(chunk // 8, 8, chans), axis=0)
    lanes = total[:, lane_block(0)]
    for o in range(1, blocks):
        lanes = lanes + total[:, lane_block(o)]
    lanes = lanes + pltpu.roll(lanes, 4, axis=0)

    velocity[...] = jnp.zeros(velocity.shape, F32)
    for index in range(PAIRS):
        slot = taps[index][1] - lax.div((lax.axis_index("gy") * 2 + lax.axis_index("gx_1")) * PAIRS, 9)
        part = jnp.dot(
            rows_ref[index * 256 : index * 256 + 256, :], wc[:, lane_block(index)], preferred_element_type=F32
        )
        velocity[slot] = velocity[slot] + part
    for target in range(8):
        for slot in range(2):
            out_ref[target, slot * 32 : slot * 32 + 32, :] = velocity[slot, target * 32 : target * 32 + 32, :]
        out_ref[target, 64:72, :] = lanes


def step_kernel(parts_ref, start_ref, rows_ref, mass_ref):
    blocks = start_ref.shape[1] // LANES
    total = parts_ref[0, 64:72, :]
    for source in range(1, 8):
        total = total + parts_ref[source, 64:72, :]
    mass = jnp.sum(total, axis=1, keepdims=True)
    lane = lax.broadcasted_iota(jnp.int32, (8, LANES), 1)
    latents = lax.broadcasted_iota(jnp.int32, (8, LANES), 0)
    line = jnp.sum(jnp.where(lane == latents, mass, 0.0), axis=0, keepdims=True)
    mass_ref[...] = jnp.broadcast_to(line, mass_ref.shape)
    velocity = [jnp.zeros((32, LANES), F32) for _ in range(blocks)]
    for source in range(8):
        for slot in range(2):
            o = first_block(source) + slot
            if o < blocks:
                velocity[o] = velocity[o] + parts_ref[source, slot * 32 : slot * 32 + 32, :]
    for o in range(blocks):
        rows_ref[:, lane_block(o)] = (start_ref[:, lane_block(o)] + 0.25 * velocity[o]).astype(BF16)


def final_kernel(scale, mass_ref, rows0, rows1, next_ref, out_ref, lines):
    blocks = lines.shape[0]
    total = jnp.sum(mass_ref[...], axis=0, keepdims=True)
    lane = lax.broadcasted_iota(jnp.int32, (1, LANES), 1)
    for b in range(4):
        out_ref[b] = scale * jnp.sum(jnp.where(lane == b, total, 0.0))
    for start, rows in ((half_rows(), rows0), (2 - half_rows(), rows1)):
        for o in range(blocks):
            lines[o] = rows[:, lane_block(o)].astype(F32)
        for o in range(blocks):
            for b in range(4):
                for r in range(2):
                    value = lines[o, pl.ds(r * 16 + b, 4, stride=4), :].astype(BF16)
                    next_ref[b, start + r, :, lane_block(o)] = value


def shape(dims, kind):
    return jax.ShapeDtypeStruct(dims, kind)


def body(state, probe_signs, timesteps, time_table, gn_gain, gn_shift, conv_weight, conv_bias):
    chans = state.shape[3]
    blocks = chans // LANES
    each = conv_weight.shape[1] * PAIRS
    params = pltpu.CompilerParams(vmem_limit_bytes=40 * 1024 * 1024)
    far = lambda array: pltpu.with_memory_space_constraint(array, pltpu.HBM)
    main, rim, base, wsend = pl.pallas_call(
        pack_kernel,
        out_shape=(
            shape((192, chans), BF16),
            shape((56, chans), BF16),
            shape((32, chans), F32),
            pltpu.HBM((32, each, LANES), BF16),
        ),
        in_specs=[HBM] * 3,
        out_specs=(VMEM,) * 3 + (HBM,),
        scratch_shapes=[
            pltpu.VMEM(conv_weight.shape, BF16),
            pltpu.VMEM(state.shape, BF16),
            pltpu.VMEM(probe_signs.shape, jnp.int32),
            pltpu.VMEM((blocks, 128, LANES), F32),
            pltpu.VMEM((blocks, 64, LANES), F32),
            pltpu.VMEM((each, LANES), F32),
            pltpu.VMEM((32, each, LANES), BF16),
            pltpu.VMEM((56, chans), F32),
            pltpu.VMEM((32, chans), F32),
            pltpu.SemaphoreType.DMA((3,)),
            pltpu.SemaphoreType.DMA,
        ],
        compiler_params=params,
        name="pack",
    )(far(conv_weight), far(state), far(probe_signs))
    offset, start = pl.pallas_call(
        lookup_kernel,
        out_shape=(shape((8, chans), F32), shape((32, chans), F32)),
        in_specs=[SMEM, HBM, VMEM, VMEM, VMEM],
        out_specs=(VMEM,) * 2,
        scratch_shapes=[pltpu.VMEM((4, 8, chans), F32), pltpu.SemaphoreType.DMA((4,))],
        compiler_params=params,
        name="lookup",
    )(timesteps, far(time_table), gn_shift[None], conv_bias[None], base)

    facing = lax.ppermute(rim, GX, [(1, 2), (2, 1)])
    outer = lax.ppermute(rim[48:56], GX, [(0, 3), (3, 0)])
    weights = lax.all_to_all(wsend, PROBE, 0, 0, tiled=True)
    block = jnp.concatenate([main, facing[:48], facing[48:] + outer, rim[48:56]], axis=0)
    down = [(i, (i + 1) % 4) for i in range(4)]
    up = [(i, (i + 3) % 4) for i in range(4)]
    above = lax.ppermute(block, "gy", down)
    below = lax.ppermute(block, "gy", up)
    onward = [(x * 2 + c, (x + 1 - 2 * c) % 4 * 2 + c) for x in range(4) for c in range(2)]
    beyond = lax.ppermute(jnp.where(lax.axis_index("gx_1") == 0, above, below), ("gy", "gx_1"), onward)
    own = [block, above, below, beyond]
    swap = [(0, 1), (1, 0)]
    other = [lax.ppermute(block, "gx_1", swap)]
    other += [lax.ppermute(tile, "gx_1", swap) for tile in own[1:]]

    partial = pl.pallas_call(
        mix_kernel,
        out_shape=shape((8, 72, LANES), F32),
        in_specs=[VMEM] * 8 + [HBM] + [VMEM] * 2,
        out_specs=VMEM,
        scratch_shapes=[
            pltpu.VMEM((blocks, 1440, LANES), F32),
            pltpu.VMEM((blocks, 720, LANES), F32),
            pltpu.VMEM((blocks, 64, LANES), F32),
            pltpu.VMEM((1024, PAIRS * LANES), BF16),
            pltpu.VMEM((1024, chans), BF16),
            pltpu.VMEM((PAIRS * 256, chans), BF16),
            pltpu.VMEM((32, each, LANES), BF16),
            pltpu.VMEM((32 * each, LANES), F32),
            pltpu.VMEM((chans, PAIRS * LANES), BF16),
            pltpu.VMEM((2, 256, LANES), F32),
            pltpu.SemaphoreType.DMA,
        ],
        compiler_params=params,
        name="mix",
    )(*own, *other, far(weights), gn_gain[None], offset)

    partial = lax.all_to_all(partial, ("gy", "gx_1"), 0, 0, tiled=True)
    rows, mass = pl.pallas_call(
        step_kernel,
        out_shape=(shape((32, chans), BF16), shape((64, LANES), F32)),
        in_specs=[VMEM] * 2,
        out_specs=(VMEM,) * 2,
        compiler_params=params,
        name="step",
    )(partial, start)
    mass = lax.all_to_all(mass.reshape(64, 1, LANES), ("gx_0",) + PROBE, 0, 0, tiled=True)
    tall = lax.axis_size("probe_0")
    facing_rows = lax.ppermute(rows, "probe_0", [(y, y ^ 1) for y in range(tall)])
    scale = -0.25 / (probe_signs.shape[0] * lax.axis_size(PROBE))
    return pl.pallas_call(
        lambda *refs: final_kernel(scale, *refs),
        out_shape=(shape(state.shape, BF16), shape((4,), F32)),
        in_specs=[VMEM] * 3,
        out_specs=(VMEM, SMEM),
        scratch_shapes=[pltpu.VMEM((blocks, 32, LANES), F32)],
        compiler_params=params,
        name="final",
    )(mass.reshape(64, LANES), rows, facing_rows)


def solution(mesh):
    split = Mesh(
        mesh.devices.reshape(mesh.shape["gy"], 2, 2, 8, 4),
        ("gy", "gx_0", "gx_1", "probe_0", "probe_1"),
    )
    return jax.shard_map(
        body,
        mesh=split,
        in_specs=(
            P(None, "gy", GX, None),
            P(PROBE, None, "gy", GX, None),
            P(),
            P(),
            P(),
            P(),
            P(None, PROBE, None),
            P(),
        ),
        out_specs=(P(None, "gy", GX, None), P()),
        check_vma=False,
    )
```

```python
import jax
import jax.numpy as jnp
from jax import lax
from jax.experimental import pallas as pl
from jax.experimental.pallas import tpu as pltpu
from jax.sharding import Mesh
from jax.sharding import PartitionSpec as P


GROUPS = 32
GX = ("gx_0", "gx_1")
PROBE = ("probe_0", "probe_1")
LANES = 128
PAIRS = 6
F32 = jnp.float32
BF16 = jnp.bfloat16
VMEM = pl.BlockSpec(memory_space=pltpu.VMEM)
SMEM = pl.BlockSpec(memory_space=pltpu.SMEM)
HBM = pl.BlockSpec(memory_space=pltpu.HBM)


def three_parts(value):
    high = value.astype(BF16)
    rest = value - high.astype(F32)
    mid = rest.astype(BF16)
    low = (rest - mid.astype(F32)).astype(BF16)
    return high, mid, low


def lane_block(index):
    return slice(index * LANES, (index + 1) * LANES)


def doubled_rows(rows):
    turned = pltpu.roll(rows, 4, axis=0)
    upper = lax.broadcasted_iota(jnp.int32, rows.shape, 0) < 4
    return jnp.where(upper, rows, turned), jnp.where(upper, turned, rows)


def half_rows():
    return 2 * lax.rem(lax.axis_index("probe_0"), 2)


def first_block(member):
    return member * PAIRS // 9


def pair_of(index):
    member = lax.axis_index("gy") * 2 + lax.axis_index("gx_1")
    number = member * PAIRS + index
    return lax.rem(number, 9), lax.div(number, 9)


def lookup_kernel(step_ref, table_hbm, shift_ref, bias_ref, base_ref, offset_ref, start_ref, table, found):
    steps = [step_ref[b] for b in range(4)]
    finds = [
        pltpu.make_async_copy(
            table_hbm.at[pl.ds(pl.multiple_of(lax.div(steps[b], 8) * 8, 8), 8), :], table.at[b], found.at[b]
        )
        for b in range(4)
    ]
    for find in finds:
        find.start()
    start_ref[...] = base_ref[...] + 0.25 * bias_ref[...]
    for b in range(4):
        finds[b].wait()
        line = table[b, pl.ds(lax.rem(steps[b], 8), 1), :] + shift_ref[...]
        offset_ref[b : b + 1, :] = line
        offset_ref[b + 4 : b + 5, :] = line


def pack_kernel(
    weight_hbm, state_hbm, signs_hbm, main_ref, rim_ref, base_ref, wsend_hbm,
    weight_ref, state_ref, signs_ref, uf, xf, wf, wsend_ref, rim, sums, arrived, left,
):
    blocks = uf.shape[0]
    loads = [
        pltpu.make_async_copy(src, dst, arrived.at[index])
        for index, (src, dst) in enumerate(
            ((weight_hbm, weight_ref), (state_hbm, state_ref), (signs_hbm, signs_ref))
        )
    ]
    for load in loads:
        load.start()
    loads[0].wait()
    for index in range(PAIRS):
        tap, ob = pair_of(index)
        rows = weight_ref[tap].astype(F32)
        picked = jnp.zeros((rows.shape[0], LANES), F32)
        for o in range(blocks):
            picked = picked + jnp.where(ob == o, rows[:, lane_block(o)], 0.0)
        wf[pl.ds(index, rows.shape[0], stride=PAIRS), :] = picked
    packed = wf[...].astype(BF16)
    for target in range(wsend_ref.shape[0]):
        wsend_ref[target] = packed
    leave = pltpu.make_async_copy(wsend_ref, wsend_hbm, left)
    leave.start()
    loads[1].wait()
    loads[2].wait()
    for p in range(2):
        for b in range(4):
            for r in range(4):
                line = signs_ref[p, b, r].astype(F32)
                for o in range(blocks):
                    uf[o, pl.ds(r * 32 + p * 4 + b, 4, stride=8), :] = line[:, lane_block(o)]
    for b in range(4):
        for r in range(4):
            line = state_ref[b, r].astype(F32)
            for o in range(blocks):
                xf[o, pl.ds(r * 16 + b, 4, stride=4), :] = line[:, lane_block(o)]

    for o in range(blocks):
        base_ref[:, lane_block(o)] = xf[o, pl.ds(pl.multiple_of(half_rows() * 16, 8), 32), :]
    edge = jnp.where(lax.axis_index("gx_0") == 0, 3, 0)
    for o in range(blocks):
        sum_u = jnp.zeros((8, LANES), F32)
        cross = jnp.zeros((8, LANES), F32)
        sum_x = jnp.zeros((8, LANES), F32)
        sum_xx = jnp.zeros((8, LANES), F32)
        for two in range(8):
            pair = doubled_rows(xf[o, two * 8 : two * 8 + 8, :])
            for half in range(2):
                cell = two * 2 + half
                x = pair[half]
                u = uf[o, cell * 8 : cell * 8 + 8, :]
                sum_u, cross = sum_u + u, cross + u * x
                sum_x, sum_xx = sum_x + x, sum_xx + x * x
        for kind, part in enumerate((sum_u, cross, sum_x, sum_xx)):
            sums[kind * 8 : kind * 8 + 8, lane_block(o)] = part
        for r in range(4):
            rim[r * 8 : r * 8 + 8, lane_block(o)] = uf[o, pl.ds(pl.multiple_of((r * 4 + edge) * 8, 8), 8), :]
            rim[32 + r * 4 : 36 + r * 4, lane_block(o)] = xf[o, pl.ds((r * 4 + edge) * 4, 4), :]

    width = sums.shape[1] // GROUPS
    row = lax.broadcasted_iota(jnp.int32, (sums.shape[1], LANES), 0)
    first = lax.broadcasted_iota(jnp.int32, (sums.shape[1], LANES), 1) * width
    member = jnp.where((row >= first) & (row < first + width), 1.0, 0.0).astype(BF16)
    grouped = jnp.zeros((32, LANES), F32)
    for part in three_parts(sums[...]):
        grouped = grouped + jnp.dot(part, member, preferred_element_type=F32)
    stats = grouped[0:8]
    for kind in range(1, 4):
        stats = stats + pltpu.roll(grouped[kind * 8 : kind * 8 + 8], GROUPS * kind, axis=1)
    rim[48:56, :] = jnp.zeros((8, rim.shape[1]), F32)
    for index, part in enumerate(three_parts(stats)):
        rim[48:56, lane_block(index)] = part.astype(F32)

    for o in range(blocks):
        main_ref[0:128, lane_block(o)] = uf[o].astype(BF16)
        main_ref[128:192, lane_block(o)] = xf[o].astype(BF16)
    rim_ref[...] = rim[...].astype(BF16)
    leave.wait()


def mix_kernel(
    own0, own1, own3, own2, other0, other1, other3, other2, weight_hbm, gain_ref, offset_ref,
    out_ref, ug, xg, edges, lhs_ref, slope_ref, rows_ref, weight_ref, wf, wc, velocity, arrived,
):
    load = pltpu.make_async_copy(weight_hbm, weight_ref, arrived)
    load.start()
    blocks = ug.shape[0]
    core = lax.axis_index("gx_1")
    half = lax.axis_index("gx_0")
    chans = own0.shape[1]

    def spot(row, col):
        return pl.multiple_of((row * 10 + col) * 8, 8)

    def small(row, col):
        return pl.multiple_of((row * 10 + col) * 4, 4)

    for o in range(blocks):
        for row in (0, 17):
            ug[o, row * 80 : row * 80 + 80, :] = jnp.zeros((80, LANES), F32)
            xg[o, row * 40 : row * 40 + 40, :] = jnp.zeros((40, LANES), F32)
        for row in range(1, 17):
            for col in (0, 9):
                ug[o, row * 80 + col * 8 : row * 80 + col * 8 + 8, :] = jnp.zeros((8, LANES), F32)
                xg[o, row * 40 + col * 4 : row * 40 + col * 4 + 4, :] = jnp.zeros((4, LANES), F32)

    total = jnp.zeros((8, chans), F32)
    rim_here = core == 1 - half
    rim_col = jnp.where(half == 0, 9, 0)
    sources = ((0, own0, other0), (1, own1, other1), (3, own3, other3), (2, own2, other2))
    for back, own_ref, other_ref in sources:
        tile = lax.rem(lax.axis_index("gy") + 4 - back, 4)
        for src, base in ((own_ref, 4 * core), (other_ref, 4 * (1 - core))):
            for r in range(4):
                at = spot(4 * tile + r + 1, base + 1)
                lines = src[r * 32 : r * 32 + 32, :].astype(F32)
                states = src[128 + r * 16 : 144 + r * 16, :].astype(F32)
                for o in range(blocks):
                    ug[o, pl.ds(at, 32), :] = lines[:, lane_block(o)]
                    xg[o, pl.ds(small(4 * tile + r + 1, base + 1), 16), :] = states[:, lane_block(o)]
        mine = own_ref[192:256, :].astype(F32)
        theirs = other_ref[192:256, :].astype(F32)
        total = total + mine[48:56] + mine[56:64] + theirs[48:56] + theirs[56:64]
        rim = jnp.where(rim_here, mine[0:48], theirs[0:48])
        for r in range(4):
            at = spot(4 * tile + r + 1, rim_col)
            for o in range(blocks):
                ug[o, pl.ds(at, 8), :] = rim[r * 8 : r * 8 + 8, lane_block(o)]
        for o in range(blocks):
            edges[o, pl.ds(pl.multiple_of(tile * 16, 16), 16), :] = rim[32:48, lane_block(o)]

    stats = total[:, lane_block(0)] + total[:, lane_block(1)] + total[:, lane_block(2)]
    width = chans // GROUPS
    lane = lax.broadcasted_iota(jnp.int32, (LANES, chans), 1)
    first = lax.broadcasted_iota(jnp.int32, (LANES, chans), 0) * width
    spread = jnp.where((lane >= first) & (lane < first + width), 1.0, 0.0).astype(BF16)

    def expanded(kind):
        turned = stats if kind == 0 else pltpu.roll(stats, LANES - GROUPS * kind, axis=1)
        out = jnp.zeros((8, chans), F32)
        for part in three_parts(turned):
            out = out + jnp.dot(part, spread, preferred_element_type=F32)
        return out

    count = 256 * width
    sum_u, cross, sum_x, sum_xx = (expanded(kind) for kind in range(4))
    mean = sum_x / count
    sigma = jnp.sqrt(sum_xx / count - mean * mean + 1e-05)
    inverse = 1.0 / sigma
    mean_u = sum_u / count
    mean_cu = (cross - mean * sum_u) / count
    bend = mean_cu / (sigma * sigma * sigma)
    offset = offset_ref[...]
    gain = gain_ref[...]

    scale = inverse * gain
    tilt = gain * inverse

    def fields(x, o, rows):
        at = lane_block(o)
        centered = x - mean[:rows, at]
        pre = centered * scale[:rows, at] + offset[:rows, at]
        sig = 0.5 + 0.5 * jnp.tanh(0.5 * pre)
        return centered, pre, sig

    def grid_row(gr, carry):
        at = spot(gr + 1, 1)
        near = small(gr + 1, 1)
        for o in range(blocks):
            ln = lane_block(o)
            x = xg[o, pl.ds(near, 32), :].reshape(4, 8, LANES)
            centered, pre, sig = fields(x, o, 8)
            xg[o, pl.ds(near, 32), :] = (pre * sig).reshape(32, LANES)
            slope = sig * (1.0 + pre * (1.0 - sig))
            along = slope * tilt[:, ln]
            across = slope * gain[:, ln] * centered
            for two in range(4):
                spans = zip(doubled_rows(along[two]), doubled_rows(across[two]))
                cells = []
                for half_cell, (first, second) in enumerate(spans):
                    u = ug[o, pl.ds(pl.multiple_of(at + (two * 2 + half_cell) * 8, 8), 8), :]
                    cells.append(first * (u - mean_u[:, ln]) - second * bend[:, ln])
                out = jnp.concatenate(cells, axis=0).astype(BF16)
                slope_ref[pl.ds(pl.multiple_of(gr * 64 + two * 16, 16), 16), ln] = out
        return carry

    lax.fori_loop(0, 16, grid_row, 0)

    for o in range(blocks):
        _, pre, sig = fields(edges[o].reshape(8, 8, LANES), o, 8)
        edges[o] = (pre * sig).reshape(64, LANES)
        for row in range(16):
            xg[o, pl.ds(small(row + 1, rim_col), 4), :] = edges[o, row * 4 : row * 4 + 4, :]

    taps = [pair_of(index) for index in range(PAIRS)]

    def lhs_row(gr, carry):
        for index, (tap, ob) in enumerate(taps):
            dy, dx = lax.div(tap, 3), lax.rem(tap, 3)
            at = spot(gr + 2 - dy, 2 - dx)
            value = ug[jnp.minimum(ob, blocks - 1), pl.ds(at, 64), :]
            lhs_ref[pl.ds(pl.multiple_of(gr * 64, 64), 64), lane_block(index)] = value.astype(BF16)
        return carry

    lax.fori_loop(0, 16, lhs_row, 0)

    for index, (tap, ob) in enumerate(taps):
        dy, dx = lax.div(tap, 3), lax.rem(tap, 3)
        for target in range(8):
            for line in range(2):
                at = small(4 * (target // 2) + half_rows() + line + dy, 4 * (target % 2) + dx)
                to = index * 256 + target * 32 + line * 16
                for o in range(blocks):
                    rows_ref[to : to + 16, lane_block(o)] = xg[o, pl.ds(at, 16), :].astype(BF16)

    load.wait()
    each = weight_ref.shape[1]
    for source in range(weight_ref.shape[0]):
        wf[source * each : (source + 1) * each, :] = weight_ref[source].astype(F32)
    for index in range(PAIRS):
        wc[:, lane_block(index)] = wf[pl.ds(index, chans, stride=PAIRS), :].astype(BF16)

    chunk = 512
    total = jnp.zeros((8, chans), F32)
    for start in range(0, lhs_ref.shape[0], chunk):
        value = lax.dot_general(
            lhs_ref[start : start + chunk, :], wc[...], (((1,), (1,)), ((), ())), preferred_element_type=F32
        )
        value = value * slope_ref[start : start + chunk, :].astype(F32)
        total = total + jnp.sum(value.reshape(chunk // 8, 8, chans), axis=0)
    lanes = total[:, lane_block(0)]
    for o in range(1, blocks):
        lanes = lanes + total[:, lane_block(o)]
    lanes = lanes + pltpu.roll(lanes, 4, axis=0)

    velocity[...] = jnp.zeros(velocity.shape, F32)
    for index in range(PAIRS):
        slot = taps[index][1] - lax.div((lax.axis_index("gy") * 2 + lax.axis_index("gx_1")) * PAIRS, 9)
        part = jnp.dot(
            rows_ref[index * 256 : index * 256 + 256, :], wc[:, lane_block(index)], preferred_element_type=F32
        )
        velocity[slot] = velocity[slot] + part
    for target in range(8):
        for slot in range(2):
            out_ref[target, slot * 32 : slot * 32 + 32, :] = velocity[slot, target * 32 : target * 32 + 32, :]
        out_ref[target, 64:72, :] = lanes


def step_kernel(parts_ref, start_ref, rows_ref, mass_ref):
    blocks = start_ref.shape[1] // LANES
    total = parts_ref[0, 64:72, :]
    for source in range(1, 8):
        total = total + parts_ref[source, 64:72, :]
    mass = jnp.sum(total, axis=1, keepdims=True)
    lane = lax.broadcasted_iota(jnp.int32, (8, LANES), 1)
    latents = lax.broadcasted_iota(jnp.int32, (8, LANES), 0)
    line = jnp.sum(jnp.where(lane == latents, mass, 0.0), axis=0, keepdims=True)
    mass_ref[...] = jnp.broadcast_to(line, mass_ref.shape)
    velocity = [jnp.zeros((32, LANES), F32) for _ in range(blocks)]
    for source in range(8):
        for slot in range(2):
            o = first_block(source) + slot
            if o < blocks:
                velocity[o] = velocity[o] + parts_ref[source, slot * 32 : slot * 32 + 32, :]
    for o in range(blocks):
        rows_ref[:, lane_block(o)] = (start_ref[:, lane_block(o)] + 0.25 * velocity[o]).astype(BF16)


def final_kernel(scale, mass_ref, rows0, rows1, next_ref, out_ref, lines):
    blocks = lines.shape[0]
    total = jnp.sum(mass_ref[...], axis=0, keepdims=True)
    lane = lax.broadcasted_iota(jnp.int32, (1, LANES), 1)
    for b in range(4):
        out_ref[b] = scale * jnp.sum(jnp.where(lane == b, total, 0.0))
    for start, rows in ((half_rows(), rows0), (2 - half_rows(), rows1)):
        for o in range(blocks):
            lines[o] = rows[:, lane_block(o)].astype(F32)
        for o in range(blocks):
            for b in range(4):
                for r in range(2):
                    value = lines[o, pl.ds(r * 16 + b, 4, stride=4), :].astype(BF16)
                    next_ref[b, start + r, :, lane_block(o)] = value


def shape(dims, kind):
    return jax.ShapeDtypeStruct(dims, kind)


def body(state, probe_signs, timesteps, time_table, gn_gain, gn_shift, conv_weight, conv_bias):
    chans = state.shape[3]
    blocks = chans // LANES
    each = conv_weight.shape[1] * PAIRS
    params = pltpu.CompilerParams(vmem_limit_bytes=40 * 1024 * 1024)
    far = lambda array: pltpu.with_memory_space_constraint(array, pltpu.HBM)
    main, rim, base, wsend = pl.pallas_call(
        pack_kernel,
        out_shape=(
            shape((192, chans), BF16),
            shape((56, chans), BF16),
            shape((32, chans), F32),
            pltpu.HBM((32, each, LANES), BF16),
        ),
        in_specs=[HBM] * 3,
        out_specs=(VMEM,) * 3 + (HBM,),
        scratch_shapes=[
            pltpu.VMEM(conv_weight.shape, BF16),
            pltpu.VMEM(state.shape, BF16),
            pltpu.VMEM(probe_signs.shape, jnp.int32),
            pltpu.VMEM((blocks, 128, LANES), F32),
            pltpu.VMEM((blocks, 64, LANES), F32),
            pltpu.VMEM((each, LANES), F32),
            pltpu.VMEM((32, each, LANES), BF16),
            pltpu.VMEM((56, chans), F32),
            pltpu.VMEM((32, chans), F32),
            pltpu.SemaphoreType.DMA((3,)),
            pltpu.SemaphoreType.DMA,
        ],
        compiler_params=params,
        name="pack",
    )(far(conv_weight), far(state), far(probe_signs))
    offset, start = pl.pallas_call(
        lookup_kernel,
        out_shape=(shape((8, chans), F32), shape((32, chans), F32)),
        in_specs=[SMEM, HBM, VMEM, VMEM, VMEM],
        out_specs=(VMEM,) * 2,
        scratch_shapes=[pltpu.VMEM((4, 8, chans), F32), pltpu.SemaphoreType.DMA((4,))],
        compiler_params=params,
        name="lookup",
    )(timesteps, far(time_table), gn_shift[None], conv_bias[None], base)

    across = [(a * 2 + b, (1 - a) * 2 + 1 - b) for a in range(2) for b in range(2)]
    facing = lax.ppermute(rim, GX, across)
    weights = lax.all_to_all(wsend, PROBE, 0, 0, tiled=True)
    block = jnp.concatenate([main, facing, rim[48:56]], axis=0)
    down = [(i, (i + 1) % 4) for i in range(4)]
    up = [(i, (i + 3) % 4) for i in range(4)]
    above = lax.ppermute(block, "gy", down)
    below = lax.ppermute(block, "gy", up)
    lower = lax.axis_index("gx_1") == 0
    onward = [(x * 2 + c, (x + 1 - 2 * c) % 4 * 2 + c) for x in range(4) for c in range(2)]
    crossing = [(x * 2 + c, (x - 1 + 2 * c) % 4 * 2 + 1 - c) for x in range(4) for c in range(2)]
    beyond = lax.ppermute(jnp.where(lower, above, below), ("gy", "gx_1"), onward)
    crossed = lax.ppermute(jnp.where(lower, below, above), ("gy", "gx_1"), crossing)
    own = [block, above, below, beyond]
    swap = [(0, 1), (1, 0)]
    other = [lax.ppermute(block, "gx_1", swap)]
    other += [lax.ppermute(tile, "gx_1", swap) for tile in (above, below)]
    other.append(crossed)

    partial = pl.pallas_call(
        mix_kernel,
        out_shape=shape((8, 72, LANES), F32),
        in_specs=[VMEM] * 8 + [HBM] + [VMEM] * 2,
        out_specs=VMEM,
        scratch_shapes=[
            pltpu.VMEM((blocks, 1440, LANES), F32),
            pltpu.VMEM((blocks, 720, LANES), F32),
            pltpu.VMEM((blocks, 64, LANES), F32),
            pltpu.VMEM((1024, PAIRS * LANES), BF16),
            pltpu.VMEM((1024, chans), BF16),
            pltpu.VMEM((PAIRS * 256, chans), BF16),
            pltpu.VMEM((32, each, LANES), BF16),
            pltpu.VMEM((32 * each, LANES), F32),
            pltpu.VMEM((chans, PAIRS * LANES), BF16),
            pltpu.VMEM((2, 256, LANES), F32),
            pltpu.SemaphoreType.DMA,
        ],
        compiler_params=params,
        name="mix",
    )(*own, *other, far(weights), gn_gain[None], offset)

    partial = lax.all_to_all(partial, ("gy", "gx_1"), 0, 0, tiled=True)
    rows, mass = pl.pallas_call(
        step_kernel,
        out_shape=(shape((32, chans), BF16), shape((64, LANES), F32)),
        in_specs=[VMEM] * 2,
        out_specs=(VMEM,) * 2,
        compiler_params=params,
        name="step",
    )(partial, start)
    mass = lax.all_to_all(mass.reshape(64, 1, LANES), ("gx_0",) + PROBE, 0, 0, tiled=True)
    tall = lax.axis_size("probe_0")
    facing_rows = lax.ppermute(rows, "probe_0", [(y, y ^ 1) for y in range(tall)])
    scale = -0.25 / (probe_signs.shape[0] * lax.axis_size(PROBE))
    return pl.pallas_call(
        lambda *refs: final_kernel(scale, *refs),
        out_shape=(shape(state.shape, BF16), shape((4,), F32)),
        in_specs=[VMEM] * 3,
        out_specs=(VMEM, SMEM),
        scratch_shapes=[pltpu.VMEM((blocks, 32, LANES), F32)],
        compiler_params=params,
        name="final",
    )(mass.reshape(64, LANES), rows, facing_rows)


def solution(mesh):
    split = Mesh(
        mesh.devices.reshape(mesh.shape["gy"], 2, 2, 8, 4),
        ("gy", "gx_0", "gx_1", "probe_0", "probe_1"),
    )
    return jax.shard_map(
        body,
        mesh=split,
        in_specs=(
            P(None, "gy", GX, None),
            P(PROBE, None, "gy", GX, None),
            P(),
            P(),
            P(),
            P(),
            P(None, PROBE, None),
            P(),
        ),
        out_specs=(P(None, "gy", GX, None), P()),
        check_vma=False,
    )
```

```python
import jax
import jax.numpy as jnp
from jax import lax
from jax.experimental import pallas as pl
from jax.experimental.pallas import tpu as pltpu
from jax.sharding import Mesh
from jax.sharding import PartitionSpec as P


GROUPS = 32
GX = ("gx_0", "gx_1")
PROBE = ("probe_0", "probe_1")
LANES = 128
PAIRS = 6
F32 = jnp.float32
BF16 = jnp.bfloat16
VMEM = pl.BlockSpec(memory_space=pltpu.VMEM)
SMEM = pl.BlockSpec(memory_space=pltpu.SMEM)
HBM = pl.BlockSpec(memory_space=pltpu.HBM)


def three_parts(value):
    high = value.astype(BF16)
    rest = value - high.astype(F32)
    mid = rest.astype(BF16)
    low = (rest - mid.astype(F32)).astype(BF16)
    return high, mid, low


def lane_block(index):
    return slice(index * LANES, (index + 1) * LANES)


def doubled_rows(rows):
    turned = pltpu.roll(rows, 4, axis=0)
    upper = lax.broadcasted_iota(jnp.int32, rows.shape, 0) < 4
    return jnp.where(upper, rows, turned), jnp.where(upper, turned, rows)


def half_rows():
    return 2 * lax.rem(lax.axis_index("probe_0"), 2)


def first_block(member):
    return member * PAIRS // 9


def pair_of(index):
    member = lax.axis_index("gy") * 2 + lax.axis_index("gx_1")
    number = member * PAIRS + index
    return lax.rem(number, 9), lax.div(number, 9)


def lookup_kernel(step_ref, table_hbm, shift_ref, bias_ref, base_ref, offset_ref, start_ref, table, found):
    steps = [step_ref[b] for b in range(4)]
    finds = [
        pltpu.make_async_copy(
            table_hbm.at[pl.ds(pl.multiple_of(lax.div(steps[b], 8) * 8, 8), 8), :], table.at[b], found.at[b]
        )
        for b in range(4)
    ]
    for find in finds:
        find.start()
    start_ref[...] = base_ref[...] + 0.25 * bias_ref[...]
    for b in range(4):
        finds[b].wait()
        line = table[b, pl.ds(lax.rem(steps[b], 8), 1), :] + shift_ref[...]
        offset_ref[b : b + 1, :] = line
        offset_ref[b + 4 : b + 5, :] = line


def pack_kernel(
    weight_hbm, state_hbm, signs_hbm, main_ref, rim_ref, base_ref, wsend_hbm,
    weight_ref, state_ref, signs_ref, uf, xf, wf, wsend_ref, rim, sums, arrived, left,
):
    blocks = uf.shape[0]
    loads = [
        pltpu.make_async_copy(src, dst, arrived.at[index])
        for index, (src, dst) in enumerate(
            ((weight_hbm, weight_ref), (state_hbm, state_ref), (signs_hbm, signs_ref))
        )
    ]
    for load in loads:
        load.start()
    loads[0].wait()
    for index in range(PAIRS):
        tap, ob = pair_of(index)
        rows = weight_ref[tap].astype(F32)
        picked = jnp.zeros((rows.shape[0], LANES), F32)
        for o in range(blocks):
            picked = picked + jnp.where(ob == o, rows[:, lane_block(o)], 0.0)
        wf[pl.ds(index, rows.shape[0], stride=PAIRS), :] = picked
    packed = wf[...].astype(BF16)
    for target in range(wsend_ref.shape[0]):
        wsend_ref[target] = packed
    leave = pltpu.make_async_copy(wsend_ref, wsend_hbm, left)
    leave.start()
    loads[1].wait()
    loads[2].wait()
    for p in range(2):
        for b in range(4):
            for r in range(4):
                line = signs_ref[p, b, r].astype(F32)
                for o in range(blocks):
                    uf[o, pl.ds(r * 32 + p * 4 + b, 4, stride=8), :] = line[:, lane_block(o)]
    for b in range(4):
        for r in range(4):
            line = state_ref[b, r].astype(F32)
            for o in range(blocks):
                xf[o, pl.ds(r * 16 + b, 4, stride=4), :] = line[:, lane_block(o)]

    for o in range(blocks):
        base_ref[:, lane_block(o)] = xf[o, pl.ds(pl.multiple_of(half_rows() * 16, 8), 32), :]
    edge = jnp.where(lax.axis_index("gx_0") == 0, 3, 0)
    for o in range(blocks):
        sum_u = jnp.zeros((8, LANES), F32)
        cross = jnp.zeros((8, LANES), F32)
        sum_x = jnp.zeros((8, LANES), F32)
        sum_xx = jnp.zeros((8, LANES), F32)
        for two in range(8):
            pair = doubled_rows(xf[o, two * 8 : two * 8 + 8, :])
            for half in range(2):
                cell = two * 2 + half
                x = pair[half]
                u = uf[o, cell * 8 : cell * 8 + 8, :]
                sum_u, cross = sum_u + u, cross + u * x
                sum_x, sum_xx = sum_x + x, sum_xx + x * x
        for kind, part in enumerate((sum_u, cross, sum_x, sum_xx)):
            sums[kind * 8 : kind * 8 + 8, lane_block(o)] = part
        for r in range(4):
            rim[r * 8 : r * 8 + 8, lane_block(o)] = uf[o, pl.ds(pl.multiple_of((r * 4 + edge) * 8, 8), 8), :]
            rim[32 + r * 4 : 36 + r * 4, lane_block(o)] = xf[o, pl.ds((r * 4 + edge) * 4, 4), :]

    width = sums.shape[1] // GROUPS
    row = lax.broadcasted_iota(jnp.int32, (sums.shape[1], LANES), 0)
    first = lax.broadcasted_iota(jnp.int32, (sums.shape[1], LANES), 1) * width
    member = jnp.where((row >= first) & (row < first + width), 1.0, 0.0).astype(BF16)
    grouped = jnp.zeros((32, LANES), F32)
    for part in three_parts(sums[...]):
        grouped = grouped + jnp.dot(part, member, preferred_element_type=F32)
    stats = grouped[0:8]
    for kind in range(1, 4):
        stats = stats + pltpu.roll(grouped[kind * 8 : kind * 8 + 8], GROUPS * kind, axis=1)
    rim[48:56, :] = jnp.zeros((8, rim.shape[1]), F32)
    for index, part in enumerate(three_parts(stats)):
        rim[48:56, lane_block(index)] = part.astype(F32)

    for o in range(blocks):
        main_ref[0:128, lane_block(o)] = uf[o].astype(BF16)
        main_ref[128:192, lane_block(o)] = xf[o].astype(BF16)
    rim_ref[...] = rim[...].astype(BF16)
    leave.wait()


def mix_kernel(
    own0, own1, own3, own2, other0, other1, other3, other2, weight_hbm, gain_ref, offset_ref,
    out_ref, ug, xg, edges, lhs_ref, slope_ref, rows_ref, weight_ref, wf, wc, velocity, arrived,
):
    load = pltpu.make_async_copy(weight_hbm, weight_ref, arrived)
    load.start()
    blocks = ug.shape[0]
    core = lax.axis_index("gx_1")
    half = lax.axis_index("gx_0")
    chans = own0.shape[1]

    def spot(row, col):
        return pl.multiple_of((row * 10 + col) * 8, 8)

    def small(row, col):
        return pl.multiple_of((row * 10 + col) * 4, 4)

    for o in range(blocks):
        for row in (0, 17):
            ug[o, row * 80 : row * 80 + 80, :] = jnp.zeros((80, LANES), F32)
            xg[o, row * 40 : row * 40 + 40, :] = jnp.zeros((40, LANES), F32)
        for row in range(1, 17):
            for col in (0, 9):
                ug[o, row * 80 + col * 8 : row * 80 + col * 8 + 8, :] = jnp.zeros((8, LANES), F32)
                xg[o, row * 40 + col * 4 : row * 40 + col * 4 + 4, :] = jnp.zeros((4, LANES), F32)

    total = jnp.zeros((8, chans), F32)
    rim_here = core == 1 - half
    rim_col = jnp.where(half == 0, 9, 0)
    sources = ((0, own0, other0), (1, own1, other1), (3, own3, other3), (2, own2, other2))
    for back, own_ref, other_ref in sources:
        tile = lax.rem(lax.axis_index("gy") + 4 - back, 4)
        for src, base in ((own_ref, 4 * core), (other_ref, 4 * (1 - core))):
            for r in range(4):
                at = spot(4 * tile + r + 1, base + 1)
                lines = src[r * 32 : r * 32 + 32, :].astype(F32)
                states = src[128 + r * 16 : 144 + r * 16, :].astype(F32)
                for o in range(blocks):
                    ug[o, pl.ds(at, 32), :] = lines[:, lane_block(o)]
                    xg[o, pl.ds(small(4 * tile + r + 1, base + 1), 16), :] = states[:, lane_block(o)]
        mine = own_ref[192:256, :].astype(F32)
        theirs = other_ref[192:256, :].astype(F32)
        total = total + mine[48:56] + mine[56:64] + theirs[48:56] + theirs[56:64]
        rim = jnp.where(rim_here, mine[0:48], theirs[0:48])
        for r in range(4):
            at = spot(4 * tile + r + 1, rim_col)
            for o in range(blocks):
                ug[o, pl.ds(at, 8), :] = rim[r * 8 : r * 8 + 8, lane_block(o)]
        for o in range(blocks):
            edges[o, pl.ds(pl.multiple_of(tile * 16, 16), 16), :] = rim[32:48, lane_block(o)]

    stats = total[:, lane_block(0)] + total[:, lane_block(1)] + total[:, lane_block(2)]
    width = chans // GROUPS
    lane = lax.broadcasted_iota(jnp.int32, (LANES, chans), 1)
    first = lax.broadcasted_iota(jnp.int32, (LANES, chans), 0) * width
    spread = jnp.where((lane >= first) & (lane < first + width), 1.0, 0.0).astype(BF16)

    def expanded(kind):
        turned = stats if kind == 0 else pltpu.roll(stats, LANES - GROUPS * kind, axis=1)
        out = jnp.zeros((8, chans), F32)
        for part in three_parts(turned):
            out = out + jnp.dot(part, spread, preferred_element_type=F32)
        return out

    count = 256 * width
    sum_u, cross, sum_x, sum_xx = (expanded(kind) for kind in range(4))
    mean = sum_x / count
    sigma = jnp.sqrt(sum_xx / count - mean * mean + 1e-05)
    inverse = 1.0 / sigma
    mean_u = sum_u / count
    mean_cu = (cross - mean * sum_u) / count
    bend = mean_cu / (sigma * sigma * sigma)
    offset = offset_ref[...]
    gain = gain_ref[...]

    scale = inverse * gain
    tilt = gain * inverse

    def fields(x, o, rows):
        at = lane_block(o)
        centered = x - mean[:rows, at]
        pre = centered * scale[:rows, at] + offset[:rows, at]
        sig = 0.5 + 0.5 * jnp.tanh(0.5 * pre)
        return centered, pre, sig

    def grid_row(gr, carry):
        at = spot(gr + 1, 1)
        near = small(gr + 1, 1)
        for o in range(blocks):
            ln = lane_block(o)
            x = xg[o, pl.ds(near, 32), :].reshape(4, 8, LANES)
            centered, pre, sig = fields(x, o, 8)
            xg[o, pl.ds(near, 32), :] = (pre * sig).reshape(32, LANES)
            slope = sig * (1.0 + pre * (1.0 - sig))
            along = slope * tilt[:, ln]
            across = slope * gain[:, ln] * centered
            for two in range(4):
                spans = zip(doubled_rows(along[two]), doubled_rows(across[two]))
                cells = []
                for half_cell, (first, second) in enumerate(spans):
                    u = ug[o, pl.ds(pl.multiple_of(at + (two * 2 + half_cell) * 8, 8), 8), :]
                    cells.append(first * (u - mean_u[:, ln]) - second * bend[:, ln])
                out = jnp.concatenate(cells, axis=0).astype(BF16)
                slope_ref[pl.ds(pl.multiple_of(gr * 64 + two * 16, 16), 16), ln] = out
        return carry

    for o in range(blocks):
        _, pre, sig = fields(edges[o].reshape(8, 8, LANES), o, 8)
        edges[o] = (pre * sig).reshape(64, LANES)
        for row in range(16):
            xg[o, pl.ds(small(row + 1, rim_col), 4), :] = edges[o, row * 4 : row * 4 + 4, :]

    taps = [pair_of(index) for index in range(PAIRS)]

    def lhs_row(gr):
        for index, (tap, ob) in enumerate(taps):
            dy, dx = lax.div(tap, 3), lax.rem(tap, 3)
            at = spot(gr + 2 - dy, 2 - dx)
            value = ug[jnp.minimum(ob, blocks - 1), pl.ds(at, 64), :]
            lhs_ref[pl.ds(pl.multiple_of(gr * 64, 64), 64), lane_block(index)] = value.astype(BF16)

    load.wait()
    each = weight_ref.shape[1]
    for source in range(weight_ref.shape[0]):
        wf[source * each : (source + 1) * each, :] = weight_ref[source].astype(F32)
    for index in range(PAIRS):
        wc[:, lane_block(index)] = wf[pl.ds(index, chans, stride=PAIRS), :].astype(BF16)

    def grid_rows(quad, total):
        for sub in range(4):
            lhs_row(quad * 4 + sub)
        span = pl.ds(pl.multiple_of(quad * 256, 256), 256)
        value = lax.dot_general(lhs_ref[span, :], wc[...], (((1,), (1,)), ((), ())), preferred_element_type=F32)
        for sub in range(4):
            grid_row(quad * 4 + sub, 0)
        value = value * slope_ref[span, :].astype(F32)
        return total + jnp.sum(value.reshape(32, 8, chans), axis=0)

    total = lax.fori_loop(0, 4, grid_rows, jnp.zeros((8, chans), F32))

    for index, (tap, ob) in enumerate(taps):
        dy, dx = lax.div(tap, 3), lax.rem(tap, 3)
        for target in range(8):
            for line in range(2):
                at = small(4 * (target // 2) + half_rows() + line + dy, 4 * (target % 2) + dx)
                to = index * 256 + target * 32 + line * 16
                for o in range(blocks):
                    rows_ref[to : to + 16, lane_block(o)] = xg[o, pl.ds(at, 16), :].astype(BF16)

    lanes = total[:, lane_block(0)]
    for o in range(1, blocks):
        lanes = lanes + total[:, lane_block(o)]
    lanes = lanes + pltpu.roll(lanes, 4, axis=0)

    velocity[...] = jnp.zeros(velocity.shape, F32)
    for index in range(PAIRS):
        slot = taps[index][1] - lax.div((lax.axis_index("gy") * 2 + lax.axis_index("gx_1")) * PAIRS, 9)
        part = jnp.dot(
            rows_ref[index * 256 : index * 256 + 256, :], wc[:, lane_block(index)], preferred_element_type=F32
        )
        velocity[slot] = velocity[slot] + part
    for target in range(8):
        for slot in range(2):
            out_ref[target, slot * 32 : slot * 32 + 32, :] = velocity[slot, target * 32 : target * 32 + 32, :]
        out_ref[target, 64:72, :] = lanes


def step_kernel(parts_ref, start_ref, rows_ref, mass_ref):
    blocks = start_ref.shape[1] // LANES
    total = parts_ref[0, 64:72, :]
    for source in range(1, 8):
        total = total + parts_ref[source, 64:72, :]
    mass = jnp.sum(total, axis=1, keepdims=True)
    lane = lax.broadcasted_iota(jnp.int32, (8, LANES), 1)
    latents = lax.broadcasted_iota(jnp.int32, (8, LANES), 0)
    line = jnp.sum(jnp.where(lane == latents, mass, 0.0), axis=0, keepdims=True)
    mass_ref[...] = jnp.broadcast_to(line, mass_ref.shape)
    velocity = [jnp.zeros((32, LANES), F32) for _ in range(blocks)]
    for source in range(8):
        for slot in range(2):
            o = first_block(source) + slot
            if o < blocks:
                velocity[o] = velocity[o] + parts_ref[source, slot * 32 : slot * 32 + 32, :]
    for o in range(blocks):
        rows_ref[:, lane_block(o)] = (start_ref[:, lane_block(o)] + 0.25 * velocity[o]).astype(BF16)


def final_kernel(scale, mass_ref, rows0, rows1, next_ref, out_ref, lines):
    blocks = lines.shape[0]
    total = jnp.sum(mass_ref[...], axis=0, keepdims=True)
    lane = lax.broadcasted_iota(jnp.int32, (1, LANES), 1)
    for b in range(4):
        out_ref[b] = scale * jnp.sum(jnp.where(lane == b, total, 0.0))
    for start, rows in ((half_rows(), rows0), (2 - half_rows(), rows1)):
        for o in range(blocks):
            lines[o] = rows[:, lane_block(o)].astype(F32)
        for o in range(blocks):
            for b in range(4):
                for r in range(2):
                    value = lines[o, pl.ds(r * 16 + b, 4, stride=4), :].astype(BF16)
                    next_ref[b, start + r, :, lane_block(o)] = value


def shape(dims, kind):
    return jax.ShapeDtypeStruct(dims, kind)


def body(state, probe_signs, timesteps, time_table, gn_gain, gn_shift, conv_weight, conv_bias):
    chans = state.shape[3]
    blocks = chans // LANES
    each = conv_weight.shape[1] * PAIRS
    params = pltpu.CompilerParams(vmem_limit_bytes=40 * 1024 * 1024)
    far = lambda array: pltpu.with_memory_space_constraint(array, pltpu.HBM)
    main, rim, base, wsend = pl.pallas_call(
        pack_kernel,
        out_shape=(
            shape((192, chans), BF16),
            shape((56, chans), BF16),
            shape((32, chans), F32),
            pltpu.HBM((32, each, LANES), BF16),
        ),
        in_specs=[HBM] * 3,
        out_specs=(VMEM,) * 3 + (HBM,),
        scratch_shapes=[
            pltpu.VMEM(conv_weight.shape, BF16),
            pltpu.VMEM(state.shape, BF16),
            pltpu.VMEM(probe_signs.shape, jnp.int32),
            pltpu.VMEM((blocks, 128, LANES), F32),
            pltpu.VMEM((blocks, 64, LANES), F32),
            pltpu.VMEM((each, LANES), F32),
            pltpu.VMEM((32, each, LANES), BF16),
            pltpu.VMEM((56, chans), F32),
            pltpu.VMEM((32, chans), F32),
            pltpu.SemaphoreType.DMA((3,)),
            pltpu.SemaphoreType.DMA,
        ],
        compiler_params=params,
        name="pack",
    )(far(conv_weight), far(state), far(probe_signs))
    offset, start = pl.pallas_call(
        lookup_kernel,
        out_shape=(shape((8, chans), F32), shape((32, chans), F32)),
        in_specs=[SMEM, HBM, VMEM, VMEM, VMEM],
        out_specs=(VMEM,) * 2,
        scratch_shapes=[pltpu.VMEM((4, 8, chans), F32), pltpu.SemaphoreType.DMA((4,))],
        compiler_params=params,
        name="lookup",
    )(timesteps, far(time_table), gn_shift[None], conv_bias[None], base)

    across = [(a * 2 + b, (1 - a) * 2 + 1 - b) for a in range(2) for b in range(2)]
    facing = lax.ppermute(rim, GX, across)
    weights = lax.all_to_all(wsend, PROBE, 0, 0, tiled=True)
    block = jnp.concatenate([main, facing, rim[48:56]], axis=0)
    down = [(i, (i + 1) % 4) for i in range(4)]
    up = [(i, (i + 3) % 4) for i in range(4)]
    above = lax.ppermute(block, "gy", down)
    below = lax.ppermute(block, "gy", up)
    lower = lax.axis_index("gx_1") == 0
    onward = [(x * 2 + c, (x + 1 - 2 * c) % 4 * 2 + c) for x in range(4) for c in range(2)]
    crossing = [(x * 2 + c, (x - 1 + 2 * c) % 4 * 2 + 1 - c) for x in range(4) for c in range(2)]
    beyond = lax.ppermute(jnp.where(lower, above, below), ("gy", "gx_1"), onward)
    crossed = lax.ppermute(jnp.where(lower, below, above), ("gy", "gx_1"), crossing)
    own = [block, above, below, beyond]
    swap = [(0, 1), (1, 0)]
    other = [lax.ppermute(block, "gx_1", swap)]
    other += [lax.ppermute(tile, "gx_1", swap) for tile in (above, below)]
    other.append(crossed)

    partial = pl.pallas_call(
        mix_kernel,
        out_shape=shape((8, 72, LANES), F32),
        in_specs=[VMEM] * 8 + [HBM] + [VMEM] * 2,
        out_specs=VMEM,
        scratch_shapes=[
            pltpu.VMEM((blocks, 1440, LANES), F32),
            pltpu.VMEM((blocks, 720, LANES), F32),
            pltpu.VMEM((blocks, 64, LANES), F32),
            pltpu.VMEM((1024, PAIRS * LANES), BF16),
            pltpu.VMEM((1024, chans), BF16),
            pltpu.VMEM((PAIRS * 256, chans), BF16),
            pltpu.VMEM((32, each, LANES), BF16),
            pltpu.VMEM((32 * each, LANES), F32),
            pltpu.VMEM((chans, PAIRS * LANES), BF16),
            pltpu.VMEM((2, 256, LANES), F32),
            pltpu.SemaphoreType.DMA,
        ],
        compiler_params=params,
        name="mix",
    )(*own, *other, far(weights), gn_gain[None], offset)

    partial = lax.all_to_all(partial, ("gy", "gx_1"), 0, 0, tiled=True)
    rows, mass = pl.pallas_call(
        step_kernel,
        out_shape=(shape((32, chans), BF16), shape((64, LANES), F32)),
        in_specs=[VMEM] * 2,
        out_specs=(VMEM,) * 2,
        compiler_params=params,
        name="step",
    )(partial, start)
    mass = lax.all_to_all(mass.reshape(64, 1, LANES), ("gx_0",) + PROBE, 0, 0, tiled=True)
    tall = lax.axis_size("probe_0")
    facing_rows = lax.ppermute(rows, "probe_0", [(y, y ^ 1) for y in range(tall)])
    scale = -0.25 / (probe_signs.shape[0] * lax.axis_size(PROBE))
    return pl.pallas_call(
        lambda *refs: final_kernel(scale, *refs),
        out_shape=(shape(state.shape, BF16), shape((4,), F32)),
        in_specs=[VMEM] * 3,
        out_specs=(VMEM, SMEM),
        scratch_shapes=[pltpu.VMEM((blocks, 32, LANES), F32)],
        compiler_params=params,
        name="final",
    )(mass.reshape(64, LANES), rows, facing_rows)


def solution(mesh):
    split = Mesh(
        mesh.devices.reshape(mesh.shape["gy"], 2, 2, 8, 4),
        ("gy", "gx_0", "gx_1", "probe_0", "probe_1"),
    )
    return jax.shard_map(
        body,
        mesh=split,
        in_specs=(
            P(None, "gy", GX, None),
            P(PROBE, None, "gy", GX, None),
            P(),
            P(),
            P(),
            P(),
            P(None, PROBE, None),
            P(),
        ),
        out_specs=(P(None, "gy", GX, None), P()),
        check_vma=False,
    )
```

```python
import jax
import jax.numpy as jnp
from jax import lax
from jax.experimental import pallas as pl
from jax.experimental.pallas import tpu as pltpu
from jax.sharding import Mesh
from jax.sharding import PartitionSpec as P


GROUPS = 32
GX = ("gx_0", "gx_1")
PROBE = ("probe_0", "probe_1")
LANES = 128
PAIRS = 6
F32 = jnp.float32
BF16 = jnp.bfloat16
VMEM = pl.BlockSpec(memory_space=pltpu.VMEM)
SMEM = pl.BlockSpec(memory_space=pltpu.SMEM)
HBM = pl.BlockSpec(memory_space=pltpu.HBM)


def three_parts(value):
    high = value.astype(BF16)
    rest = value - high.astype(F32)
    mid = rest.astype(BF16)
    low = (rest - mid.astype(F32)).astype(BF16)
    return high, mid, low


def lane_block(index):
    return slice(index * LANES, (index + 1) * LANES)


def doubled_rows(rows):
    turned = pltpu.roll(rows, 4, axis=0)
    upper = lax.broadcasted_iota(jnp.int32, rows.shape, 0) < 4
    return jnp.where(upper, rows, turned), jnp.where(upper, turned, rows)


def half_rows():
    return 2 * lax.rem(lax.axis_index("probe_0"), 2)


def first_block(member):
    return member * PAIRS // 9


def pair_of(index):
    member = lax.axis_index("gy") * 2 + lax.axis_index("gx_1")
    number = member * PAIRS + index
    return lax.rem(number, 9), lax.div(number, 9)


def lookup_kernel(step_ref, table_hbm, shift_ref, bias_ref, base_ref, offset_ref, start_ref, table, found):
    steps = [step_ref[b] for b in range(4)]
    finds = [
        pltpu.make_async_copy(
            table_hbm.at[pl.ds(pl.multiple_of(lax.div(steps[b], 8) * 8, 8), 8), :], table.at[b], found.at[b]
        )
        for b in range(4)
    ]
    for find in finds:
        find.start()
    start_ref[...] = base_ref[...] + 0.25 * bias_ref[...]
    for b in range(4):
        finds[b].wait()
        line = table[b, pl.ds(lax.rem(steps[b], 8), 1), :] + shift_ref[...]
        offset_ref[b : b + 1, :] = line
        offset_ref[b + 4 : b + 5, :] = line


def pack_kernel(
    weight_hbm, state_hbm, signs_hbm, main_ref, rim_ref, base_ref, wsend_hbm,
    weight_ref, state_ref, signs_ref, uf, xf, wf, wsend_ref, rim, sums, arrived, left,
):
    blocks = uf.shape[0]
    loads = [
        pltpu.make_async_copy(src, dst, arrived.at[index])
        for index, (src, dst) in enumerate(
            ((weight_hbm, weight_ref), (state_hbm, state_ref), (signs_hbm, signs_ref))
        )
    ]
    for load in loads:
        load.start()
    loads[0].wait()
    for index in range(PAIRS):
        tap, ob = pair_of(index)
        rows = weight_ref[tap].astype(F32)
        picked = jnp.zeros((rows.shape[0], LANES), F32)
        for o in range(blocks):
            picked = picked + jnp.where(ob == o, rows[:, lane_block(o)], 0.0)
        wf[pl.ds(index, rows.shape[0], stride=PAIRS), :] = picked
    packed = wf[0 : wsend_ref.shape[1], :].astype(BF16)
    for target in range(wsend_ref.shape[0]):
        wsend_ref[target] = packed
    leave = pltpu.make_async_copy(wsend_ref, wsend_hbm, left)
    leave.start()
    loads[1].wait()
    loads[2].wait()
    for p in range(2):
        for b in range(4):
            for r in range(4):
                line = signs_ref[p, b, r].astype(F32)
                for o in range(blocks):
                    uf[o, pl.ds(r * 32 + p * 4 + b, 4, stride=8), :] = line[:, lane_block(o)]
    for b in range(4):
        for r in range(4):
            line = state_ref[b, r].astype(F32)
            for o in range(blocks):
                xf[o, pl.ds(r * 16 + b, 4, stride=4), :] = line[:, lane_block(o)]

    for o in range(blocks):
        base_ref[:, lane_block(o)] = xf[o, pl.ds(pl.multiple_of(half_rows() * 16, 8), 32), :]
    edge = jnp.where(lax.axis_index("gx_0") == 0, 3, 0)
    for o in range(blocks):
        sum_u = jnp.zeros((8, LANES), F32)
        cross = jnp.zeros((8, LANES), F32)
        sum_x = jnp.zeros((8, LANES), F32)
        sum_xx = jnp.zeros((8, LANES), F32)
        for two in range(8):
            pair = doubled_rows(xf[o, two * 8 : two * 8 + 8, :])
            for half in range(2):
                cell = two * 2 + half
                x = pair[half]
                u = uf[o, cell * 8 : cell * 8 + 8, :]
                sum_u, cross = sum_u + u, cross + u * x
                sum_x, sum_xx = sum_x + x, sum_xx + x * x
        for kind, part in enumerate((sum_u, cross, sum_x, sum_xx)):
            sums[kind * 8 : kind * 8 + 8, lane_block(o)] = part
        for r in range(4):
            rim[r * 8 : r * 8 + 8, lane_block(o)] = uf[o, pl.ds(pl.multiple_of((r * 4 + edge) * 8, 8), 8), :]
            rim[32 + r * 4 : 36 + r * 4, lane_block(o)] = xf[o, pl.ds((r * 4 + edge) * 4, 4), :]

    width = sums.shape[1] // GROUPS
    row = lax.broadcasted_iota(jnp.int32, (sums.shape[1], LANES), 0)
    first = lax.broadcasted_iota(jnp.int32, (sums.shape[1], LANES), 1) * width
    member = jnp.where((row >= first) & (row < first + width), 1.0, 0.0).astype(BF16)
    grouped = jnp.zeros((32, LANES), F32)
    for part in three_parts(sums[...]):
        grouped = grouped + jnp.dot(part, member, preferred_element_type=F32)
    stats = grouped[0:8]
    for kind in range(1, 4):
        stats = stats + pltpu.roll(grouped[kind * 8 : kind * 8 + 8], GROUPS * kind, axis=1)
    rim[48:56, :] = jnp.zeros((8, rim.shape[1]), F32)
    for index, part in enumerate(three_parts(stats)):
        rim[48:56, lane_block(index)] = part.astype(F32)

    for o in range(blocks):
        main_ref[0:128, lane_block(o)] = uf[o, 0:128, :].astype(BF16)
        main_ref[128:192, lane_block(o)] = xf[o, 0:64, :].astype(BF16)
    rim_ref[...] = rim[...].astype(BF16)
    leave.wait()


def mix_kernel(
    own0, own1, own3, own2, other0, other1, other3, other2, weight_hbm, gain_ref, offset_ref,
    out_ref, ug, xg, edges, lhs_ref, slope_ref, rows_ref, weight_ref, wf, wc, velocity, arrived,
):
    load = pltpu.make_async_copy(weight_hbm, weight_ref, arrived)
    load.start()
    blocks = ug.shape[0]
    core = lax.axis_index("gx_1")
    half = lax.axis_index("gx_0")
    chans = own0.shape[1]

    def spot(row, col):
        return pl.multiple_of((row * 10 + col) * 8, 8)

    def small(row, col):
        return pl.multiple_of((row * 10 + col) * 4, 4)

    for o in range(blocks):
        for row in (0, 17):
            ug[o, row * 80 : row * 80 + 80, :] = jnp.zeros((80, LANES), F32)
            xg[o, row * 40 : row * 40 + 40, :] = jnp.zeros((40, LANES), F32)
        for row in range(1, 17):
            for col in (0, 9):
                ug[o, row * 80 + col * 8 : row * 80 + col * 8 + 8, :] = jnp.zeros((8, LANES), F32)
                xg[o, row * 40 + col * 4 : row * 40 + col * 4 + 4, :] = jnp.zeros((4, LANES), F32)

    total = jnp.zeros((8, chans), F32)
    rim_here = core == 1 - half
    rim_col = jnp.where(half == 0, 9, 0)
    sources = ((0, own0, other0), (1, own1, other1), (3, own3, other3), (2, own2, other2))
    for back, own_ref, other_ref in sources:
        tile = lax.rem(lax.axis_index("gy") + 4 - back, 4)
        for src, base in ((own_ref, 4 * core), (other_ref, 4 * (1 - core))):
            for r in range(4):
                at = spot(4 * tile + r + 1, base + 1)
                lines = src[r * 32 : r * 32 + 32, :].astype(F32)
                states = src[128 + r * 16 : 144 + r * 16, :].astype(F32)
                for o in range(blocks):
                    ug[o, pl.ds(at, 32), :] = lines[:, lane_block(o)]
                    xg[o, pl.ds(small(4 * tile + r + 1, base + 1), 16), :] = states[:, lane_block(o)]
        mine = own_ref[192:256, :].astype(F32)
        theirs = other_ref[192:256, :].astype(F32)
        total = total + mine[48:56] + mine[56:64] + theirs[48:56] + theirs[56:64]
        rim = jnp.where(rim_here, mine[0:48], theirs[0:48])
        for r in range(4):
            at = spot(4 * tile + r + 1, rim_col)
            for o in range(blocks):
                ug[o, pl.ds(at, 8), :] = rim[r * 8 : r * 8 + 8, lane_block(o)]
        for o in range(blocks):
            edges[o, pl.ds(pl.multiple_of(tile * 16, 16), 16), :] = rim[32:48, lane_block(o)]

    stats = total[:, lane_block(0)] + total[:, lane_block(1)] + total[:, lane_block(2)]
    width = chans // GROUPS
    lane = lax.broadcasted_iota(jnp.int32, (LANES, chans), 1)
    first = lax.broadcasted_iota(jnp.int32, (LANES, chans), 0) * width
    spread = jnp.where((lane >= first) & (lane < first + width), 1.0, 0.0).astype(BF16)

    def expanded(kind):
        turned = stats if kind == 0 else pltpu.roll(stats, LANES - GROUPS * kind, axis=1)
        out = jnp.zeros((8, chans), F32)
        for part in three_parts(turned):
            out = out + jnp.dot(part, spread, preferred_element_type=F32)
        return out

    count = 256 * width
    sum_u, cross, sum_x, sum_xx = (expanded(kind) for kind in range(4))
    mean = sum_x / count
    sigma = jnp.sqrt(sum_xx / count - mean * mean + 1e-05)
    inverse = 1.0 / sigma
    mean_u = sum_u / count
    mean_cu = (cross - mean * sum_u) / count
    bend = mean_cu / (sigma * sigma * sigma)
    offset = offset_ref[...]
    gain = gain_ref[...]

    scale = inverse * gain
    tilt = gain * inverse

    def fields(x, o, rows):
        at = lane_block(o)
        centered = x - mean[:rows, at]
        pre = centered * scale[:rows, at] + offset[:rows, at]
        sig = 0.5 + 0.5 * jnp.tanh(0.5 * pre)
        return centered, pre, sig

    def grid_row(gr, carry):
        at = spot(gr + 1, 1)
        near = small(gr + 1, 1)
        for o in range(blocks):
            ln = lane_block(o)
            x = xg[o, pl.ds(near, 32), :].reshape(4, 8, LANES)
            centered, pre, sig = fields(x, o, 8)
            xg[o, pl.ds(near, 32), :] = (pre * sig).reshape(32, LANES)
            slope = sig * (1.0 + pre * (1.0 - sig))
            along = slope * tilt[:, ln]
            across = slope * gain[:, ln] * centered
            for two in range(4):
                spans = zip(doubled_rows(along[two]), doubled_rows(across[two]))
                cells = []
                for half_cell, (first, second) in enumerate(spans):
                    u = ug[o, pl.ds(pl.multiple_of(at + (two * 2 + half_cell) * 8, 8), 8), :]
                    cells.append(first * (u - mean_u[:, ln]) - second * bend[:, ln])
                out = jnp.concatenate(cells, axis=0).astype(BF16)
                slope_ref[pl.ds(pl.multiple_of(gr * 64 + two * 16, 16), 16), ln] = out
        return carry

    lax.fori_loop(0, 16, grid_row, 0)

    for o in range(blocks):
        _, pre, sig = fields(edges[o].reshape(8, 8, LANES), o, 8)
        edges[o] = (pre * sig).reshape(64, LANES)
        for row in range(16):
            xg[o, pl.ds(small(row + 1, rim_col), 4), :] = edges[o, row * 4 : row * 4 + 4, :]

    taps = [pair_of(index) for index in range(PAIRS)]

    def lhs_row(gr, carry):
        for index, (tap, ob) in enumerate(taps):
            dy, dx = lax.div(tap, 3), lax.rem(tap, 3)
            at = spot(gr + 2 - dy, 2 - dx)
            value = ug[jnp.minimum(ob, blocks - 1), pl.ds(at, 64), :]
            lhs_ref[pl.ds(pl.multiple_of(gr * 64, 64), 64), lane_block(index)] = value.astype(BF16)
        return carry

    lax.fori_loop(0, 16, lhs_row, 0)

    for index, (tap, ob) in enumerate(taps):
        dy, dx = lax.div(tap, 3), lax.rem(tap, 3)
        for target in range(8):
            for line in range(2):
                at = small(4 * (target // 2) + half_rows() + line + dy, 4 * (target % 2) + dx)
                to = index * 256 + target * 32 + line * 16
                for o in range(blocks):
                    rows_ref[to : to + 16, lane_block(o)] = xg[o, pl.ds(at, 16), :].astype(BF16)

    load.wait()
    each = weight_ref.shape[1]
    for source in range(weight_ref.shape[0]):
        wf[source * each : (source + 1) * each, :] = weight_ref[source].astype(F32)
    for index in range(PAIRS):
        wc[:, lane_block(index)] = wf[pl.ds(index, chans, stride=PAIRS), :].astype(BF16)

    chunk = 512
    total = jnp.zeros((8, chans), F32)
    for start in range(0, lhs_ref.shape[0], chunk):
        value = lax.dot_general(
            lhs_ref[start : start + chunk, :], wc[...], (((1,), (1,)), ((), ())), preferred_element_type=F32
        )
        value = value * slope_ref[start : start + chunk, :].astype(F32)
        total = total + jnp.sum(value.reshape(chunk // 8, 8, chans), axis=0)
    lanes = total[:, lane_block(0)]
    for o in range(1, blocks):
        lanes = lanes + total[:, lane_block(o)]
    lanes = lanes + pltpu.roll(lanes, 4, axis=0)

    velocity[...] = jnp.zeros(velocity.shape, F32)
    for index in range(PAIRS):
        slot = taps[index][1] - lax.div((lax.axis_index("gy") * 2 + lax.axis_index("gx_1")) * PAIRS, 9)
        part = jnp.dot(
            rows_ref[index * 256 : index * 256 + 256, :], wc[:, lane_block(index)], preferred_element_type=F32
        )
        velocity[slot] = velocity[slot] + part
    for target in range(8):
        for slot in range(2):
            out_ref[target, slot * 32 : slot * 32 + 32, :] = velocity[slot, target * 32 : target * 32 + 32, :]
        out_ref[target, 64:72, :] = lanes


def step_kernel(parts_ref, start_ref, rows_ref, mass_ref):
    blocks = start_ref.shape[1] // LANES
    total = parts_ref[0, 64:72, :]
    for source in range(1, 8):
        total = total + parts_ref[source, 64:72, :]
    mass = jnp.sum(total, axis=1, keepdims=True)
    lane = lax.broadcasted_iota(jnp.int32, (8, LANES), 1)
    latents = lax.broadcasted_iota(jnp.int32, (8, LANES), 0)
    line = jnp.sum(jnp.where(lane == latents, mass, 0.0), axis=0, keepdims=True)
    mass_ref[...] = jnp.broadcast_to(line, mass_ref.shape)
    velocity = [jnp.zeros((32, LANES), F32) for _ in range(blocks)]
    for source in range(8):
        for slot in range(2):
            o = first_block(source) + slot
            if o < blocks:
                velocity[o] = velocity[o] + parts_ref[source, slot * 32 : slot * 32 + 32, :]
    for o in range(blocks):
        rows_ref[:, lane_block(o)] = (start_ref[:, lane_block(o)] + 0.25 * velocity[o]).astype(BF16)


def final_kernel(scale, mass_ref, rows0, rows1, next_ref, out_ref, lines):
    blocks = lines.shape[0]
    total = jnp.sum(mass_ref[...], axis=0, keepdims=True)
    lane = lax.broadcasted_iota(jnp.int32, (1, LANES), 1)
    for b in range(4):
        out_ref[b] = scale * jnp.sum(jnp.where(lane == b, total, 0.0))
    for start, rows in ((half_rows(), rows0), (2 - half_rows(), rows1)):
        for o in range(blocks):
            lines[o, 0:32, :] = rows[:, lane_block(o)].astype(F32)
        for o in range(blocks):
            for b in range(4):
                for r in range(2):
                    value = lines[o, pl.ds(r * 16 + b, 4, stride=4), :].astype(BF16)
                    next_ref[b, start + r, :, lane_block(o)] = value


def shape(dims, kind):
    return jax.ShapeDtypeStruct(dims, kind)


def body(state, probe_signs, timesteps, time_table, gn_gain, gn_shift, conv_weight, conv_bias):
    chans = state.shape[3]
    blocks = chans // LANES
    each = conv_weight.shape[1] * PAIRS
    params = pltpu.CompilerParams(vmem_limit_bytes=40 * 1024 * 1024)
    far = lambda array: pltpu.with_memory_space_constraint(array, pltpu.HBM)
    main, rim, base, wsend = pl.pallas_call(
        pack_kernel,
        out_shape=(
            shape((192, chans), BF16),
            shape((56, chans), BF16),
            shape((32, chans), F32),
            pltpu.HBM((32, each, LANES), BF16),
        ),
        in_specs=[HBM] * 3,
        out_specs=(VMEM,) * 3 + (HBM,),
        scratch_shapes=[
            pltpu.VMEM(conv_weight.shape, BF16),
            pltpu.VMEM(state.shape, BF16),
            pltpu.VMEM(probe_signs.shape, jnp.int32),
            pltpu.VMEM((blocks, 192, LANES), F32),
            pltpu.VMEM((blocks, 96, LANES), F32),
            pltpu.VMEM((each + 40, LANES), F32),
            pltpu.VMEM((32, each, LANES), BF16),
            pltpu.VMEM((56, chans), F32),
            pltpu.VMEM((32, chans), F32),
            pltpu.SemaphoreType.DMA((3,)),
            pltpu.SemaphoreType.DMA,
        ],
        compiler_params=params,
        name="pack",
    )(far(conv_weight), far(state), far(probe_signs))
    offset, start = pl.pallas_call(
        lookup_kernel,
        out_shape=(shape((8, chans), F32), shape((32, chans), F32)),
        in_specs=[SMEM, HBM, VMEM, VMEM, VMEM],
        out_specs=(VMEM,) * 2,
        scratch_shapes=[pltpu.VMEM((4, 8, chans), F32), pltpu.SemaphoreType.DMA((4,))],
        compiler_params=params,
        name="lookup",
    )(timesteps, far(time_table), gn_shift[None], conv_bias[None], base)

    across = [(a * 2 + b, (1 - a) * 2 + 1 - b) for a in range(2) for b in range(2)]
    facing = lax.ppermute(rim, GX, across)
    weights = lax.all_to_all(wsend, PROBE, 0, 0, tiled=True)
    block = jnp.concatenate([main, facing, rim[48:56]], axis=0)
    down = [(i, (i + 1) % 4) for i in range(4)]
    up = [(i, (i + 3) % 4) for i in range(4)]
    above = lax.ppermute(block, "gy", down)
    below = lax.ppermute(block, "gy", up)
    lower = lax.axis_index("gx_1") == 0
    onward = [(x * 2 + c, (x + 1 - 2 * c) % 4 * 2 + c) for x in range(4) for c in range(2)]
    crossing = [(x * 2 + c, (x - 1 + 2 * c) % 4 * 2 + 1 - c) for x in range(4) for c in range(2)]
    beyond = lax.ppermute(jnp.where(lower, above, below), ("gy", "gx_1"), onward)
    crossed = lax.ppermute(jnp.where(lower, below, above), ("gy", "gx_1"), crossing)
    own = [block, above, below, beyond]
    swap = [(0, 1), (1, 0)]
    other = [lax.ppermute(block, "gx_1", swap)]
    other += [lax.ppermute(tile, "gx_1", swap) for tile in (above, below)]
    other.append(crossed)

    partial = pl.pallas_call(
        mix_kernel,
        out_shape=shape((8, 72, LANES), F32),
        in_specs=[VMEM] * 8 + [HBM] + [VMEM] * 2,
        out_specs=VMEM,
        scratch_shapes=[
            pltpu.VMEM((blocks, 1440, LANES), F32),
            pltpu.VMEM((blocks, 720, LANES), F32),
            pltpu.VMEM((blocks, 64, LANES), F32),
            pltpu.VMEM((1024, PAIRS * LANES), BF16),
            pltpu.VMEM((1024, chans), BF16),
            pltpu.VMEM((PAIRS * 256, chans), BF16),
            pltpu.VMEM((32, each, LANES), BF16),
            pltpu.VMEM((32 * each, LANES), F32),
            pltpu.VMEM((chans, PAIRS * LANES), BF16),
            pltpu.VMEM((2, 256, LANES), F32),
            pltpu.SemaphoreType.DMA,
        ],
        compiler_params=params,
        name="mix",
    )(*own, *other, far(weights), gn_gain[None], offset)

    partial = lax.all_to_all(partial, ("gy", "gx_1"), 0, 0, tiled=True)
    rows, mass = pl.pallas_call(
        step_kernel,
        out_shape=(shape((32, chans), BF16), shape((64, LANES), F32)),
        in_specs=[VMEM] * 2,
        out_specs=(VMEM,) * 2,
        compiler_params=params,
        name="step",
    )(partial, start)
    mass = lax.all_to_all(mass.reshape(64, 1, LANES), ("gx_0",) + PROBE, 0, 0, tiled=True)
    tall = lax.axis_size("probe_0")
    facing_rows = lax.ppermute(rows, "probe_0", [(y, y ^ 1) for y in range(tall)])
    scale = -0.25 / (probe_signs.shape[0] * lax.axis_size(PROBE))
    return pl.pallas_call(
        lambda *refs: final_kernel(scale, *refs),
        out_shape=(shape(state.shape, BF16), shape((4,), F32)),
        in_specs=[VMEM] * 3,
        out_specs=(VMEM, SMEM),
        scratch_shapes=[pltpu.VMEM((blocks, 64, LANES), F32)],
        compiler_params=params,
        name="final",
    )(mass.reshape(64, LANES), rows, facing_rows)


def solution(mesh):
    split = Mesh(
        mesh.devices.reshape(mesh.shape["gy"], 2, 2, 8, 4),
        ("gy", "gx_0", "gx_1", "probe_0", "probe_1"),
    )
    return jax.shard_map(
        body,
        mesh=split,
        in_specs=(
            P(None, "gy", GX, None),
            P(PROBE, None, "gy", GX, None),
            P(),
            P(),
            P(),
            P(),
            P(None, PROBE, None),
            P(),
        ),
        out_specs=(P(None, "gy", GX, None), P()),
        check_vma=False,
    )
```
